32 devices in a mesh: patch: 8 (over z, y), dir: 4 (over x, core).
Axes of the slice: x: 2, y: 2, z: 4, core: 2. Of those that a mesh axis runs over, the one named last changes fastest.
Arguments:
- right_side: float32 [96, 192, 256], P('dir', 'patch'), may hold values from -6 to 6
- guess: float32 [96, 192, 256], P('dir', 'patch'), may hold values from -3 to 3
- mask_fine: int32 [96, 192, 2], P('dir', 'patch'), may hold values 0 or 1
- mask_next: int32 [48, 96, 1], P('dir', 'patch'), may hold values 0 or 1
Outputs:
- solution: float32 [96, 192, 256], P('dir', 'patch')
The draws below stay inside these ranges and needn't reach their ends.
All inputs are finite; a program needn't handle non-finite values. No bound on the sum of `mask_fine` or of `mask_next` on one device may be relied on, other than what follows from the above.
Results may differ from the reference program's by a relative error of at most 0.00005.
Values sent between devices are 32-bit elements; how exact they have to be, the bound alone decides.
A program may use at most 64 MiB of HBM per device.

```python
import jax
import jax.numpy as jnp
from jax import lax

NW = 256
TILE = 128
SWEEPS = 3
LEVELS = 4
NU = 96
NV = 192


def with_ends(result, rng, low, top_value):
    index_at = [jax.random.randint(jax.random.fold_in(rng, axis), (), 0, length) for axis, length in enumerate(result.shape)]
    main_axis = result.shape.index(max(result.shape))
    neighbour = index_at[:main_axis] + [(index_at[main_axis] + 1) % result.shape[main_axis]] + index_at[main_axis + 1:]
    return result.at[tuple(index_at)].set(low).at[tuple(neighbour)].set(top_value)


def steps_of(rng, extent, cuts, smallest, largest):
    level, own = 1.0, jax.random.fold_in(rng, 6)
    for dim, blocks in cuts:
        steps = jnp.exp(jax.random.uniform(jax.random.fold_in(own, dim), (blocks,), jnp.float32, smallest / len(cuts), largest / len(cuts)))
        level = level * jnp.repeat(steps, extent[dim] // blocks).reshape([-1 if axis == dim else 1 for axis in range(len(extent))])
    return level


def normal_values(rng, dims, scale, most, shards=(), kind=jnp.bfloat16):
    values = jax.random.normal(rng, dims, jnp.float32) * scale
    if len(shards) > 0:
        values = steps_of(rng, dims, shards, -0.22, 0.18) * values
    return jnp.clip(values, min=-most, max=most).astype(kind)


def setup_inputs(seed: int = 0) -> dict:
    arg_keys = jax.random.split(jax.random.key(seed), 5)
    right_side = normal_values(arg_keys[0], (NU, NV, NW), 1.0, 6.0, ((0, 4), (1, 8)), jnp.float32)
    guess = normal_values(arg_keys[1], (NU, NV, NW), 0.5, 3.0, ((0, 4), (1, 8)), jnp.float32)
    mask_fine = with_ends((jax.random.randint(arg_keys[2], (NU, NV, NW // TILE), 0, 4) < 3).astype(jnp.int32), jax.random.fold_in(arg_keys[2], 1), 0, 1)
    mask_next = with_ends((jax.random.randint(arg_keys[3], (NU // 2, NV // 2, NW // (2 * TILE)), 0, 4) < 3).astype(jnp.int32), jax.random.fold_in(arg_keys[3], 1), 0, 1)
    return {"right_side": right_side, "guess": guess, "mask_fine": mask_fine, "mask_next": mask_next}


MASS = (1.0 / 5040, 120.0 / 5040, 1191.0 / 5040, 2416.0 / 5040, 1191.0 / 5040, 120.0 / 5040, 1.0 / 5040)
STIFF = (-1.0 / 120, -0.2, -0.125, 2.0 / 3, -0.125, -0.2, -1.0 / 120)
SUBDIV = (0.125, 0.5, 0.75, 0.5, 0.125)
OMEGA = 0.5


def wrap_pad(values, dimension, width, periodic):
    length = values.shape[dimension]
    if periodic:
        return jnp.concatenate([lax.slice_in_dim(values, length - width, length, axis=dimension), values, lax.slice_in_dim(values, 0, width, axis=dimension)], axis=dimension)
    widths = [(0, 0)] * values.ndim
    widths[dimension] = (width, width)
    return jnp.pad(values, widths)


def band_line(values, dimension, stencil, periodic):
    length = values.shape[dimension]
    padded = wrap_pad(values, dimension, 3, periodic)
    running = stencil[0] * lax.slice_in_dim(padded, 0, length, axis=dimension)
    for offset in range(1, 7):
        running = running + stencil[offset] * lax.slice_in_dim(padded, offset, offset + length, axis=dimension)
    return running


def restrict_line(values, dimension, periodic):
    halved = values.shape[dimension] // 2
    padded = wrap_pad(values, dimension, 2, periodic)
    running = SUBDIV[0] * lax.slice_in_dim(padded, 0, 2 * halved - 1, stride=2, axis=dimension)
    for offset in range(1, 5):
        running = running + SUBDIV[offset] * lax.slice_in_dim(padded, offset, offset + 2 * halved - 1, stride=2, axis=dimension)
    return running


def prolong_line(values, dimension, periodic):
    length = values.shape[dimension]
    padded = wrap_pad(values, dimension, 1, periodic)
    upper_part = lax.slice_in_dim(padded, 2, length + 2, axis=dimension)
    middle_part = lax.slice_in_dim(padded, 1, length + 1, axis=dimension)
    lower_part = lax.slice_in_dim(padded, 0, length, axis=dimension)
    even_part = SUBDIV[0] * upper_part + SUBDIV[2] * middle_part + SUBDIV[4] * lower_part
    odd_part = SUBDIV[1] * upper_part + SUBDIV[3] * middle_part
    joined = jnp.stack([even_part, odd_part], axis=dimension + 1)
    old_shape = values.shape
    return joined.reshape(old_shape[:dimension] + (2 * length,) + old_shape[dimension + 1:])


def operate(current, scale_factor):
    mass_side = band_line(current, 2, MASS, False)
    stiff_side = band_line(current, 2, STIFF, False)
    first_term = band_line(mass_side, 1, MASS, True)
    second = band_line(mass_side, 1, STIFF, True) + band_line(stiff_side, 1, MASS, True)
    return scale_factor * (band_line(first_term, 0, STIFF, False) + band_line(second, 0, MASS, False))


def smooth(current, load, scale_factor, active):
    update = (OMEGA / scale_factor) * (load - operate(current, scale_factor))
    if active is not None:
        update = update * active
    return current + update


def cycle(load, current, level_index, actives):
    scale_factor = float(2 ** level_index)
    active = actives[level_index]
    for sweep_index in range(SWEEPS):
        current = smooth(current, load, scale_factor, active)
    if level_index + 1 < LEVELS:
        residual_field = load - operate(current, scale_factor)
        if active is not None:
            residual_field = residual_field * active
        coarse_load = restrict_line(restrict_line(restrict_line(residual_field, 2, False), 1, True), 0, False)
        correction = cycle(coarse_load, jnp.zeros_like(coarse_load), level_index + 1, actives)
        finer = prolong_line(prolong_line(prolong_line(correction, 2, False), 1, True), 0, False)
        if active is not None:
            finer = finer * active
        current = current + finer
    for sweep_index in range(SWEEPS):
        current = smooth(current, load, scale_factor, active)
    return current


def reference(right_side, guess, mask_fine, mask_next):
    actives = [jnp.repeat(mask_fine.astype(jnp.float32), TILE, axis=2), jnp.repeat(mask_next.astype(jnp.float32), TILE, axis=2)] + [None] * (LEVELS - 2)
    return cycle(right_side, guess * actives[0], 0, actives)
```

```python
import functools

import jax
import jax.numpy as jnp
import numpy as np
from jax import lax
from jax.experimental import pallas as pl
from jax.experimental.pallas import tpu as pltpu
from jax.sharding import PartitionSpec as P

TILE = 128
SWEEPS = 3
LEVELS = 4
MASS = tuple(v / 5040 for v in (1, 120, 1191, 2416, 1191, 120, 1))
STIFF = tuple(v / 120 for v in (-1, -24, -15, 80, -15, -24, -1))
SUBDIV = (0.125, 0.5, 0.75, 0.5, 0.125)
OMEGA = 0.5
MESH = pl.DeviceIdType.MESH
WAYS = ((0, 1), (0, -1), (1, 0), (1, 1), (1, -1), (-1, 0), (-1, 1), (-1, -1))


def up8(n):
    return -(-n // 8) * 8


def band(n, size, coeffs):
    i, j = np.indices((size, size))
    out = np.zeros((size, size), np.float32)
    for k, c in enumerate(coeffs):
        out[(j - i + 3 == k) & (i < n) & (j < n)] = c
    return out


def subdivision(n, rows, columns):
    i, j = np.indices((rows, columns))
    out = np.zeros((rows, columns), np.float32)
    for k, c in enumerate(SUBDIV):
        out[(i - 2 * j + 2 == k) & (i < 2 * n) & (j < n)] = c
    return out


def weights(width):
    bands, moves = [], []
    for level in range(LEVELS):
        n = width >> level
        size = max(n, 128)
        mass = band(n, size, (1, 120, 1191, 2416, 1191, 120, 1))
        high = mass.astype(jnp.bfloat16)
        low = (mass - high.astype(np.float32)).astype(jnp.bfloat16)
        stiff = band(n, size, (-1, -24, -15, 80, -15, -24, -1)).astype(jnp.bfloat16)
        bands.append(np.stack([high, low, stiff]))
        if level + 1 < LEVELS:
            move = subdivision(n // 2, size, max(n // 2, 128))
            moves.append((move.astype(jnp.bfloat16), np.ascontiguousarray(move.T).astype(jnp.bfloat16)))
    return bands, moves


def parts(x):
    high = x.astype(jnp.bfloat16)
    return high, (x - high.astype(jnp.float32)).astype(jnp.bfloat16)


def mul(a, b):
    return jnp.dot(a, b, preferred_element_type=jnp.float32)


def taps(x, coeffs):
    sums = (x[0] + x[6], x[1] + x[5], x[2] + x[4], x[3])
    total = coeffs[3] * sums[3]
    for k in range(3):
        total = total + coeffs[k] * sums[k]
    return total


BASIS = (2496, 1176, 96)
KAPPA = OMEGA * 42 / 5040.0**3


def coarse_weights(width):
    wide, narrow = width >> 2, width >> 3
    tables = []
    for n in (wide, narrow):
        copies = np.eye(128 // n, dtype=np.float32)
        five = band(n, n, (0, 96, 1176, 2496, 1176, 96, 0))
        stiff = band(n, n, (-1, -24, -15, 80, -15, -24, -1))
        tables.append(np.stack([np.kron(copies, five), np.kron(copies, stiff)]))
    move = subdivision(narrow, wide, narrow)
    halves = np.eye(128 // wide, dtype=np.float32)
    down = np.kron(halves, np.concatenate([move, move], axis=1))
    zero = np.zeros_like(move.T)
    even = np.kron(halves, np.concatenate([move.T, zero], axis=0))
    odd = np.kron(halves, np.concatenate([zero, move.T], axis=0))
    tables.append(np.stack([down, even, odd]))
    return [t.astype(jnp.bfloat16) for t in tables]


def sums(x):
    return x[3], x[2] + x[4], x[1] + x[5], x[0] + x[6]


def five_taps(s):
    return BASIS[0] * s[0] + BASIS[1] * s[1] + BASIS[2] * s[2]


def stiff_taps(s):
    return 80.0 * s[0] - 15.0 * s[1] - 24.0 * s[2] - s[3]


def first_pass(x):
    s = sums(x)
    b, k = five_taps(s), stiff_taps(s)
    d = b - 2.0 * k
    return d, d + (b - k)


def second_pass(d, e):
    d, e = sums(d), sums(e)
    g = five_taps(e) - (4912.0 * d[0] + 2367.0 * d[1] + 216.0 * d[2] + d[3])
    q = five_taps(d) - stiff_taps(e)
    return g, q


def split_mul(x, table):
    high, low = parts(x)
    n = x.shape[0]
    both = mul(jnp.concatenate([high, low], axis=0), table)
    return both[:n] + both[n:]


def last_pass(g, q, table):
    return split_mul(g, table[0]) + split_mul(q, table[1])


def rows_at_once(count, rows):
    best = 1
    for n in range(1, count + 1):
        if count % n == 0 and n * rows <= 192:
            best = n
    return best


def loop(count, body, unroll=1):
    while count % unroll:
        unroll -= 1
    lax.fori_loop(0, count, lambda i, _: (body(i), 0)[1], 0, unroll=unroll)


def apply_packed(x, d, e, table, at, base, rows, count, use):
    def one(u):
        d[u + 3], e[u + 3] = first_pass([x[at + u, base - 3 + k : base - 3 + k + rows, :] for k in range(7)])

    loop(count, one, 3)
    size = rows_at_once(count, rows)

    def some(i):
        u = i * size
        gs, qs = [], []
        for j in range(size):
            g, q = second_pass([d[u + j + k] for k in range(7)], [e[u + j + k] for k in range(7)])
            gs.append(g)
            qs.append(q)
        value = last_pass(jnp.concatenate(gs, axis=0), jnp.concatenate(qs, axis=0), table)
        for j in range(size):
            use(u + j, value[j * rows : (j + 1) * rows])

    loop(count // size, some)


def coarse_cycle(shape, load2, tables, refs):
    nu, nh = shape
    cu, nq = nu // 2, nh // 4
    nqp = up8(nq)
    x2, d2, e2, b2, t2, x3, f3, d3, e3, z3 = refs
    edge = (x2.shape[0] - nu) // 2

    def put2(u, new):
        x2[edge + u, 8 : 8 + nh] = new
        x2[edge + u, 0:8] = pltpu.roll(new[nh - 8 : nh], 64, 1)
        x2[edge + u, 8 + nh : 16 + nh] = pltpu.roll(new[0:8], 64, 1)

    def put3(u, new):
        x3[u, 8 : 8 + nqp] = new
        left, right = pltpu.roll(new, 32, 1), pltpu.roll(new[0:8], 96, 1)
        x3[u, 5:8] = left[nq - 3 : nq]
        x3[u, 8 + nq : 11 + nq] = right[0:3]

    def smooth2():
        def use(u, value):
            put2(u, x2[edge + u, 8 : 8 + nh] + ((OMEGA / 4) * load2[u] - KAPPA * value))
        apply_packed(x2, d2, e2, tables[0], edge, 8, nh, nu, use)

    loop(nu, lambda u: put2(u, (OMEGA / 4) * load2[u]), 4)
    loop(SWEEPS - 1, lambda i: smooth2())

    size = rows_at_once(nu, nh)

    def keep(u, value):
        t2[u] = load2[u] - (8 * KAPPA) * value

    apply_packed(x2, d2, e2, tables[0], edge, 8, nh, nu, keep)

    def narrow(i):
        at = pl.ds(i * size, size)
        n = split_mul(t2[at].reshape(size * nh, 128), tables[2][0]).reshape(size, nh, 128)
        b2[pl.ds(i * size + 2, size), 8 : 8 + nh] = n
        for j in range(size):
            b2[i * size + 2 + j, 0:8] = pltpu.roll(n[j, nh - 8 : nh], 64, 1)
            b2[i * size + 2 + j, 8 + nh : 16 + nh] = pltpu.roll(n[j, 0:8], 64, 1)

    loop(nu // size, narrow)
    lane = lax.broadcasted_iota(jnp.int32, (nq, 128), 1)
    first = lax.rem(lane // 32, 2) == 0

    def restrict(i):
        total = None
        for k in range(5):
            term = SUBDIV[k] * b2[2 * i + k]
            total = term if total is None else total + term
        z3[i] = total
        lines = []
        for start in (6, 6 + 2 * nq):
            line = None
            for m in range(5):
                term = SUBDIV[m] * z3[i, pl.ds(start + m, nq, stride=2), :]
                line = term if line is None else line + term
            lines.append(line)
        f3[i, 0:nq] = jnp.where(first, lines[0], lines[1])

    loop(cu, restrict, 4)
    loop(cu, lambda u: put3(u, (OMEGA / 8) * f3[u]), 4)

    def smooth3(i):
        def use(u, value):
            put3(u, x3[u, 8 : 8 + nqp] + ((OMEGA / 8) * f3[u] - KAPPA * value))
        apply_packed(x3, d3, e3, tables[1], 0, 8, nqp, cu, use)

    loop(2 * SWEEPS - 1, smooth3)

    nf = 2 * nq
    for u in range(cu):
        b, h, a = (x3[u, 7 + s : 7 + s + nq] for s in range(3))
        b2[2 + u, pl.ds(0, nq, stride=2), :] = 0.125 * (b + a) + 0.75 * h
        b2[2 + u, pl.ds(1, nq, stride=2), :] = 0.5 * (h + a)
    fine = up8(nf)
    for u in range(cu):
        here = b2[2 + u, 0:fine]
        after = b2[3 + u, 0:fine] if u + 1 < cu else jnp.zeros_like(here)
        before = b2[1 + u, 0:fine] if u > 0 else jnp.zeros_like(here)
        t2[2 * u, 0:fine] = 0.125 * (before + after) + 0.75 * here
        t2[2 * u + 1, 0:fine] = 0.5 * (here + after)

    def widen(i):
        at = pl.ds(i * size, size)
        z = t2[at, 0:fine].reshape(size * fine, 128)
        y = (split_mul(z, tables[2][1]).reshape(size, fine, 128), split_mul(z, tables[2][2]).reshape(size, fine, 128))
        for j in range(size):
            u = edge + i * size + j
            for s in range(2):
                x2[u, 8 + s * nf : 8 + (s + 1) * nf] += y[s][j, 0:nf]
            put2(i * size + j, x2[u, 8 : 8 + nh])

    loop(nu // size, widen)
    loop(SWEEPS, lambda i: smooth2())


def kernel(sets, n_dir, n_patch, rs, guess, s0, s1, *refs):
    bands, refs = refs[:2], refs[2:]
    moves, refs = refs[:4], refs[4:]
    tables, refs = refs[:3], refs[3:]
    out, refs = refs[0], refs[1:]
    bufs = []
    for _ in sets:
        bufs.append(refs[:6])
        refs = refs[6:]
    fields = []
    for level in range(2):
        fields.append(refs[:6])
        refs = refs[6:]
    c2, packed, slots, load2 = refs[:4]
    coarse, refs = refs[4:14], refs[14:]
    send_sem, recv_sem, all_send, all_recv = refs
    masks = (s0, s1)

    me_u, me_v = lax.axis_index("dir"), lax.axis_index("patch")
    has_down, has_up = me_u > 0, me_u < n_dir - 1

    def device(a, b):
        return {"dir": me_u + a, "patch": lax.rem(me_v + b + n_patch, n_patch)}

    def when_way(a, body):
        if a == 0:
            body()
        else:
            pl.when(has_up if a > 0 else has_down)(body)

    n_all = n_dir * n_patch
    me = me_u * n_patch + me_v

    def place(flat):
        return lax.div(flat, n_patch), lax.rem(flat, n_patch)

    barrier = pltpu.get_barrier_semaphore()

    def greet(i):
        u, v = place(lax.rem(me + 1 + i, n_all))
        pl.semaphore_signal(barrier, inc=1, device_id={"dir": u, "patch": v}, device_id_type=MESH)

    loop(n_all - 1, greet)
    for ref in (coarse[0], coarse[1], coarse[2], coarse[3], coarse[6], coarse[7], coarse[8]):
        ref[...] = jnp.zeros_like(ref)

    for (nu, nv, nvp, w), (c, sl, sr, rl, rr, p) in zip(sets, bufs):
        p[:, nvp + 8 :, :] = jnp.zeros((nu + 6, 8, w), jnp.float32)
        for flag, at in ((me_u == 0, 0), (me_u == n_dir - 1, nu + 3)):
            @pl.when(flag)
            def _():
                c[:, at : at + 3] = jnp.zeros((2, 3, nvp, w), jnp.float32)
                rl[:, at : at + 3] = jnp.zeros((2, 3, 3, w), jnp.float32)
                rr[:, at : at + 3] = jnp.zeros((2, 3, 3, w), jnp.float32)

    pl.semaphore_wait(barrier, n_all - 1)

    def exchange(which, x, number):
        nu, nv, nvp, w = sets[which]
        c, sl, sr, rl, rr, p = bufs[which]
        slot = lax.rem(number, 2)

        def stage(u, _):
            row = x[u]
            c[slot, u + 3] = row
            sl[slot, u] = row[0:3]
            sr[slot, u] = row[nv - 3 : nv]
            return 0

        lax.fori_loop(0, nu, stage, 0, unroll=min(nu, 4))

        def copy(index):
            a, b = WAYS[index]
            if b == 0:
                at, to = (nu, 0) if a > 0 else (3, nu + 3)
                src, dst = c.at[slot, at : at + 3], c.at[slot, to : to + 3]
            else:
                near, far = (sr, rl) if b > 0 else (sl, rr)
                if a == 0:
                    src, dst = near.at[slot], far.at[slot, 3 : nu + 3]
                else:
                    at, to = (nu - 3, 0) if a > 0 else (0, nu + 3)
                    src, dst = near.at[slot, at : at + 3], far.at[slot, to : to + 3]
            return pltpu.make_async_remote_copy(
                src_ref=src,
                dst_ref=dst,
                send_sem=send_sem.at[slot, index],
                recv_sem=recv_sem.at[slot, index],
                device_id=device(a, b),
                device_id_type=MESH,
            )

        for step in (1, -1, 0):
            def start():
                for index, (a, b) in enumerate(WAYS):
                    if a == step:
                        copy(index).start()
            when_way(step, start)
        for step in (0, 1, -1):
            def finish():
                for index, (a, b) in enumerate(WAYS):
                    if a == step:
                        copy(index).wait_send()
                    if a == -step:
                        copy(index).wait_recv()
            when_way(step, finish)

        def gather(u, _):
            p[u, 8 : 8 + nvp] = c[slot, u]
            p[u, 5:8] = rl[slot, u]
            p[u, 8 + nv : 11 + nv] = rr[slot, u]
            return 0

        lax.fori_loop(0, nu + 6, gather, 0, unroll=6 if nu % 6 == 0 else 3)

    def chunked(which, body):
        nu, nv, nvp, w = sets[which]
        size = nu
        while size * nvp > 192 and size % 2 == 0:
            size //= 2
        if size == nu:
            body(0, nu)
        else:
            lax.fori_loop(0, nu // size, lambda i, _: (body(i * size, size), 0)[1], 0)

    def operate(level, x, number, use):
        which = set_of[level]
        nu, nv, nvp, w = sets[which]
        p = bufs[which][5]
        load, field, pu, ku, g, h = fields[level]
        exchange(which, x, number)

        def sublanes(u, _):
            t = [p[u, 5 + k : 5 + k + nvp, :] for k in range(7)]
            pu[u] = taps(t, [v / 5040 for v in MASS])
            ku[u] = taps(t, [v / 5040 for v in STIFF])
            return 0

        lax.fori_loop(0, nu + 6, sublanes, 0, unroll=6 if nu % 6 == 0 else 3)

        def leading(u, _):
            a = [pu[u + k] for k in range(7)]
            b = [ku[u + k] for k in range(7)]
            g[u] = taps(a, STIFF) + taps(b, MASS)
            h[u] = taps(a, [v * 42 for v in MASS])
            return 0

        lax.fori_loop(0, nu, leading, 0, unroll=4 if nu % 4 == 0 else 3)
        table = bands[level]

        def finish(u, size):
            g_high, g_low = parts(g[pl.ds(u, size)].reshape(size * nvp, w))
            h_high, h_low = parts(h[pl.ds(u, size)].reshape(size * nvp, w))
            value = mul(g_high, table[0]) + mul(g_low, table[0]) + mul(g_high, table[1])
            value = value + mul(h_high, table[2]) + mul(h_low, table[2])
            use(pl.ds(u, size), value.reshape(size, nvp, w))

        chunked(which, finish)

    def sweep(level, number):
        load, field = fields[level][:2]
        mask = masks[level]

        def use(at, value):
            update = (OMEGA / 2**level) * load[at] - OMEGA * value
            if mask is not None:
                update = update * mask[at]
            field[at] = field[at] + update

        operate(level, field, number, use)

    def sweeps(level, count, number):
        def body(i, _):
            sweep(level, number + i)
            return 0

        lax.fori_loop(0, count, body, 0)
        return number + count

    def descend(level, number):
        which = set_of[level]
        nu, nv, nvp, w = sets[which]
        load, field, pu, ku, g, h = fields[level]
        mask = masks[level]
        if level == 0:
            number = sweeps(level, SWEEPS, number)
        else:
            first = (OMEGA / 2**level) * load[...]
            field[...] = first if mask is None else first * mask[...]
            number = sweeps(level, SWEEPS - 1, number)
        if True:
            low_which = 1 if level == 0 else which
            low_p = bufs[low_which][5]
            down, up = moves[2 * level], moves[2 * level + 1]
            lanes = down.shape[1]

            def residual(at, value):
                r = load[at] - float(2**level) * value
                if mask is not None:
                    r = r * mask[at]
                size = r.shape[0]
                r_high, r_low = parts(r.reshape(size * nvp, w))
                n = mul(r_high, down[...]) + mul(r_low, down[...])
                g[at, :, 0:lanes] = n.reshape(size, nvp, lanes)

            operate(level, field, number, residual)
            number += 1
            exchange(low_which, g.at[:, :, 0:lanes], number)
            number += 1
            if level == 0:
                cu, cv, cvp, cw = sets[set_of[1]]
                c_load, c_field = fields[1][:2]
                c_p = bufs[set_of[1]][5]
                corner = (3, 8)
            else:
                cu, cv, cvp, cw = nu // 2, nv // 2, up8(nv // 2), 128
                c_load = c2
                c_p = coarse[0]
                corner = ((c_p.shape[0] - cu * n_dir) // 2 + me_u * cu, 8 + cv)
            c_load[...] = jnp.zeros((cu, cvp, cw), jnp.float32)
            for i in range(cu):
                total = None
                for k in range(5):
                    line = None
                    for m in range(5):
                        term = SUBDIV[m] * low_p[2 * i + k + 1, pl.ds(6 + m, cv, stride=2), :]
                        line = term if line is None else line + term
                    total = SUBDIV[k] * line if total is None else total + SUBDIV[k] * line
                c_load[i, 0:cv, :] = total
            if level == 0:
                number = descend(1, number)
                exchange(set_of[1], c_field, number)
                number += 1
            else:
                gather_all(cu, cv)
                coarse_cycle((cu * n_dir, cv * n_patch // 2), load2, tables, coarse)
            for u in range(nu):
                i = u // 2 + corner[0]
                mix = ((i - 1, 0.125), (i, 0.75), (i + 1, 0.125)) if u % 2 == 0 else ((i, 0.5), (i + 1, 0.5))
                shifted = []
                for d in range(3):
                    total = None
                    for row, c in mix:
                        term = c * c_p[row, corner[1] - 1 + d : corner[1] - 1 + d + cv, :]
                        total = term if total is None else total + term
                    shifted.append(total)
                before, here, after = shifted
                spread[level][u, pl.ds(0, cv, stride=2), :] = 0.125 * (before + after) + 0.75 * here
                spread[level][u, pl.ds(1, cv, stride=2), :] = 0.5 * (here + after)

            def correct(at, size):
                at = pl.ds(at, size)
                y_high, y_low = parts(spread[level][at].reshape(size * nvp, lanes))
                y = (mul(y_high, up[...]) + mul(y_low, up[...])).reshape(size, nvp, w)
                if mask is not None:
                    y = y * mask[at]
                field[at] = field[at] + y

            chunked(which, correct)
        return sweeps(level, SWEEPS, number)

    def gather_all(cu, cv):
        half = cu // 2
        for j in range(half):
            packed[j] = (c2[j] + pltpu.roll(c2[j + half], 64, 1))[0:cv]
            slots[me_u, 1, j] = packed[j]

        def copy(i, incoming):
            flat = lax.rem(me + 1 + i, n_all) if not incoming else lax.rem(me + n_all - 1 - i, n_all)
            u, v = place(flat)
            source_u, source_v, target_v = (u, v, me_v) if incoming else (me_u, me_v, v)
            return pltpu.make_async_remote_copy(
                src_ref=packed,
                dst_ref=slots.at[source_u, lax.rem(source_v - target_v + 1 + n_patch, n_patch)],
                send_sem=all_send.at[i],
                recv_sem=all_recv.at[i],
                device_id={"dir": u, "patch": v},
                device_id_type=MESH,
            )

        loop(n_all - 1, lambda i: copy(i, False).start())
        loop(n_all - 1, lambda i: copy(i, False).wait_send())
        loop(n_all - 1, lambda i: copy(i, True).wait_recv())
        low = lax.broadcasted_iota(jnp.int32, (cv, 128), 1) < 64
        for d in range(n_dir):
            for k in range(n_patch // 2):
                for j in range(half):
                    a, b = slots[d, k, j], slots[d, k + n_patch // 2, j]
                    load2[d * cu + j, k * cv : (k + 1) * cv] = jnp.where(low, a, pltpu.roll(b, 64, 1))
                    load2[d * cu + half + j, k * cv : (k + 1) * cv] = jnp.where(low, pltpu.roll(a, 64, 1), b)

    set_of = [0, 2]
    spread = [bufs[1][0].at[0], fields[1][3]]
    load, field = fields[0][:2]
    load[...] = rs[...]
    field[...] = guess[...] * s0[...]
    descend(0, 0)
    out[...] = field[...]


def on_device(right_side, guess, mask_fine, mask_next):
    nu, nv, nw = right_side.shape
    sets = [(nu, nv, up8(nv), nw), (nu, nv, up8(nv), max(nw // 2, 128))]
    sets.append((nu >> 1, nv >> 1, up8(nv >> 1), max(nw >> 1, 128)))
    sets = tuple(sets)
    bands, moves = weights(nw)
    s0 = jnp.repeat(mask_fine.astype(jnp.float32), TILE, axis=2)
    s1 = jnp.repeat(mask_next.astype(jnp.float32), TILE, axis=2)
    s1 = jnp.pad(s1, ((0, 0), (0, sets[2][2] - sets[2][1]), (0, sets[2][3] - s1.shape[2])))
    operands = [right_side, guess, s0, s1] + [jnp.asarray(b) for b in bands[:2]]
    operands += [jnp.asarray(m) for pair in moves[:2] for m in pair]
    operands += [jnp.asarray(t) for t in coarse_weights(nw)]
    n_dir, n_patch = lax.axis_size("dir"), lax.axis_size("patch")
    cu, cv = nu >> 2, nv >> 2
    gu, gh = cu * n_dir, cv * n_patch // 2
    eu, eq = gu // 2, up8(gh // 4)
    scratch = []
    for u, v, vp, w in sets:
        scratch += [pltpu.VMEM((2, u + 6, vp, w), jnp.float32)]
        scratch += [pltpu.VMEM((2, u, 3, w), jnp.float32)] * 2
        scratch += [pltpu.VMEM((2, u + 6, 3, w), jnp.float32)] * 2
        scratch += [pltpu.VMEM((u + 6, vp + 16, w), jnp.float32)]
    for which in (0, 2):
        u, v, vp, w = sets[which]
        scratch += [pltpu.VMEM((u, vp, w), jnp.float32)] * 2
        scratch += [pltpu.VMEM((u + 6, vp, w), jnp.float32)] * 2
        scratch += [pltpu.VMEM((u, vp, w), jnp.float32)] * 2
    scratch += [
        pltpu.VMEM((cu, up8(cv), 128), jnp.float32),
        pltpu.VMEM((cu // 2, cv, 128), jnp.float32),
        pltpu.VMEM((n_dir, n_patch, cu // 2, cv, 128), jnp.float32),
        pltpu.VMEM((gu, gh, 128), jnp.float32),
        pltpu.VMEM((gu + 18, gh + 16, 128), jnp.float32),
        pltpu.VMEM((gu + 6, gh, 128), jnp.float32),
        pltpu.VMEM((gu + 6, gh, 128), jnp.float32),
        pltpu.VMEM((gu + 4, gh + 16, 128), jnp.float32),
        pltpu.VMEM((gu, gh, 128), jnp.float32),
        pltpu.VMEM((eu, eq + 16, 128), jnp.float32),
        pltpu.VMEM((eu, eq, 128), jnp.float32),
        pltpu.VMEM((eu + 6, eq, 128), jnp.float32),
        pltpu.VMEM((eu + 6, eq, 128), jnp.float32),
        pltpu.VMEM((eu, gh + 16, 128), jnp.float32),
    ]
    scratch += [pltpu.SemaphoreType.DMA((2, 8)), pltpu.SemaphoreType.DMA((2, 8))]
    scratch += [pltpu.SemaphoreType.DMA((n_dir * n_patch - 1,))] * 2
    vmem = pl.BlockSpec(memory_space=pltpu.VMEM)
    return pl.pallas_call(
        functools.partial(kernel, sets, n_dir, n_patch),
        out_shape=jax.ShapeDtypeStruct(right_side.shape, jnp.float32),
        in_specs=[vmem] * len(operands),
        out_specs=vmem,
        scratch_shapes=scratch,
        compiler_params=pltpu.CompilerParams(
            collective_id=0, has_side_effects=True, vmem_limit_bytes=60 * 2**20
        ),
        name="vcycle",
    )(*operands)


def solution(mesh):
    spec = P("dir", "patch", None)
    return jax.shard_map(
        on_device, mesh=mesh, in_specs=(spec,) * 4, out_specs=spec, check_vma=False
    )
```

```python
import functools

import jax
import jax.numpy as jnp
import numpy as np
from jax import lax
from jax.experimental import pallas as pl
from jax.experimental.pallas import tpu as pltpu
from jax.sharding import PartitionSpec as P

TILE = 128
SWEEPS = 3
LEVELS = 4
SUBDIV = (0.125, 0.5, 0.75, 0.5, 0.125)
OMEGA = 0.5
MESH = pl.DeviceIdType.MESH
AROUND = ((0, 1), (0, -1), (1, 0), (-1, 0), (1, 1), (1, -1), (-1, 1), (-1, -1))
BASIS = (2496, 1176, 96)
KAPPA = OMEGA * 42 / 5040.0**3
FAR = 4


def up8(n):
    return -(-n // 8) * 8


def band(n, size, coeffs):
    i, j = np.indices((size, size))
    out = np.zeros((size, size), np.float32)
    for k, c in enumerate(coeffs):
        out[(j - i + 3 == k) & (i < n) & (j < n)] = c
    return out


def subdivision(n, rows, columns):
    i, j = np.indices((rows, columns))
    out = np.zeros((rows, columns), np.float32)
    for k, c in enumerate(SUBDIV):
        out[(i - 2 * j + 2 == k) & (i < 2 * n) & (j < n)] = c
    return out


def coarse_weights(width):
    wide, narrow = width >> 2, width >> 3
    tables = []
    for n in (wide, narrow):
        copies = np.eye(128 // n, dtype=np.float32)
        five = band(n, n, (0, 96, 1176, 2496, 1176, 96, 0))
        stiff = band(n, n, (-1, -24, -15, 80, -15, -24, -1))
        tables.append(np.stack([np.kron(copies, five), np.kron(copies, stiff)]))
    move = subdivision(narrow, wide, narrow)
    halves = np.eye(128 // wide, dtype=np.float32)
    down = np.kron(halves, np.concatenate([move, move], axis=1))
    zero = np.zeros_like(move.T)
    even = np.kron(halves, np.concatenate([move.T, zero], axis=0))
    odd = np.kron(halves, np.concatenate([zero, move.T], axis=0))
    tables.append(np.stack([down, even, odd]))
    return [t.astype(jnp.bfloat16) for t in tables]


def parts(x):
    high = x.astype(jnp.bfloat16)
    return high, (x - high.astype(jnp.float32)).astype(jnp.bfloat16)


def mul(a, b):
    return jnp.dot(a, b, preferred_element_type=jnp.float32)


def sums(x):
    return x[3], x[2] + x[4], x[1] + x[5], x[0] + x[6]


def five_taps(s):
    return BASIS[0] * s[0] + BASIS[1] * s[1] + BASIS[2] * s[2]


def stiff_taps(s):
    return 80.0 * s[0] - 15.0 * s[1] - 24.0 * s[2] - s[3]


def first_pass(x):
    s = sums(x)
    d, e = 2 * KAPPA * s[3], 3 * KAPPA * s[3]
    for k, (p, q) in enumerate(((2336, 4752), (1206, 2397), (144, 264))):
        d, e = d + p * KAPPA * s[k], e + q * KAPPA * s[k]
    return d, e


def second_pass(d, e):
    d, e = sums(d), sums(e)
    g = five_taps(e) - (4912.0 * d[0] + 2367.0 * d[1] + 216.0 * d[2] + d[3])
    q = five_taps(d) - stiff_taps(e)
    return g, q


def split_mul(x, table):
    high, low = parts(x)
    n = x.shape[0]
    both = mul(jnp.concatenate([high, low], axis=0), table)
    return both[:n] + both[n:]


def last_pass(g, q, table):
    return split_mul(g, table[0]) + split_mul(q, table[1])


def rows_at_once(count, rows):
    best = 1
    for n in range(1, count + 1):
        if count % n == 0 and n * rows <= 240:
            best = n
    return best


def loop(count, body, unroll=1):
    while count % unroll:
        unroll -= 1
    lax.fori_loop(0, count, lambda i, _: (body(i), 0)[1], 0, unroll=unroll)


def apply_packed(x, d, e, table, at, base, rows, count, use):
    def one(u):
        d[u + 3], e[u + 3] = first_pass([x[at + u, base - 3 + k : base - 3 + k + rows, :] for k in range(7)])

    loop(count, one, 3)
    size = rows_at_once(count, rows)

    def some(i):
        u = i * size
        gs, qs = [], []
        for j in range(size):
            g, q = second_pass([d[u + j + k] for k in range(7)], [e[u + j + k] for k in range(7)])
            gs.append(g)
            qs.append(q)
        value = last_pass(jnp.concatenate(gs, axis=0), jnp.concatenate(qs, axis=0), table)
        for j in range(size):
            use(u + j, value[j * rows : (j + 1) * rows])

    loop(count // size, some)


def coarse_cycle(shape, load2, tables, refs, midway):
    nu, nh = shape
    cu, nq = nu // 2, nh // 4
    nqp = up8(nq)
    x2, d2, e2, b2, t2, x3, f3, d3, e3, z3 = refs
    edge = (x2.shape[0] - nu) // 2

    def put2(u, new):
        x2[edge + u, 8 : 8 + nh] = new
        x2[edge + u, 0:8] = pltpu.roll(new[nh - 8 : nh], 64, 1)
        x2[edge + u, 8 + nh : 16 + nh] = pltpu.roll(new[0:8], 64, 1)

    def put3(u, new):
        x3[u, 8 : 8 + nqp] = new
        left, right = pltpu.roll(new, 32, 1), pltpu.roll(new[0:8], 96, 1)
        x3[u, 5:8] = left[nq - 3 : nq]
        x3[u, 8 + nq : 11 + nq] = right[0:3]

    def smooth2():
        def use(u, value):
            put2(u, x2[edge + u, 8 : 8 + nh] + ((OMEGA / 4) * load2[u] - value))
        apply_packed(x2, d2, e2, tables[0], edge, 8, nh, nu, use)

    loop(nu, lambda u: put2(u, (OMEGA / 4) * load2[u]), 4)
    loop(SWEEPS - 1, lambda i: smooth2())

    size = rows_at_once(nu, nh)

    def keep(u, value):
        t2[u] = load2[u] - 8.0 * value

    apply_packed(x2, d2, e2, tables[0], edge, 8, nh, nu, keep)

    def narrow(i):
        at = pl.ds(i * size, size)
        n = split_mul(t2[at].reshape(size * nh, 128), tables[2][0]).reshape(size, nh, 128)
        b2[pl.ds(i * size + 2, size), 8 : 8 + nh] = n
        for j in range(size):
            b2[i * size + 2 + j, 0:8] = pltpu.roll(n[j, nh - 8 : nh], 64, 1)
            b2[i * size + 2 + j, 8 + nh : 16 + nh] = pltpu.roll(n[j, 0:8], 64, 1)

    loop(nu // size, narrow)
    midway()
    lane = lax.broadcasted_iota(jnp.int32, (nq, 128), 1)
    first = lax.rem(lane // 32, 2) == 0

    def restrict(i):
        total = None
        for k in range(5):
            term = SUBDIV[k] * b2[2 * i + k]
            total = term if total is None else total + term
        z3[i] = total
        lines = []
        for start in (6, 6 + 2 * nq):
            line = None
            for m in range(5):
                term = SUBDIV[m] * z3[i, pl.ds(start + m, nq, stride=2), :]
                line = term if line is None else line + term
            lines.append(line)
        f3[i, 0:nq] = jnp.where(first, lines[0], lines[1])

    loop(cu, restrict, 4)
    loop(cu, lambda u: put3(u, (OMEGA / 8) * f3[u]), 4)

    def smooth3(i):
        def use(u, value):
            put3(u, x3[u, 8 : 8 + nqp] + ((OMEGA / 8) * f3[u] - value))
        apply_packed(x3, d3, e3, tables[1], 0, 8, nqp, cu, use)

    loop(2 * SWEEPS - 1, smooth3)

    nf = 2 * nq
    for u in range(cu):
        b, h, a = (x3[u, 7 + s : 7 + s + nq] for s in range(3))
        b2[2 + u, pl.ds(0, nq, stride=2), :] = 0.125 * (b + a) + 0.75 * h
        b2[2 + u, pl.ds(1, nq, stride=2), :] = 0.5 * (h + a)
    fine = up8(nf)
    for u in range(cu):
        here = b2[2 + u, 0:fine]
        after = b2[3 + u, 0:fine] if u + 1 < cu else jnp.zeros_like(here)
        before = b2[1 + u, 0:fine] if u > 0 else jnp.zeros_like(here)
        t2[2 * u, 0:fine] = 0.125 * (before + after) + 0.75 * here
        t2[2 * u + 1, 0:fine] = 0.5 * (here + after)

    def widen(i):
        at = pl.ds(i * size, size)
        z = t2[at, 0:fine].reshape(size * fine, 128)
        y = (split_mul(z, tables[2][1]).reshape(size, fine, 128), split_mul(z, tables[2][2]).reshape(size, fine, 128))
        for j in range(size):
            u = edge + i * size + j
            for s in range(2):
                x2[u, 8 + s * nf : 8 + (s + 1) * nf] += y[s][j, 0:nf]
            put2(i * size + j, x2[u, 8 : 8 + nh])

    loop(nu // size, widen)
    loop(SWEEPS, lambda i: smooth2())


def fine_weights(width):
    tables = []
    for n in (width, width // 2):
        five = band(n, n, (0, 96, 1176, 2496, 1176, 96, 0))
        stiff = band(n, n, (-1, -24, -15, 80, -15, -24, -1))
        move = subdivision(n // 2, n, max(n // 2, 128))
        tables += [np.stack([five, stiff]), move, np.ascontiguousarray(move.T)]
    return [t.astype(jnp.bfloat16) for t in tables]


def spots(n, at, rows, gap, reach):
    out = np.zeros((rows, 128), np.float32)
    for p in range(at - reach, at + n + reach):
        b, v = divmod(p - at, n)
        out[p, gap * (b % (128 // gap)) + v] = 1
    return out


class Halo:
    def __init__(self, refs, near):
        self.near, self.reach = near, near + FAR
        (self.send_near, self.send_far, self.near_v, self.far_v, self.near_u, self.far_u) = refs

    @staticmethod
    def scratch(planes, nu, nv, near):
        rows = nu + 2 * (near + FAR)
        shapes = [(2, planes, nu, near, 128), (2, planes, nu, FAR, 128), (2, planes, rows, near, 128)]
        shapes += [(2, planes, rows, FAR, 128), (2, planes, near, nv, 128), (2, planes, FAR, nv, 128)]
        return [pltpu.VMEM(shape, jnp.float32) for shape in shapes]


def kernel(dims, rs, guess, mask0, mask1, *refs):
    n_dir, n_patch, nu, nv, planes = dims
    mu, mv = nu // 2, nv // 2
    cu, cv = mu // 2, mv // 2
    band0, down0, up0, band1, down1, up1 = refs[:6]
    tables, (pick, pick0, pick1), out, refs = refs[6:9], refs[9:12], refs[12], refs[13:]
    x0, s0, f0, d0, e0, x1, s1, f1, d1, e1, r1, r2, t1, tv, tw = refs[:15]
    refs = refs[15:]
    side_send, side_recv, up_recv = refs[:3]
    xh, fh = Halo(refs[3:9], 5), Halo(refs[9:15], 2)
    lines0, lines1, line0, line1 = refs[15:19]
    slab_f, slab_x, strip_x, slab_far = refs[19:23]
    c2, packed, slots, load2 = refs[23:27]
    coarse = refs[27:37]
    send_sem, recv_sem, all_send, all_recv = refs[37:]

    U0, V0, U1, V1 = 9, 16, mu + 3, mv + 10
    wide = (V0 - 8, nv + 16)
    me_u, me_v = lax.axis_index("dir"), lax.axis_index("patch")
    n_all = n_dir * n_patch
    me = me_u * n_patch + me_v

    def place(flat):
        return lax.div(flat, n_patch), lax.rem(flat, n_patch)

    def present(a):
        return None if a == 0 else (me_u < n_dir - a if a > 0 else me_u >= -a)

    def given(flag, body):
        body() if flag is None else pl.when(flag)(body)

    taken = [0]

    def number(count):
        taken[0] += count
        return taken[0] - count

    def copies(items, first):
        made = []
        for k, (src, dst, a, b) in enumerate(items):
            made.append((a, functools.partial(
                pltpu.make_async_remote_copy,
                src_ref=src, dst_ref=dst, send_sem=send_sem.at[first + k], recv_sem=recv_sem.at[first + k],
                device_id={"dir": me_u + a, "patch": lax.rem(me_v + b + 2 * n_patch, n_patch)},
                device_id_type=MESH)))
        return made

    def grouped(made, sign, act):
        for step in sorted({a for a, _ in made}, key=abs):
            def body():
                for a, make in made:
                    if a == step:
                        act(make())
            given(present(sign * step), body)

    def start(made):
        grouped(made, 1, lambda c: c.start())

    def sent(made):
        grouped(made, 1, lambda c: c.wait_send())

    def received(made):
        grouped(made, -1, lambda c: c.wait_recv())

    barrier = pltpu.get_barrier_semaphore()

    def greet(i):
        u, v = place(lax.rem(me + 1 + i, n_all))
        pl.semaphore_signal(barrier, inc=1, device_id={"dir": u, "patch": v}, device_id_type=MESH)

    loop(n_all - 1, greet)

    for k, at in enumerate((0, 32, 96)):
        line0[k] = jnp.zeros(line0.shape[1:], jnp.float32)
        line0[k, :, :, at : at + nv] = mask0[...].astype(jnp.float32)
    for k, at in enumerate((0, 16, 32, 96, 112)):
        line1[k] = jnp.zeros(line1.shape[1:], jnp.float32)
        line1[k, :, :, at : at + mv] = mask1[...].astype(jnp.float32)
    ones = jnp.ones((128, 128), jnp.bfloat16)

    def spread(pattern, line):
        return (pattern * line).astype(jnp.bfloat16)

    def own(i):
        marks = [[spread(pick[...], line0[0, i * 4 + j, w : w + 1, :]) for j in range(4)] for w in range(planes)]
        full = mul(jnp.concatenate([m for row in marks for m in row], axis=0), ones)
        for w in range(planes):
            for j in range(4):
                u, k = i * 4 + j, w * 4 + j
                m = full[k * nv : (k + 1) * nv]
                lanes = slice(w * 128, w * 128 + 128)
                x0[w, U0 + u, V0 : V0 + nv] = m * guess[u, :, lanes]
                f0[w, U0 + u, V0 : V0 + nv] = OMEGA * m * rs[u, :, lanes]
                s0[w, U0 + u, V0 : V0 + nv] = m

    for ref in (x0, s0, f0, x1, s1, f1):
        def clear(u):
            ref[:, u] = jnp.zeros((ref.shape[0],) + ref.shape[2:], jnp.float32)
        loop(ref.shape[1], clear, 3)
    loop(nu // 4, own)
    for ref in (coarse[0], coarse[1], coarse[2], coarse[3], coarse[6], coarse[7], coarse[8], c2, tv):
        ref[...] = jnp.zeros_like(ref)
    pl.semaphore_wait(barrier, n_all - 1)

    def mask_items():
        first, second = [], []
        for b in (0, 1, -1):
            for a in (0, 1, -1):
                if a or b:
                    rows = slice(0, nu) if a == 0 else (slice(nu - U0, nu) if a > 0 else slice(0, U0))
                    to = slice(U0, U0 + nu) if a == 0 else (slice(0, U0) if a > 0 else slice(U0 + nu, U0 + nu + U0))
                    first.append((line0.at[{0: 0, 1: 2, -1: 1}[b], rows], lines0.at[(-b) % 3, to], a, b))
        for b in range(-2, 3):
            for a in range(-2, 3):
                if a or b:
                    rows, to = block_rows(a)
                    second.append((line1.at[(-b) % 5, rows], lines1.at[(-b) % 5, to], a, b))
        return first + second

    def block_rows(a):
        edge = U1 - mu
        if abs(a) < 2:
            return slice(0, mu), slice(U1 - a * mu, U1 - a * mu + mu)
        return (slice(mu - edge, mu), slice(0, edge)) if a > 0 else (slice(0, edge), slice(U1 + 2 * mu, U1 + 2 * mu + edge))

    masks = copies(mask_items(), number(8 + 24))

    def expand():
        received(masks)
        for a, at, n in ((0, U0, nu), (-1, 0, U0), (1, U0 + nu, U0)):
            def body():
                def one(i):
                    u = at + 3 * i
                    marks = []
                    for w in range(planes):
                        for j in range(3):
                            line = lines0[1, u + j, w : w + 1, :] + lines0[2, u + j, w : w + 1, :]
                            if a == 0:
                                line = line + line0[0, u + j - U0, w : w + 1, :]
                            else:
                                line = line + lines0[0, u + j, w : w + 1, :]
                            marks.append(spread(pick0[...], line))
                    full = mul(jnp.concatenate(marks, axis=0), ones)
                    n0 = s0.shape[2]
                    for w in range(planes):
                        for j in range(3):
                            s0[w, u + j] = full[(w * 3 + j) * n0 : (w * 3 + j + 1) * n0]
                loop(n // 3, one)
            given(present(a), body)
        for a in (0, -1, 1, -2, 2):
            rows, to = block_rows(-a)
            def body():
                def one(i):
                    marks = []
                    for j in range(3):
                        u = to.start + 3 * i + j
                        line = line1[0, u - U1] if a == 0 else lines1[0, u]
                        for b in range(1, 5):
                            line = line + lines1[b, u]
                        marks.append(spread(pick1[...], line))
                    full = mul(jnp.concatenate(marks, axis=0), ones)
                    n1 = s1.shape[2]
                    for j in range(3):
                        s1[0, to.start + 3 * i + j] = full[j * n1 : (j + 1) * n1]
                loop((to.stop - to.start) // 3, one)
            given(present(a), body)

    def operate(x, d, e, table, u0, count, window, use):
        lo, size = window
        n = x.shape[0]

        def one(i):
            u = u0 - 3 + i
            for w in range(n):
                t = [x[w, u, lo - 3 + k : lo - 3 + k + size, :] for k in range(7)]
                d[w, u, 0:size], e[w, u, 0:size] = first_pass(t)

        loop(count + 6, one, 3)
        rows = rows_at_once(count, size)

        def some(i):
            u = u0 + i * rows
            gs, qs = [], []
            for w in range(n):
                both = [second_pass([d[w, u + j + k, 0:size] for k in range(-3, 4)], [e[w, u + j + k, 0:size] for k in range(-3, 4)])
                        for j in range(rows)]
                gs.append(jnp.concatenate([g for g, _ in both], axis=0))
                qs.append(jnp.concatenate([q for _, q in both], axis=0))
            use(u, rows, last_pass(jnp.concatenate(gs, axis=1), jnp.concatenate(qs, axis=1), table))

        loop(count // rows, some)

    def sweep(x, s, f, d, e, table, u0, count, window, result=None):
        lo, size = window

        def use(u, rows, value):
            for j in range(rows):
                for w in range(x.shape[0]):
                    v = value[j * size : (j + 1) * size, w * 128 : (w + 1) * 128]
                    at = (w, u + j, slice(lo, lo + size))
                    new = x[at] + (f[at] - s[at] * v)
                    if result is None:
                        x[at] = new
                    else:
                        result[u + j - u0, :, w * 128 : (w + 1) * 128] = new

        operate(x, d, e, table, u0, count, window, use)

    def residual(x, s, f, d, e, table, down, scale, u0, count, window, narrow):
        lo, size = window

        def use(u, rows, value):
            lines = []
            for j in range(rows):
                line = []
                for w in range(x.shape[0]):
                    v = value[j * size : (j + 1) * size, w * 128 : (w + 1) * 128]
                    at = (w, u + j, slice(lo, lo + size))
                    line.append(scale * (f[at] - s[at] * v))
                lines.append(jnp.concatenate(line, axis=1))
            n = split_mul(jnp.concatenate(lines, axis=0), down[...])
            for j in range(rows):
                narrow[u + j - u0, 0:size] = n[j * size : (j + 1) * size]

        operate(x, d, e, table, u0, count, window, use)

    def restrict(narrow, i, size, first, n):
        total = None
        for k in range(5):
            term = SUBDIV[k] * narrow[2 * i + k, 0:size]
            total = term if total is None else total + term
        t1[i, 0:size] = total
        line = None
        for m in range(5):
            term = SUBDIV[m] * t1[i, pl.ds(first + m, n, stride=2), :]
            line = term if line is None else line + term
        return line

    def near_items(x, h, strips, sides, ups):
        items = []
        top = U0 + nu
        for a, b in AROUND:
            k = 0 if b > 0 else 1
            if b == 0:
                rows = slice(top - h, top) if a > 0 else slice(U0, U0 + h)
                items.append((x.at[:, rows, V0 : V0 + nv], ups.at[0 if a > 0 else 1], a, b))
                continue
            reach = (sides.shape[-3] - nu) // 2
            rows = slice(0, nu) if a == 0 else (slice(nu - h, nu) if a > 0 else slice(0, h))
            at = reach if a == 0 else (reach - h if a > 0 else reach + nu)
            to = slice(at, at + rows.stop - rows.start)
            items.append((strips.at[1 - k, :, rows], sides.at[k, :, to], a, b))
        return items

    def stage(x, h, strips, skip=0):
        def one(u):
            for w in range(planes):
                strips[0, w, u] = x[w, U0 + u, V0 + skip : V0 + skip + h]
                strips[1, w, u] = x[w, U0 + u, V0 + nv - skip - h : V0 + nv - skip]
        loop(nu, one, 4)

    def lay_sides(x, h, sides, reach, skip=0, extra=None):
        extra = reach if extra is None else extra
        for a, at, n in ((0, U0, nu), (-1, U0 - extra, extra), (1, U0 + nu, extra)):
            def body():
                def one(i):
                    u = at + i
                    for w in range(planes):
                        x[w, u, V0 - skip - h : V0 - skip] = sides[0, w, u - U0 + reach]
                        x[w, u, V0 + nv + skip : V0 + nv + skip + h] = sides[1, w, u - U0 + reach]
                loop(n, one, 4)
            given(present(a), body)

    def lay_ups(x, h, ups, skip=0):
        def low():
            x[:, U0 - skip - h : U0 - skip, V0 : V0 + nv] = ups[0]
        def high():
            x[:, U0 + nu + skip : U0 + nu + skip + h, V0 : V0 + nv] = ups[1]
        given(present(-1), low)
        given(present(1), high)

    base = number(8 * SWEEPS)
    f_near = copies(near_items(f0, fh.near, fh.send_near, fh.near_v, fh.near_u), number(8))
    block0 = (V0, nv)

    def smooth0(i):
        stage(x0, 3, side_send.at[i])
        made = copies(near_items(x0, 3, side_send.at[i], side_recv.at[i], up_recv.at[i]), base + 8 * i)
        start(made)

        @pl.when(i == 0)
        def _():
            start(masks)
            stage(f0, fh.near, fh.send_near)
            start(f_near)

        pl.when(i == 1)(expand)
        received(made)
        sent(made)
        lay_sides(x0, 3, side_recv.at[i], 3)
        lay_ups(x0, 3, up_recv.at[i])
        sweep(x0, s0, f0, d0, e0, band0, U0, nu, block0)

    loop(SWEEPS, smooth0)

    stage(x0, xh.near, xh.send_near)
    x_near = copies(near_items(x0, xh.near, xh.send_near, xh.near_v, xh.near_u), number(8))
    start(x_near)
    stage(x0, FAR, xh.send_far, xh.near)
    stage(f0, FAR, fh.send_far, fh.near)
    received(f_near)
    lay_sides(f0, fh.near, fh.near_v, fh.reach, 0, fh.near)
    lay_ups(f0, fh.near, fh.near_u)
    received(x_near)
    lay_sides(x0, xh.near, xh.near_v, xh.reach, 0, xh.near)
    lay_ups(x0, xh.near, xh.near_u)
    residual(x0, s0, f0, d0, e0, band0, down0, 2.0, U0 - 2, nu + 4, wide, r1)

    mid = slice(U1, U1 + mu)

    def load1(i):
        line = (OMEGA / 2) * s1[0, U1 + i, V1 : V1 + mv] * restrict(r1, i, wide[1], V0 - wide[0] - 2, mv)
        slab_f[0, U1 + i] = line

    loop(mu, load1, 4)

    def slab_items(slab, b_from, steps):
        items = []
        for a in steps:
            rows, to = block_rows(a)
            items.append((slab.at[b_from, slice(U1 + rows.start, U1 + rows.stop)], slab.at[b_from, to], a, 0))
        return items

    f_v = copies([(slab_f.at[0, mid], slab_f.at[(-b) % 3, mid], 0, b) for b in (1, -1)]
                 + slab_items(slab_f, 0, (1, -1)), number(4))
    f_u = copies(slab_items(slab_f, 1, (1, -1)) + slab_items(slab_f, 2, (1, -1)), number(4))
    start(f_v)
    received(f_v[:2])
    start(f_u)
    received(f_v[2:])
    received(f_u)

    def lay_slab(slab, targets, steps):
        for a in steps:
            rows, to = block_rows(-a)
            def body():
                def one(i):
                    u = to.start + i
                    for x in targets:
                        for b in (-1, 0, 1):
                            x[0, u, V1 + b * mv : V1 + (b + 1) * mv] = slab[b % 3, u]
                loop(to.stop - to.start, one, 3)
            given(present(a), body)

    lay_slab(slab_f, (f1, x1), (0, -1, 1))

    def window1(h):
        lo = (V1 - h) // 8 * 8
        return lo, up8(V1 + mv + h) - lo

    level1 = (x1, s1, f1, d1, e1, band1)
    sweep(*level1, U1 - 8, mu + 16, window1(8))
    sweep(*level1, U1 - 6, mu + 12, window1(5))

    def own_x1(u):
        slab_x[0, U1 + u] = x1[0, U1 + u, V1 : V1 + mv]
        strip_x[0, u] = x1[0, U1 + u, V1 : V1 + 3]
        strip_x[1, u] = x1[0, U1 + u, V1 + mv - 3 : V1 + mv]

    loop(mu, own_x1, 3)
    at1 = window1(2)
    residual(*level1, down1, 4.0, U1 - 2, mu + 4, at1, r2)

    def load_2(i):
        c2[i, 0:cv] = restrict(r2, i, at1[1], V1 - at1[0] - 2, cv)

    loop(cu, load_2, 3)

    half = cu // 2
    for j in range(half):
        packed[j] = (c2[j] + pltpu.roll(c2[j + half], 64, 1))[0:cv]
        slots[me_u, 1, j] = packed[j]

    def gather(i, incoming):
        flat = lax.rem(me + 1 + i, n_all) if not incoming else lax.rem(me + n_all - 1 - i, n_all)
        u, v = place(flat)
        source_u, source_v, target_v = (u, v, me_v) if incoming else (me_u, me_v, v)
        return pltpu.make_async_remote_copy(
            src_ref=packed,
            dst_ref=slots.at[source_u, lax.rem(source_v - target_v + 1 + n_patch, n_patch)],
            send_sem=all_send.at[i],
            recv_sem=all_recv.at[i],
            device_id={"dir": u, "patch": v},
            device_id_type=MESH,
        )

    loop(n_all - 1, lambda i: gather(i, False).start())
    loop(n_all - 1, lambda i: gather(i, False).wait_send())
    loop(n_all - 1, lambda i: gather(i, True).wait_recv())

    x_v = copies([(slab_x.at[0, mid], slab_x.at[(-b) % 3, mid], 0, b) for b in (1, -1)]
                 + [(strip_x.at[1], slab_far.at[0, mid], 0, 2), (strip_x.at[0], slab_far.at[1, mid], 0, -2)], number(4))
    x_u = []
    for b in range(3):
        x_u += slab_items(slab_x, b, (1, -1, 2, -2))
    for b in range(2):
        x_u += slab_items(slab_far, b, (1, -1, 2, -2))
    x_u = copies(x_u, number(len(x_u)))

    def far_items(x, halo):
        h, near = halo.reach, halo.near
        body = slice(h, h + nu)
        first = [(halo.send_far.at[1], halo.far_v.at[0, :, body], 0, 1), (halo.send_far.at[0], halo.far_v.at[1, :, body], 0, -1)]
        top = U0 + nu
        first.append((x.at[:, top - h : top - near, V0 : V0 + nv], halo.far_u.at[0], 1, 0))
        first.append((x.at[:, U0 + near : U0 + h, V0 : V0 + nv], halo.far_u.at[1], -1, 0))
        second = []
        for k in range(2):
            second.append((halo.far_v.at[k, :, nu : nu + h], halo.far_v.at[k, :, 0:h], 1, 0))
            second.append((halo.far_v.at[k, :, h : 2 * h], halo.far_v.at[k, :, h + nu : nu + 2 * h], -1, 0))
            second.append((halo.near_v.at[k, :, nu : nu + FAR], halo.near_v.at[k, :, 0:FAR], 1, 0))
            second.append((halo.near_v.at[k, :, h + near : 2 * h], halo.near_v.at[k, :, h + nu + near : nu + 2 * h], -1, 0))
        return first, second

    xf, xs = far_items(x0, xh)
    ff, fs = far_items(f0, fh)
    far_first = copies(xf + ff, number(8))
    far_second = copies(xs + fs, number(16))
    start(x_v)
    start(far_first)

    low = lax.broadcasted_iota(jnp.int32, (cv, 128), 1) < 64
    for d in range(n_dir):
        for k in range(n_patch // 2):
            for j in range(half):
                a, b = slots[d, k, j], slots[d, k + n_patch // 2, j]
                load2[d * cu + j, k * cv : (k + 1) * cv] = jnp.where(low, a, pltpu.roll(b, 64, 1))
                load2[d * cu + half + j, k * cv : (k + 1) * cv] = jnp.where(low, pltpu.roll(a, 64, 1), b)

    def second_leg():
        received(x_v)
        start(x_u)
        received([far_first[0], far_first[1], far_first[4], far_first[5]])
        start(far_second)

    coarse_cycle((cu * n_dir, cv * n_patch // 2), load2, tables, coarse, second_leg)

    span = (tv.shape[1] - 12) // 2

    def prolong(line, first, table, x, s):
        def one(i):
            b, h, a = (line(i, first + k) for k in range(3))
            tv[i, pl.ds(6, span, stride=2), :] = 0.125 * (b + a) + 0.75 * h
            tv[i, pl.ds(7, span, stride=2), :] = 0.5 * (h + a)

        loop(24, one, 3)
        n = tv.shape[1]

        def widen(i):
            y = split_mul(tv[pl.ds(4 * i, 4)].reshape(4 * n, 128), table[...])
            for w in range(x.shape[0]):
                for j in range(4):
                    tw[w, 4 * i + j] = y[j * n : (j + 1) * n, w * 128 : (w + 1) * 128]

        loop(6, widen)

        def add(t):
            for w in range(x.shape[0]):
                p, q, r = tw[w, t], tw[w, t + 1], tw[w, t + 2]
                for j, y in enumerate((0.5 * (p + q), 0.125 * (p + r) + 0.75 * q)):
                    u = 2 * t + j
                    x[w, u] = x[w, u] + jnp.where(s[w, u] > 0.5, y, 0.0)

        loop(21, add)

    received(x_u)
    lay_slab(slab_x, (x1,), (0, -1, 1, -2, 2))
    for a in (0, -1, 1, -2, 2):
        rows, to = block_rows(-a)
        def body():
            def one(i):
                u = to.start + i
                x1[0, u, V1 - mv - 3 : V1 - mv] = slab_far[0, u]
                x1[0, u, V1 + 2 * mv : V1 + 2 * mv + 3] = slab_far[1, u]
            loop(to.stop - to.start, one, 3)
        given(present(a), body)
    x2 = coarse[0]
    edge = (x2.shape[0] - cu * n_dir) // 2
    prolong(lambda i, k: x2[edge + me_u * cu - (U1 + 1) // 2 + i, k : k + span], 5, up1, x1, s1)
    sweep(*level1, U1 - 12, mu + 24, window1(12))
    sweep(*level1, U1 - 9, mu + 18, window1(9))
    sweep(*level1, U1 - 6, mu + 12, window1(6))
    received([far_first[k] for k in (2, 3, 6, 7)])
    received(far_second)
    for x, halo in ((x0, xh), (f0, fh)):
        lay_sides(x, FAR, halo.far_v, halo.reach, halo.near)
        lay_sides(x, halo.near, halo.near_v, halo.reach)
        lay_ups(x, FAR, halo.far_u, halo.near)
    for made in (masks, f_near, x_near, f_v, f_u, x_v, x_u, far_first, far_second):
        sent(made)
    prolong(lambda i, k: x1[0, U1 - (U0 + 1) // 2 + i, k : k + span], 16, up0, x0, s0)
    level0 = (x0, s0, f0, d0, e0, band0)
    sweep(*level0, U0 - 6, nu + 12, wide)
    sweep(*level0, U0 - 3, nu + 6, wide)
    sweep(*level0, U0, nu, block0, out)
    assert taken[0] <= send_sem.shape[0]


def on_device(right_side, guess, mask_fine, mask_next):
    nu, nv, nw = right_side.shape
    n_dir, n_patch = lax.axis_size("dir"), lax.axis_size("patch")
    planes = nw // 128
    mu, mv = nu // 2, nv // 2
    cu, cv = mu // 2, mv // 2
    gu, gh = cu * n_dir, cv * n_patch // 2
    eu, eq = gu // 2, up8(gh // 4)
    rows0, cols0, rows1, cols1 = nu + 18, nv + 32, mu + 30, up8(mv + 37)
    operands = [right_side, guess, jnp.transpose(mask_fine, (0, 2, 1)), jnp.transpose(mask_next, (0, 2, 1))]
    operands += [jnp.asarray(t) for t in fine_weights(nw)]
    operands += [jnp.asarray(t) for t in coarse_weights(nw)]
    operands += [jnp.asarray(np.eye(nv, 128, dtype=np.float32))]
    operands += [jnp.asarray(spots(nv, 16, cols0, 32, 9)[:, :]), jnp.asarray(spots(mv, 22, cols1, 16, 15))]

    def vmem(*shape):
        return pltpu.VMEM(shape, jnp.float32)

    scratch = [vmem(planes, rows0, cols0, 128)] * 3 + [vmem(planes, rows0, nv + 16, 128)] * 2
    scratch += [vmem(1, rows1, cols1, 128)] * 3 + [vmem(1, rows1, cols1 - 16, 128)] * 2
    scratch += [vmem(nu + 4, nv + 16, 128), vmem(mu + 4, cols1 - 16, 128), vmem(mu, nv + 16, 128)]
    scratch += [vmem(24, cols1, 128), vmem(planes, 24, cols1, 128)]
    scratch += [vmem(SWEEPS, 2, planes, nu, 3, 128), vmem(SWEEPS, 2, planes, nu + 6, 3, 128)]
    scratch += [vmem(SWEEPS, 2, planes, 3, nv, 128)]
    scratch += Halo.scratch(planes, nu, nv, 5) + Halo.scratch(planes, nu, nv, 2)
    scratch += [vmem(3, rows0, planes, 128), vmem(5, rows1, 1, 128), vmem(3, nu, planes, 128), vmem(5, mu, 1, 128)]
    scratch += [vmem(3, rows1, mv, 128), vmem(3, rows1, mv, 128), vmem(2, mu, 3, 128), vmem(2, rows1, 3, 128)]
    scratch += [vmem(cu, up8(cv), 128), vmem(cu // 2, cv, 128), vmem(n_dir, n_patch, cu // 2, cv, 128)]
    scratch += [vmem(gu, gh, 128), vmem(gu + 20, gh + 16, 128), vmem(gu + 6, gh, 128), vmem(gu + 6, gh, 128)]
    scratch += [vmem(gu + 4, gh + 16, 128), vmem(gu, gh, 128), vmem(eu, eq + 16, 128), vmem(eu, eq, 128)]
    scratch += [vmem(eu + 6, eq, 128), vmem(eu + 6, eq, 128), vmem(eu, gh + 16, 128)]
    scratch += [pltpu.SemaphoreType.DMA((160,))] * 2 + [pltpu.SemaphoreType.DMA((n_dir * n_patch - 1,))] * 2
    space = pl.BlockSpec(memory_space=pltpu.VMEM)
    return pl.pallas_call(
        functools.partial(kernel, (n_dir, n_patch, nu, nv, planes)),
        out_shape=jax.ShapeDtypeStruct(right_side.shape, jnp.float32),
        in_specs=[space] * len(operands),
        out_specs=space,
        scratch_shapes=scratch,
        compiler_params=pltpu.CompilerParams(
            collective_id=0, has_side_effects=True, vmem_limit_bytes=60 * 2**20
        ),
        name="vcycle",
    )(*operands)


def solution(mesh):
    spec = P("dir", "patch", None)
    return jax.shard_map(
        on_device, mesh=mesh, in_specs=(spec,) * 4, out_specs=spec, check_vma=False
    )
```

```python
import functools

import jax
import jax.numpy as jnp
import numpy as np
from jax import lax
from jax.experimental import pallas as pl
from jax.experimental.pallas import tpu as pltpu
from jax.sharding import PartitionSpec as P

TILE = 128
SWEEPS = 3
LEVELS = 4
SUBDIV = (0.125, 0.5, 0.75, 0.5, 0.125)
OMEGA = 0.5
MESH = pl.DeviceIdType.MESH
AROUND = ((0, 1), (0, -1), (1, 0), (-1, 0), (1, 1), (1, -1), (-1, 1), (-1, -1))
BASIS = (2496, 1176, 96)
KAPPA = OMEGA * 42 / 5040.0**3
FAR = 4


def up8(n):
    return -(-n // 8) * 8


def band(n, size, coeffs):
    i, j = np.indices((size, size))
    out = np.zeros((size, size), np.float32)
    for k, c in enumerate(coeffs):
        out[(j - i + 3 == k) & (i < n) & (j < n)] = c
    return out


def subdivision(n, rows, columns):
    i, j = np.indices((rows, columns))
    out = np.zeros((rows, columns), np.float32)
    for k, c in enumerate(SUBDIV):
        out[(i - 2 * j + 2 == k) & (i < 2 * n) & (j < n)] = c
    return out


def coarse_weights(width):
    wide, narrow = width >> 2, width >> 3
    tables = []
    for n in (wide, narrow):
        copies = np.eye(128 // n, dtype=np.float32)
        five = band(n, n, (0, 96, 1176, 2496, 1176, 96, 0))
        stiff = band(n, n, (-1, -24, -15, 80, -15, -24, -1))
        tables.append(np.stack([np.kron(copies, five), np.kron(copies, stiff)]))
    move = subdivision(narrow, wide, narrow)
    halves = np.eye(128 // wide, dtype=np.float32)
    down = np.kron(halves, np.concatenate([move, move], axis=1))
    zero = np.zeros_like(move.T)
    even = np.kron(halves, np.concatenate([move.T, zero], axis=0))
    odd = np.kron(halves, np.concatenate([zero, move.T], axis=0))
    tables.append(np.stack([down, even, odd]))
    return [t.astype(jnp.bfloat16) for t in tables]


def parts(x):
    high = x.astype(jnp.bfloat16)
    return high, (x - high.astype(jnp.float32)).astype(jnp.bfloat16)


def mul(a, b):
    return jnp.dot(a, b, preferred_element_type=jnp.float32)


def sums(x):
    return x[3], x[2] + x[4], x[1] + x[5], x[0] + x[6]


def five_taps(s):
    return BASIS[0] * s[0] + BASIS[1] * s[1] + BASIS[2] * s[2]


def stiff_taps(s):
    return 80.0 * s[0] - 15.0 * s[1] - 24.0 * s[2] - s[3]


def first_pass(x):
    s = sums(x)
    d, e = 2 * KAPPA * s[3], 3 * KAPPA * s[3]
    for k, (p, q) in enumerate(((2336, 4752), (1206, 2397), (144, 264))):
        d, e = d + p * KAPPA * s[k], e + q * KAPPA * s[k]
    return d, e


def second_pass(d, e):
    d, e = sums(d), sums(e)
    g = five_taps(e) - (4912.0 * d[0] + 2367.0 * d[1] + 216.0 * d[2] + d[3])
    q = five_taps(d) - stiff_taps(e)
    return g, q


def split_mul(x, table):
    high, low = parts(x)
    n = x.shape[0]
    both = mul(jnp.concatenate([high, low], axis=0), table)
    return both[:n] + both[n:]


def last_pass(g, q, table):
    width = g.shape[1]
    if width < 256:
        return split_mul(jnp.concatenate([g, q], axis=1), table[...].reshape(2 * width, width))
    return split_mul(g, table[0]) + split_mul(q, table[1])


def rows_at_once(count, rows):
    best = 1
    for n in range(1, count + 1):
        if count % n == 0 and n * rows <= 240:
            best = n
    return best


def loop(count, body, unroll=1):
    while count % unroll:
        unroll -= 1
    lax.fori_loop(0, count, lambda i, _: (body(i), 0)[1], 0, unroll=unroll)


def apply_packed(x, d, e, table, at, base, rows, count, use):
    def one(u):
        d[u + 3], e[u + 3] = first_pass([x[at + u, base - 3 + k : base - 3 + k + rows, :] for k in range(7)])

    loop(count, one, 3)
    size = rows_at_once(count, rows)

    def some(i):
        u = i * size
        gs, qs = [], []
        for j in range(size):
            g, q = second_pass([d[u + j + k] for k in range(7)], [e[u + j + k] for k in range(7)])
            gs.append(g)
            qs.append(q)
        value = last_pass(jnp.concatenate(gs, axis=0), jnp.concatenate(qs, axis=0), table)
        for j in range(size):
            use(u + j, value[j * rows : (j + 1) * rows])

    loop(count // size, some)


def coarse_cycle(shape, load2, tables, refs, midway):
    nu, nh = shape
    cu, nq = nu // 2, nh // 4
    nqp = up8(nq)
    x2, d2, e2, b2, t2, x3, f3, d3, e3, z3 = refs
    edge = (x2.shape[0] - nu) // 2

    def put2(u, new):
        x2[edge + u, 8 : 8 + nh] = new
        x2[edge + u, 0:8] = pltpu.roll(new[nh - 8 : nh], 64, 1)
        x2[edge + u, 8 + nh : 16 + nh] = pltpu.roll(new[0:8], 64, 1)

    def put3(u, new):
        x3[u, 8 : 8 + nqp] = new
        left, right = pltpu.roll(new, 32, 1), pltpu.roll(new[0:8], 96, 1)
        x3[u, 5:8] = left[nq - 3 : nq]
        x3[u, 8 + nq : 11 + nq] = right[0:3]

    def smooth2():
        def use(u, value):
            put2(u, x2[edge + u, 8 : 8 + nh] + ((OMEGA / 4) * load2[u] - value))
        apply_packed(x2, d2, e2, tables[0], edge, 8, nh, nu, use)

    loop(nu, lambda u: put2(u, (OMEGA / 4) * load2[u]), 4)
    loop(SWEEPS - 1, lambda i: smooth2())

    size = rows_at_once(nu, nh)

    def keep(u, value):
        t2[u] = load2[u] - 8.0 * value

    apply_packed(x2, d2, e2, tables[0], edge, 8, nh, nu, keep)

    def narrow(i):
        at = pl.ds(i * size, size)
        n = split_mul(t2[at].reshape(size * nh, 128), tables[2][0]).reshape(size, nh, 128)
        b2[pl.ds(i * size + 2, size), 8 : 8 + nh] = n
        for j in range(size):
            b2[i * size + 2 + j, 0:8] = pltpu.roll(n[j, nh - 8 : nh], 64, 1)
            b2[i * size + 2 + j, 8 + nh : 16 + nh] = pltpu.roll(n[j, 0:8], 64, 1)

    loop(nu // size, narrow)
    lane = lax.broadcasted_iota(jnp.int32, (nq, 128), 1)
    first = lax.rem(lane // 32, 2) == 0

    def restrict(i):
        total = None
        for k in range(5):
            term = SUBDIV[k] * b2[2 * i + k]
            total = term if total is None else total + term
        z3[i] = total
        lines = []
        for start in (6, 6 + 2 * nq):
            line = None
            for m in range(5):
                term = SUBDIV[m] * z3[i, pl.ds(start + m, nq, stride=2), :]
                line = term if line is None else line + term
            lines.append(line)
        f3[i, 0:nq] = jnp.where(first, lines[0], lines[1])

    loop(cu, restrict, 4)
    loop(cu, lambda u: put3(u, (OMEGA / 8) * f3[u]), 4)

    def smooth3(i):
        def use(u, value):
            put3(u, x3[u, 8 : 8 + nqp] + ((OMEGA / 8) * f3[u] - value))
        apply_packed(x3, d3, e3, tables[1], 0, 8, nqp, cu, use)

    loop(2 * SWEEPS - 1, smooth3)

    midway()
    nf = 2 * nq
    for u in range(cu):
        b, h, a = (x3[u, 7 + s : 7 + s + nq] for s in range(3))
        b2[2 + u, pl.ds(0, nq, stride=2), :] = 0.125 * (b + a) + 0.75 * h
        b2[2 + u, pl.ds(1, nq, stride=2), :] = 0.5 * (h + a)
    fine = up8(nf)
    for u in range(cu):
        here = b2[2 + u, 0:fine]
        after = b2[3 + u, 0:fine] if u + 1 < cu else jnp.zeros_like(here)
        before = b2[1 + u, 0:fine] if u > 0 else jnp.zeros_like(here)
        t2[2 * u, 0:fine] = 0.125 * (before + after) + 0.75 * here
        t2[2 * u + 1, 0:fine] = 0.5 * (here + after)

    def widen(i):
        at = pl.ds(i * size, size)
        z = t2[at, 0:fine].reshape(size * fine, 128)
        y = (split_mul(z, tables[2][1]).reshape(size, fine, 128), split_mul(z, tables[2][2]).reshape(size, fine, 128))
        for j in range(size):
            u = edge + i * size + j
            for s in range(2):
                x2[u, 8 + s * nf : 8 + (s + 1) * nf] += y[s][j, 0:nf]
            put2(i * size + j, x2[u, 8 : 8 + nh])

    loop(nu // size, widen)
    loop(SWEEPS, lambda i: smooth2())


def fine_weights(width):
    tables = []
    for n in (width, width // 2):
        five = band(n, n, (0, 96, 1176, 2496, 1176, 96, 0))
        stiff = band(n, n, (-1, -24, -15, 80, -15, -24, -1))
        move = subdivision(n // 2, n, max(n // 2, 128))
        tables += [np.stack([five, stiff]), move, np.ascontiguousarray(move.T)]
    return [t.astype(jnp.bfloat16) for t in tables]


def spots(n, at, rows, gap, reach):
    out = np.zeros((rows, 128), np.float32)
    for p in range(at - reach, at + n + reach):
        b, v = divmod(p - at, n)
        out[p, gap * (b % (128 // gap)) + v] = 1
    return out


class Halo:
    def __init__(self, refs, near):
        self.near, self.reach = near, near + FAR
        (self.send_near, self.send_far, self.near_v, self.far_v, self.near_u, self.far_u) = refs

    @staticmethod
    def scratch(planes, nu, nv, near):
        rows = nu + 2 * (near + FAR)
        shapes = [(2, planes, nu, near, 128), (2, planes, nu, FAR, 128), (2, planes, rows, near, 128)]
        shapes += [(2, planes, rows, FAR, 128), (2, planes, near, nv, 128), (2, planes, FAR, nv, 128)]
        return [pltpu.VMEM(shape, jnp.float32) for shape in shapes]


def kernel(dims, *refs):
    n_dir, n_patch, nu, nv, planes = dims
    mu, mv = nu // 2, nv // 2
    cu, cv = mu // 2, mv // 2
    sources, out, held, refs = refs[:16], refs[16], refs[17:33], refs[33:]
    rs, guess, mask0, mask1, pick, pick0, pick1, band0, down0, up0, band1, down1, up1 = held[:13]
    tables = held[13:]
    x0, s0, f0, d0, e0, x1, s1, f1, d1, e1, r1, r2, t1, tv, tw = refs[:15]
    refs = refs[15:]
    side_send, side_recv, up_recv = refs[:3]
    xh, fh = Halo(refs[3:9], 5), Halo(refs[9:15], 2)
    lines0, lines1, line0, line1 = refs[15:19]
    slab_f, slab_x, strip_x, slab_far = refs[19:23]
    c2, packed, slots, load2 = refs[23:27]
    coarse = refs[27:37]
    send_sem, recv_sem, all_send, all_recv, load_sem = refs[37:]

    U0, V0, U1, V1 = 9, 16, mu + 3, mv + 10
    wide = (V0 - 8, nv + 16)
    me_u, me_v = lax.axis_index("dir"), lax.axis_index("patch")
    n_all = n_dir * n_patch
    me = me_u * n_patch + me_v

    def place(flat):
        return lax.div(flat, n_patch), lax.rem(flat, n_patch)

    def present(a):
        return None if a == 0 else (me_u < n_dir - a if a > 0 else me_u >= -a)

    def given(flag, body):
        body() if flag is None else pl.when(flag)(body)

    taken = [0]

    def number(count):
        taken[0] += count
        return taken[0] - count

    def copies(items, first):
        made = []
        for k, (src, dst, a, b) in enumerate(items):
            made.append((a, functools.partial(
                pltpu.make_async_remote_copy,
                src_ref=src, dst_ref=dst, send_sem=send_sem.at[first + k], recv_sem=recv_sem.at[first + k],
                device_id={"dir": me_u + a, "patch": lax.rem(me_v + b + 2 * n_patch, n_patch)},
                device_id_type=MESH)))
        return made

    def grouped(made, sign, act):
        for step in sorted({a for a, _ in made}, key=abs):
            def body():
                for a, make in made:
                    if a == step:
                        act(make())
            given(present(sign * step), body)

    def start(made):
        grouped(made, 1, lambda c: c.start())

    def sent(made):
        grouped(made, 1, lambda c: c.wait_send())

    def received(made):
        grouped(made, -1, lambda c: c.wait_recv())

    barrier = pltpu.get_barrier_semaphore()

    def greet(i):
        u, v = place(lax.rem(me + 1 + i, n_all))
        pl.semaphore_signal(barrier, inc=1, device_id={"dir": u, "patch": v}, device_id_type=MESH)

    loop(n_all - 1, greet)
    loads = [pltpu.make_async_copy(source, to, load_sem.at[k]) for k, (source, to) in enumerate(zip(sources, held))]
    for k in (1, 2, 4, 0, 3, *range(5, 16)):
        loads[k].start()


    def clear(*refs):
        for ref in refs:
            def one(u):
                ref[:, u] = jnp.zeros((ref.shape[0],) + ref.shape[2:], jnp.float32)
            loop(ref.shape[1], one, 3)

    clear(x0, s0, f0)
    for k in range(5):
        loads[k].wait()
    for k, at in enumerate((0, 32, 96)):
        line0[k] = jnp.zeros(line0.shape[1:], jnp.float32)
        line0[k, :, :, at : at + nv] = mask0[...].astype(jnp.float32)
    for k, at in enumerate((0, 16, 32, 96, 112)):
        line1[k] = jnp.zeros(line1.shape[1:], jnp.float32)
        line1[k, :, :, at : at + mv] = mask1[...].astype(jnp.float32)
    ones = jnp.ones((128, 128), jnp.bfloat16)

    def spread(pattern, line):
        return (pattern * line).astype(jnp.bfloat16)

    def own(i):
        marks = [[spread(pick[...], line0[0, i * 4 + j, w : w + 1, :]) for j in range(4)] for w in range(planes)]
        full = mul(jnp.concatenate([m for row in marks for m in row], axis=0), ones)
        for w in range(planes):
            for j in range(4):
                u, k = i * 4 + j, w * 4 + j
                m = full[k * nv : (k + 1) * nv]
                lanes = slice(w * 128, w * 128 + 128)
                x0[w, U0 + u, V0 : V0 + nv] = m * guess[u, :, lanes]
                f0[w, U0 + u, V0 : V0 + nv] = OMEGA * m * rs[u, :, lanes]
                s0[w, U0 + u, V0 : V0 + nv] = m

    loop(nu // 4, own)

    def prepare():
        clear(x1, s1, f1)
        for ref in (coarse[0], coarse[1], coarse[2], coarse[3], coarse[6], coarse[7], coarse[8], c2, tv):
            ref[...] = jnp.zeros_like(ref)
        for load in loads[5:]:
            load.wait()

    pl.semaphore_wait(barrier, n_all - 1)

    def mask_items():
        first, second = [], []
        for b in (0, 1, -1):
            for a in (0, 1, -1):
                if a or b:
                    rows = slice(0, nu) if a == 0 else (slice(nu - U0, nu) if a > 0 else slice(0, U0))
                    to = slice(U0, U0 + nu) if a == 0 else (slice(0, U0) if a > 0 else slice(U0 + nu, U0 + nu + U0))
                    first.append((line0.at[{0: 0, 1: 2, -1: 1}[b], rows], lines0.at[(-b) % 3, to], a, b))
        for b in range(-2, 3):
            for a in range(-2, 3):
                if a or b:
                    rows, to = block_rows(a)
                    second.append((line1.at[(-b) % 5, rows], lines1.at[(-b) % 5, to], a, b))
        return first + second

    def block_rows(a):
        edge = U1 - mu
        if abs(a) < 2:
            return slice(0, mu), slice(U1 - a * mu, U1 - a * mu + mu)
        return (slice(mu - edge, mu), slice(0, edge)) if a > 0 else (slice(0, edge), slice(U1 + 2 * mu, U1 + 2 * mu + edge))

    masks = copies(mask_items(), number(8 + 24))

    def expand():
        received(masks)
        for a, at, n in ((0, U0, nu), (-1, 0, U0), (1, U0 + nu, U0)):
            def body():
                def one(i):
                    u = at + 3 * i
                    marks = []
                    for w in range(planes):
                        for j in range(3):
                            line = lines0[1, u + j, w : w + 1, :] + lines0[2, u + j, w : w + 1, :]
                            if a == 0:
                                line = line + line0[0, u + j - U0, w : w + 1, :]
                            else:
                                line = line + lines0[0, u + j, w : w + 1, :]
                            marks.append(spread(pick0[...], line))
                    full = mul(jnp.concatenate(marks, axis=0), ones)
                    n0 = s0.shape[2]
                    for w in range(planes):
                        for j in range(3):
                            s0[w, u + j] = full[(w * 3 + j) * n0 : (w * 3 + j + 1) * n0]
                loop(n // 3, one)
            given(present(a), body)
        for a in (0, -1, 1, -2, 2):
            rows, to = block_rows(-a)
            def body():
                def one(i):
                    marks = []
                    for j in range(3):
                        u = to.start + 3 * i + j
                        line = line1[0, u - U1] if a == 0 else lines1[0, u]
                        for b in range(1, 5):
                            line = line + lines1[b, u]
                        marks.append(spread(pick1[...], line))
                    full = mul(jnp.concatenate(marks, axis=0), ones)
                    n1 = s1.shape[2]
                    for j in range(3):
                        s1[0, to.start + 3 * i + j] = full[j * n1 : (j + 1) * n1]
                loop((to.stop - to.start) // 3, one)
            given(present(a), body)

    def operate(x, d, e, table, u0, count, window, use):
        lo, size = window
        n = x.shape[0]

        def one(i):
            u = u0 - 3 + i
            for w in range(n):
                t = [x[w, u, lo - 3 + k : lo - 3 + k + size, :] for k in range(7)]
                d[w, u, 0:size], e[w, u, 0:size] = first_pass(t)

        loop(count + 6, one, 3)
        rows = rows_at_once(count, size)

        def some(i):
            u = u0 + i * rows
            gs, qs = [], []
            for w in range(n):
                both = [second_pass([d[w, u + j + k, 0:size] for k in range(-3, 4)], [e[w, u + j + k, 0:size] for k in range(-3, 4)])
                        for j in range(rows)]
                gs.append(jnp.concatenate([g for g, _ in both], axis=0))
                qs.append(jnp.concatenate([q for _, q in both], axis=0))
            use(u, rows, last_pass(jnp.concatenate(gs, axis=1), jnp.concatenate(qs, axis=1), table))

        loop(count // rows, some)

    def sweep(x, s, f, d, e, table, u0, count, window, result=None):
        lo, size = window

        def use(u, rows, value):
            for j in range(rows):
                for w in range(x.shape[0]):
                    v = value[j * size : (j + 1) * size, w * 128 : (w + 1) * 128]
                    at = (w, u + j, slice(lo, lo + size))
                    new = x[at] + (f[at] - s[at] * v)
                    if result is None:
                        x[at] = new
                    else:
                        result[u + j - u0, :, w * 128 : (w + 1) * 128] = new

        operate(x, d, e, table, u0, count, window, use)

    def residual(x, s, f, d, e, table, down, scale, u0, count, window, narrow):
        lo, size = window

        def use(u, rows, value):
            lines = []
            for j in range(rows):
                line = []
                for w in range(x.shape[0]):
                    v = value[j * size : (j + 1) * size, w * 128 : (w + 1) * 128]
                    at = (w, u + j, slice(lo, lo + size))
                    line.append(scale * (f[at] - s[at] * v))
                lines.append(jnp.concatenate(line, axis=1))
            n = split_mul(jnp.concatenate(lines, axis=0), down[...])
            for j in range(rows):
                narrow[u + j - u0, 0:size] = n[j * size : (j + 1) * size]

        operate(x, d, e, table, u0, count, window, use)

    def restrict(narrow, i, size, first, n):
        total = None
        for k in range(5):
            term = SUBDIV[k] * narrow[2 * i + k, 0:size]
            total = term if total is None else total + term
        t1[i, 0:size] = total
        line = None
        for m in range(5):
            term = SUBDIV[m] * t1[i, pl.ds(first + m, n, stride=2), :]
            line = term if line is None else line + term
        return line

    def near_items(x, h, strips, sides, ups):
        items = []
        top = U0 + nu
        for a, b in AROUND:
            k = 0 if b > 0 else 1
            if b == 0:
                rows = slice(top - h, top) if a > 0 else slice(U0, U0 + h)
                items.append((x.at[:, rows, V0 : V0 + nv], ups.at[0 if a > 0 else 1], a, b))
                continue
            reach = (sides.shape[-3] - nu) // 2
            rows = slice(0, nu) if a == 0 else (slice(nu - h, nu) if a > 0 else slice(0, h))
            at = reach if a == 0 else (reach - h if a > 0 else reach + nu)
            to = slice(at, at + rows.stop - rows.start)
            items.append((strips.at[1 - k, :, rows], sides.at[k, :, to], a, b))
        return items

    def stage(x, h, strips, skip=0):
        def one(u):
            for w in range(planes):
                strips[0, w, u] = x[w, U0 + u, V0 + skip : V0 + skip + h]
                strips[1, w, u] = x[w, U0 + u, V0 + nv - skip - h : V0 + nv - skip]
        loop(nu, one, 4)

    def lay_sides(x, h, sides, reach, skip=0, extra=None):
        extra = reach if extra is None else extra
        for a, at, n in ((0, U0, nu), (-1, U0 - extra, extra), (1, U0 + nu, extra)):
            def body():
                def one(i):
                    u = at + i
                    for w in range(planes):
                        x[w, u, V0 - skip - h : V0 - skip] = sides[0, w, u - U0 + reach]
                        x[w, u, V0 + nv + skip : V0 + nv + skip + h] = sides[1, w, u - U0 + reach]
                loop(n, one, 4)
            given(present(a), body)

    def lay_ups(x, h, ups, skip=0):
        def low():
            x[:, U0 - skip - h : U0 - skip, V0 : V0 + nv] = ups[0]
        def high():
            x[:, U0 + nu + skip : U0 + nu + skip + h, V0 : V0 + nv] = ups[1]
        given(present(-1), low)
        given(present(1), high)

    def far_items(x, halo):
        h, near = halo.reach, halo.near
        body = slice(h, h + nu)
        first = [(halo.send_far.at[1], halo.far_v.at[0, :, body], 0, 1), (halo.send_far.at[0], halo.far_v.at[1, :, body], 0, -1)]
        top = U0 + nu
        first.append((x.at[:, top - h : top - near, V0 : V0 + nv], halo.far_u.at[0], 1, 0))
        first.append((x.at[:, U0 + near : U0 + h, V0 : V0 + nv], halo.far_u.at[1], -1, 0))
        second = []
        for k in range(2):
            second.append((halo.far_v.at[k, :, nu : nu + h], halo.far_v.at[k, :, 0:h], 1, 0))
            second.append((halo.far_v.at[k, :, h : 2 * h], halo.far_v.at[k, :, h + nu : nu + 2 * h], -1, 0))
            second.append((halo.near_v.at[k, :, nu : nu + FAR], halo.near_v.at[k, :, 0:FAR], 1, 0))
            second.append((halo.near_v.at[k, :, h + near : 2 * h], halo.near_v.at[k, :, h + nu + near : nu + 2 * h], -1, 0))
        return first, second

    xf, xs = far_items(x0, xh)
    ff, fs = far_items(f0, fh)
    x_far, f_far = copies(xf, number(4)), copies(ff, number(4))
    far_second = copies(xs + fs, number(16))
    base = number(8 * SWEEPS)
    f_near = copies(near_items(f0, fh.near, fh.send_near, fh.near_v, fh.near_u), number(8))
    block0 = (V0, nv)

    def smooth0(i):
        stage(x0, 3, side_send.at[i])
        made = copies(near_items(x0, 3, side_send.at[i], side_recv.at[i], up_recv.at[i]), base + 8 * i)
        start(made)

        @pl.when(i == 0)
        def _():
            start(masks)
            stage(f0, fh.near, fh.send_near)
            start(f_near)
            prepare()

        pl.when(i == 1)(expand)
        received(made)
        sent(made)
        lay_sides(x0, 3, side_recv.at[i], 3)
        lay_ups(x0, 3, up_recv.at[i])
        sweep(x0, s0, f0, d0, e0, band0, U0, nu, block0)

    loop(SWEEPS, smooth0)

    stage(x0, xh.near, xh.send_near)
    x_near = copies(near_items(x0, xh.near, xh.send_near, xh.near_v, xh.near_u), number(8))
    start(x_near)
    stage(x0, FAR, xh.send_far, xh.near)
    stage(f0, FAR, fh.send_far, fh.near)
    received(f_near)
    lay_sides(f0, fh.near, fh.near_v, fh.reach, 0, fh.near)
    lay_ups(f0, fh.near, fh.near_u)
    received(x_near)
    start(f_far)
    lay_sides(x0, xh.near, xh.near_v, xh.reach, 0, xh.near)
    lay_ups(x0, xh.near, xh.near_u)
    residual(x0, s0, f0, d0, e0, band0, down0, 2.0, U0 - 2, nu + 4, wide, r1)

    mid = slice(U1, U1 + mu)

    def load1(i):
        line = (OMEGA / 2) * s1[0, U1 + i, V1 : V1 + mv] * restrict(r1, i, wide[1], V0 - wide[0] - 2, mv)
        slab_f[0, U1 + i] = line

    loop(mu, load1, 4)

    def slab_items(slab, b_from, steps):
        items = []
        for a in steps:
            rows, to = block_rows(a)
            items.append((slab.at[b_from, slice(U1 + rows.start, U1 + rows.stop)], slab.at[b_from, to], a, 0))
        return items

    f_v = copies([(slab_f.at[0, mid], slab_f.at[(-b) % 3, mid], 0, b) for b in (1, -1)]
                 + slab_items(slab_f, 0, (1, -1)), number(4))
    f_u = copies(slab_items(slab_f, 1, (1, -1)) + slab_items(slab_f, 2, (1, -1)), number(4))
    start(f_v)
    received(f_v[:2])
    start(f_u)
    received(f_v[2:])
    received(f_u)
    start(x_far)

    def lay_slab(slab, targets, steps):
        for a in steps:
            rows, to = block_rows(-a)
            def body():
                def one(i):
                    u = to.start + i
                    for x in targets:
                        for b in (-1, 0, 1):
                            x[0, u, V1 + b * mv : V1 + (b + 1) * mv] = slab[b % 3, u]
                loop(to.stop - to.start, one, 3)
            given(present(a), body)

    lay_slab(slab_f, (f1, x1), (0, -1, 1))

    def window1(h):
        lo = (V1 - h) // 8 * 8
        return lo, up8(V1 + mv + h) - lo

    level1 = (x1, s1, f1, d1, e1, band1)
    sweep(*level1, U1 - 8, mu + 16, window1(8))
    sweep(*level1, U1 - 6, mu + 12, window1(5))

    def own_x1(u):
        slab_x[0, U1 + u] = x1[0, U1 + u, V1 : V1 + mv]
        strip_x[0, u] = x1[0, U1 + u, V1 : V1 + 3]
        strip_x[1, u] = x1[0, U1 + u, V1 + mv - 3 : V1 + mv]

    loop(mu, own_x1, 3)
    at1 = window1(2)
    residual(*level1, down1, 4.0, U1 - 2, mu + 4, at1, r2)

    def load_2(i):
        c2[i, 0:cv] = restrict(r2, i, at1[1], V1 - at1[0] - 2, cv)

    loop(cu, load_2, 3)

    half = cu // 2
    for j in range(half):
        packed[j] = (c2[j] + pltpu.roll(c2[j + half], 64, 1))[0:cv]
        slots[me_u, 1, j] = packed[j]

    def gather(i, incoming):
        flat = lax.rem(me + 1 + i, n_all) if not incoming else lax.rem(me + n_all - 1 - i, n_all)
        u, v = place(flat)
        source_u, source_v, target_v = (u, v, me_v) if incoming else (me_u, me_v, v)
        return pltpu.make_async_remote_copy(
            src_ref=packed,
            dst_ref=slots.at[source_u, lax.rem(source_v - target_v + 1 + n_patch, n_patch)],
            send_sem=all_send.at[i],
            recv_sem=all_recv.at[i],
            device_id={"dir": u, "patch": v},
            device_id_type=MESH,
        )

    loop(n_all - 1, lambda i: gather(i, False).start())
    loop(n_all - 1, lambda i: gather(i, False).wait_send())
    loop(n_all - 1, lambda i: gather(i, True).wait_recv())

    x_v = copies([(slab_x.at[0, mid], slab_x.at[(-b) % 3, mid], 0, b) for b in (1, -1)]
                 + [(strip_x.at[1], slab_far.at[0, mid], 0, 2), (strip_x.at[0], slab_far.at[1, mid], 0, -2)], number(4))
    x_u = []
    for b in range(3):
        x_u += slab_items(slab_x, b, (1, -1, 2, -2))
    for b in range(2):
        x_u += slab_items(slab_far, b, (1, -1, 2, -2))
    x_u = copies(x_u, number(len(x_u)))

    start(x_v)

    low = lax.broadcasted_iota(jnp.int32, (cv, 128), 1) < 64
    for d in range(n_dir):
        for k in range(n_patch // 2):
            for j in range(half):
                a, b = slots[d, k, j], slots[d, k + n_patch // 2, j]
                load2[d * cu + j, k * cv : (k + 1) * cv] = jnp.where(low, a, pltpu.roll(b, 64, 1))
                load2[d * cu + half + j, k * cv : (k + 1) * cv] = jnp.where(low, pltpu.roll(a, 64, 1), b)

    def second_leg():
        received(x_v)
        start(x_u)
        received(x_far[:2])
        received(f_far[:2])
        start(far_second)

    coarse_cycle((cu * n_dir, cv * n_patch // 2), load2, tables, coarse, second_leg)

    span = (tv.shape[1] - 12) // 2

    def prolong(line, first, table, x, s):
        def one(i):
            b, h, a = (line(i, first + k) for k in range(3))
            tv[i, pl.ds(6, span, stride=2), :] = 0.125 * (b + a) + 0.75 * h
            tv[i, pl.ds(7, span, stride=2), :] = 0.5 * (h + a)

        loop(24, one, 3)
        n = tv.shape[1]

        def widen(i):
            y = split_mul(tv[pl.ds(4 * i, 4)].reshape(4 * n, 128), table[...])
            for w in range(x.shape[0]):
                for j in range(4):
                    tw[w, 4 * i + j] = y[j * n : (j + 1) * n, w * 128 : (w + 1) * 128]

        loop(6, widen)

        def add(t):
            for w in range(x.shape[0]):
                p, q, r = tw[w, t], tw[w, t + 1], tw[w, t + 2]
                for j, y in enumerate((0.5 * (p + q), 0.125 * (p + r) + 0.75 * q)):
                    u = 2 * t + j
                    x[w, u] = x[w, u] + jnp.where(s[w, u] > 0.5, y, 0.0)

        loop(21, add)

    received(x_u)
    lay_slab(slab_x, (x1,), (0, -1, 1, -2, 2))
    for a in (0, -1, 1, -2, 2):
        rows, to = block_rows(-a)
        def body():
            def one(i):
                u = to.start + i
                x1[0, u, V1 - mv - 3 : V1 - mv] = slab_far[0, u]
                x1[0, u, V1 + 2 * mv : V1 + 2 * mv + 3] = slab_far[1, u]
            loop(to.stop - to.start, one, 3)
        given(present(a), body)
    x2 = coarse[0]
    edge = (x2.shape[0] - cu * n_dir) // 2
    prolong(lambda i, k: x2[edge + me_u * cu - (U1 + 1) // 2 + i, k : k + span], 5, up1, x1, s1)
    sweep(*level1, U1 - 12, mu + 24, window1(12))
    sweep(*level1, U1 - 9, mu + 18, window1(9))
    sweep(*level1, U1 - 6, mu + 12, window1(6))
    received(x_far[2:])
    received(f_far[2:])
    received(far_second)
    for x, halo in ((x0, xh), (f0, fh)):
        lay_sides(x, FAR, halo.far_v, halo.reach, halo.near)
        lay_sides(x, halo.near, halo.near_v, halo.reach)
        lay_ups(x, FAR, halo.far_u, halo.near)
    for made in (masks, f_near, x_near, f_v, f_u, x_v, x_u, x_far, f_far, far_second):
        sent(made)
    prolong(lambda i, k: x1[0, U1 - (U0 + 1) // 2 + i, k : k + span], 16, up0, x0, s0)
    level0 = (x0, s0, f0, d0, e0, band0)
    sweep(*level0, U0 - 6, nu + 12, wide)
    sweep(*level0, U0 - 3, nu + 6, wide)
    sweep(*level0, U0, nu, block0, out)
    assert taken[0] <= send_sem.shape[0]


def on_device(right_side, guess, mask_fine, mask_next):
    nu, nv, nw = right_side.shape
    n_dir, n_patch = lax.axis_size("dir"), lax.axis_size("patch")
    planes = nw // 128
    mu, mv = nu // 2, nv // 2
    cu, cv = mu // 2, mv // 2
    gu, gh = cu * n_dir, cv * n_patch // 2
    eu, eq = gu // 2, up8(gh // 4)
    rows0, cols0, rows1, cols1 = nu + 18, nv + 32, mu + 30, up8(mv + 37)
    operands = [right_side, guess, jnp.transpose(mask_fine, (0, 2, 1)), jnp.transpose(mask_next, (0, 2, 1))]
    operands += [jnp.asarray(np.eye(nv, 128, dtype=np.float32))]
    operands += [jnp.asarray(spots(nv, 16, cols0, 32, 9)), jnp.asarray(spots(mv, mv + 10, cols1, 16, mu + 3))]
    operands += [jnp.asarray(t) for t in fine_weights(nw) + coarse_weights(nw)]

    def vmem(*shape):
        return pltpu.VMEM(shape, jnp.float32)

    scratch = [pltpu.VMEM(t.shape, t.dtype) for t in operands]
    scratch += [vmem(planes, rows0, cols0, 128)] * 3 + [vmem(planes, rows0, nv + 16, 128)] * 2
    scratch += [vmem(1, rows1, cols1, 128)] * 3 + [vmem(1, rows1, cols1 - 16, 128)] * 2
    scratch += [vmem(nu + 4, nv + 16, 128), vmem(mu + 4, cols1 - 16, 128), vmem(mu, nv + 16, 128)]
    scratch += [vmem(24, cols1, 128), vmem(planes, 24, cols1, 128)]
    scratch += [vmem(SWEEPS, 2, planes, nu, 3, 128), vmem(SWEEPS, 2, planes, nu + 6, 3, 128)]
    scratch += [vmem(SWEEPS, 2, planes, 3, nv, 128)]
    scratch += Halo.scratch(planes, nu, nv, 5) + Halo.scratch(planes, nu, nv, 2)
    scratch += [vmem(3, rows0, planes, 128), vmem(5, rows1, 1, 128), vmem(3, nu, planes, 128), vmem(5, mu, 1, 128)]
    scratch += [vmem(3, rows1, mv, 128), vmem(3, rows1, mv, 128), vmem(2, mu, 3, 128), vmem(2, rows1, 3, 128)]
    scratch += [vmem(cu, up8(cv), 128), vmem(cu // 2, cv, 128), vmem(n_dir, n_patch, cu // 2, cv, 128)]
    scratch += [vmem(gu, gh, 128), vmem(gu + 20, gh + 16, 128), vmem(gu + 6, gh, 128), vmem(gu + 6, gh, 128)]
    scratch += [vmem(gu + 4, gh + 16, 128), vmem(gu, gh, 128), vmem(eu, eq + 16, 128), vmem(eu, eq, 128)]
    scratch += [vmem(eu + 6, eq, 128), vmem(eu + 6, eq, 128), vmem(eu, gh + 16, 128)]
    scratch += [pltpu.SemaphoreType.DMA((160,))] * 2 + [pltpu.SemaphoreType.DMA((n_dir * n_patch - 1,))] * 2
    scratch += [pltpu.SemaphoreType.DMA((len(operands),))]
    space = pl.BlockSpec(memory_space=pltpu.MemorySpace.HBM)
    return pl.pallas_call(
        functools.partial(kernel, (n_dir, n_patch, nu, nv, planes)),
        out_shape=jax.ShapeDtypeStruct(right_side.shape, jnp.float32),
        in_specs=[space] * len(operands),
        out_specs=pl.BlockSpec(memory_space=pltpu.VMEM),
        scratch_shapes=scratch,
        compiler_params=pltpu.CompilerParams(
            collective_id=0, has_side_effects=True, vmem_limit_bytes=60 * 2**20
        ),
        name="vcycle",
    )(*operands)


def solution(mesh):
    spec = P("dir", "patch", None)
    return jax.shard_map(
        on_device, mesh=mesh, in_specs=(spec,) * 4, out_specs=spec, check_vma=False
    )
```

```python
import functools

import jax
import jax.numpy as jnp
import numpy as np
from jax import lax
from jax.experimental import pallas as pl
from jax.experimental.pallas import tpu as pltpu
from jax.sharding import PartitionSpec as P

TILE = 128
SWEEPS = 3
LEVELS = 4
SUBDIV = (0.125, 0.5, 0.75, 0.5, 0.125)
OMEGA = 0.5
MESH = pl.DeviceIdType.MESH
AROUND = ((0, 1), (0, -1), (1, 0), (-1, 0), (1, 1), (1, -1), (-1, 1), (-1, -1))
FIVE = (0, 192, 2352, 4992, 2352, 192, 0)
STIFF = (-3, -72, -45, 240, -45, -72, -3)
KAPPA = OMEGA * 42 / 5040.0**3
FAR = 4


def up8(n):
    return -(-n // 8) * 8


def band(n, size, coeffs):
    i, j = np.indices((size, size))
    out = np.zeros((size, size), np.float32)
    for k, c in enumerate(coeffs):
        out[(j - i + 3 == k) & (i < n) & (j < n)] = c
    return out


def subdivision(n, rows, columns):
    i, j = np.indices((rows, columns))
    out = np.zeros((rows, columns), np.float32)
    for k, c in enumerate(SUBDIV):
        out[(i - 2 * j + 2 == k) & (i < 2 * n) & (j < n)] = c
    return out


def coarse_weights(width):
    wide, narrow = width >> 2, width >> 3
    tables = []
    for n in (wide, narrow):
        copies = np.eye(128 // n, dtype=np.float32)
        five = band(n, n, FIVE)
        stiff = band(n, n, STIFF)
        tables.append(np.stack([np.kron(copies, five), np.kron(copies, stiff)]))
    move = subdivision(narrow, wide, narrow)
    halves = np.eye(128 // wide, dtype=np.float32)
    down = np.kron(halves, np.concatenate([move, move], axis=1))
    zero = np.zeros_like(move.T)
    even = np.kron(halves, np.concatenate([move.T, zero], axis=0))
    odd = np.kron(halves, np.concatenate([zero, move.T], axis=0))
    tables.append(np.stack([down, even, odd]))
    return [t.astype(jnp.bfloat16) for t in tables]


def parts(x):
    high = x.astype(jnp.bfloat16)
    return high, (x - high.astype(jnp.float32)).astype(jnp.bfloat16)


def mul(a, b):
    return jnp.dot(a, b, preferred_element_type=jnp.float32)


def sums(x):
    return x[3], x[2] + x[4], x[1] + x[5], x[0] + x[6]


def first_pass(x):
    s = sums(x)
    d = s[3] + 72.0 * s[2] + 603.0 * s[1] + 1168.0 * s[0]
    e = s[3] + 88.0 * s[2] + 799.0 * s[1] + 1584.0 * s[0]
    return d, e


def second_pass(d, e):
    d, e = sums(d), sums(e)
    g = (3744.0 * e[0] + 1764.0 * e[1] + 144.0 * e[2]) - (4912.0 * d[0] + 2367.0 * d[1] + 216.0 * d[2] + d[3])
    q = (1664.0 * d[0] + 784.0 * d[1] + 64.0 * d[2]) - (80.0 * e[0] - 15.0 * e[1] - 24.0 * e[2] - e[3])
    return g, q


def split_mul(x, table):
    high, low = parts(x)
    n = x.shape[0]
    both = mul(jnp.concatenate([high, low], axis=0), table)
    return both[:n] + both[n:]


def last_pass(g, q, table):
    width = g.shape[1]
    if width < 256:
        return split_mul(jnp.concatenate([g, q], axis=1), table[...].reshape(2 * width, width))
    return split_mul(g, table[0]) + split_mul(q, table[1])


def rows_at_once(count, rows):
    best = 1
    for n in range(1, count + 1):
        if count % n == 0 and n * rows <= 600:
            best = n
    return best


def loop(count, body, unroll=1):
    while count % unroll:
        unroll -= 1
    lax.fori_loop(0, count, lambda i, _: (body(i), 0)[1], 0, unroll=unroll)


def apply_packed(x, d, e, table, at, base, rows, count, use):
    def one(u):
        d[u + 3], e[u + 3] = first_pass([x[at + u, base - 3 + k : base - 3 + k + rows, :] for k in range(7)])

    loop(count, one, 8)
    size = rows_at_once(count, rows)

    def some(i):
        u = i * size
        gs, qs = [], []
        for j in range(size):
            g, q = second_pass([d[u + j + k] for k in range(7)], [e[u + j + k] for k in range(7)])
            gs.append(g)
            qs.append(q)
        value = last_pass(jnp.concatenate(gs, axis=0), jnp.concatenate(qs, axis=0), table)
        for j in range(size):
            use(u + j, value[j * rows : (j + 1) * rows])

    loop(count // size, some)


def coarse_cycle(shape, load2, tables, refs, midway):
    nu, nh = shape
    cu, nq = nu // 2, nh // 4
    nqp = up8(nq)
    x2, d2, e2, b2, t2, x3, f3, d3, e3, z3 = refs
    edge = (x2.shape[0] - nu) // 2

    def put2(u, new):
        x2[edge + u, 8 : 8 + nh] = new
        x2[edge + u, 0:8] = pltpu.roll(new[nh - 8 : nh], 64, 1)
        x2[edge + u, 8 + nh : 16 + nh] = pltpu.roll(new[0:8], 64, 1)

    def put3(u, new):
        x3[u, 8 : 8 + nqp] = new
        left, right = pltpu.roll(new, 32, 1), pltpu.roll(new[0:8], 96, 1)
        x3[u, 5:8] = left[nq - 3 : nq]
        x3[u, 8 + nq : 11 + nq] = right[0:3]

    def smooth2():
        def use(u, value):
            put2(u, x2[edge + u, 8 : 8 + nh] + ((OMEGA / 4) * load2[u] - KAPPA * value))
        apply_packed(x2, d2, e2, tables[0], edge, 8, nh, nu, use)

    loop(nu, lambda u: put2(u, (OMEGA / 4) * load2[u]), 4)
    loop(SWEEPS - 1, lambda i: smooth2())

    size = rows_at_once(nu, nh)

    def keep(u, value):
        t2[u] = load2[u] - (8 * KAPPA) * value

    apply_packed(x2, d2, e2, tables[0], edge, 8, nh, nu, keep)

    def narrow(i):
        at = pl.ds(i * size, size)
        n = split_mul(t2[at].reshape(size * nh, 128), tables[2][0]).reshape(size, nh, 128)
        b2[pl.ds(i * size + 2, size), 8 : 8 + nh] = n
        for j in range(size):
            b2[i * size + 2 + j, 0:8] = pltpu.roll(n[j, nh - 8 : nh], 64, 1)
            b2[i * size + 2 + j, 8 + nh : 16 + nh] = pltpu.roll(n[j, 0:8], 64, 1)

    loop(nu // size, narrow)
    lane = lax.broadcasted_iota(jnp.int32, (nq, 128), 1)
    first = lax.rem(lane // 32, 2) == 0

    def restrict(i):
        total = None
        for k in range(5):
            term = SUBDIV[k] * b2[2 * i + k]
            total = term if total is None else total + term
        z3[i] = total
        lines = []
        for start in (6, 6 + 2 * nq):
            line = None
            for m in range(5):
                term = SUBDIV[m] * z3[i, pl.ds(start + m, nq, stride=2), :]
                line = term if line is None else line + term
            lines.append(line)
        f3[i, 0:nq] = jnp.where(first, lines[0], lines[1])

    loop(cu, restrict, 4)
    loop(cu, lambda u: put3(u, (OMEGA / 8) * f3[u]), 4)

    def smooth3(i):
        def use(u, value):
            put3(u, x3[u, 8 : 8 + nqp] + ((OMEGA / 8) * f3[u] - KAPPA * value))
        apply_packed(x3, d3, e3, tables[1], 0, 8, nqp, cu, use)

    loop(2 * SWEEPS - 1, smooth3)

    midway()
    nf = 2 * nq
    for u in range(cu):
        b, h, a = (x3[u, 7 + s : 7 + s + nq] for s in range(3))
        b2[2 + u, pl.ds(0, nq, stride=2), :] = 0.125 * (b + a) + 0.75 * h
        b2[2 + u, pl.ds(1, nq, stride=2), :] = 0.5 * (h + a)
    fine = up8(nf)
    for u in range(cu):
        here = b2[2 + u, 0:fine]
        after = b2[3 + u, 0:fine] if u + 1 < cu else jnp.zeros_like(here)
        before = b2[1 + u, 0:fine] if u > 0 else jnp.zeros_like(here)
        t2[2 * u, 0:fine] = 0.125 * (before + after) + 0.75 * here
        t2[2 * u + 1, 0:fine] = 0.5 * (here + after)

    def widen(i):
        at = pl.ds(i * size, size)
        z = t2[at, 0:fine].reshape(size * fine, 128)
        y = (split_mul(z, tables[2][1]).reshape(size, fine, 128), split_mul(z, tables[2][2]).reshape(size, fine, 128))
        for j in range(size):
            u = edge + i * size + j
            for s in range(2):
                x2[u, 8 + s * nf : 8 + (s + 1) * nf] += y[s][j, 0:nf]
            put2(i * size + j, x2[u, 8 : 8 + nh])

    loop(nu // size, widen)
    loop(SWEEPS, lambda i: smooth2())


def fine_weights(width):
    tables = []
    for n in (width, width // 2):
        five = band(n, n, FIVE)
        stiff = band(n, n, STIFF)
        move = subdivision(n // 2, n, max(n // 2, 128))
        tables += [np.stack([five, stiff]), move, np.ascontiguousarray(move.T)]
    return [t.astype(jnp.bfloat16) for t in tables]


def spots(n, at, rows, gap, reach):
    out = np.zeros((rows, 128), np.float32)
    for p in range(at - reach, at + n + reach):
        b, v = divmod(p - at, n)
        out[p, gap * (b % (128 // gap)) + v] = 1
    return out


class Halo:
    def __init__(self, refs, near):
        self.near, self.reach = near, near + FAR
        (self.send_near, self.send_far, self.near_v, self.far_v, self.near_u, self.far_u) = refs

    @staticmethod
    def scratch(planes, nu, nv, near):
        rows = nu + 2 * (near + FAR)
        shapes = [(2, planes, nu, near, 128), (2, planes, nu, FAR, 128), (2, planes, rows, near, 128)]
        shapes += [(2, planes, rows, FAR, 128), (2, planes, near, nv, 128), (2, planes, FAR, nv, 128)]
        return [pltpu.VMEM(shape, jnp.float32) for shape in shapes]


def kernel(dims, *refs):
    n_dir, n_patch, nu, nv, planes = dims
    mu, mv = nu // 2, nv // 2
    cu, cv = mu // 2, mv // 2
    sources, out, held, refs = refs[:16], refs[16], refs[17:33], refs[33:]
    rs, guess, mask0, mask1, pick, pick0, pick1, band0, down0, up0, band1, down1, up1 = held[:13]
    tables = held[13:]
    x0, s0, f0, d0, e0, x1, s1, f1, d1, e1, r1, r2, t1, tv, tw, du, eu = refs[:17]
    refs = refs[17:]
    side_send, side_recv, up_recv = refs[:3]
    xh, fh = Halo(refs[3:9], 5), Halo(refs[9:15], 2)
    lines0, lines1, line0, line1 = refs[15:19]
    slab_f, slab_x, strip_x, slab_far = refs[19:23]
    c2, packed, slots, load2 = refs[23:27]
    coarse = refs[27:37]
    send_sem, recv_sem, all_send, all_recv, load_sem = refs[37:]

    U0, V0, U1, V1 = 9, 16, mu + 3, mv + 10
    wide = (V0 - 8, nv + 16)
    me_u, me_v = lax.axis_index("dir"), lax.axis_index("patch")
    n_all = n_dir * n_patch
    me = me_u * n_patch + me_v

    def place(flat):
        return lax.div(flat, n_patch), lax.rem(flat, n_patch)

    def present(a):
        return None if a == 0 else (me_u < n_dir - a if a > 0 else me_u >= -a)

    def given(flag, body):
        body() if flag is None else pl.when(flag)(body)

    taken = [0]

    def number(count):
        taken[0] += count
        return taken[0] - count

    def copies(items, first):
        made = []
        for k, (src, dst, a, b) in enumerate(items):
            made.append((a, functools.partial(
                pltpu.make_async_remote_copy,
                src_ref=src, dst_ref=dst, send_sem=send_sem.at[first + k], recv_sem=recv_sem.at[first + k],
                device_id={"dir": me_u + a, "patch": lax.rem(me_v + b + 2 * n_patch, n_patch)},
                device_id_type=MESH)))
        return made

    def grouped(made, sign, act):
        for step in sorted({a for a, _ in made}, key=abs):
            def body():
                for a, make in made:
                    if a == step:
                        act(make())
            given(present(sign * step), body)

    def start(made):
        grouped(made, 1, lambda c: c.start())

    def sent(made):
        grouped(made, 1, lambda c: c.wait_send())

    def received(made):
        grouped(made, -1, lambda c: c.wait_recv())

    barrier = pltpu.get_barrier_semaphore()

    def greet(i):
        u, v = place(lax.rem(me + 1 + i, n_all))
        pl.semaphore_signal(barrier, inc=1, device_id={"dir": u, "patch": v}, device_id_type=MESH)

    for flag, rows in ((me_u == 0, slice(0, 3)), (me_u == n_dir - 1, slice(nu + 3, nu + 6))):
        @pl.when(flag)
        def _():
            side_recv[:, :, :, rows] = jnp.zeros((SWEEPS, 2, planes, 3, 3, 128), jnp.float32)

    loop(n_all - 1, greet)
    loads = [pltpu.make_async_copy(source, to, load_sem.at[k]) for k, (source, to) in enumerate(zip(sources, held))]
    for k in (1, 2, 4, 0, 3, *range(5, 16)):
        loads[k].start()


    def clear(*refs):
        for ref in refs:
            def one(u):
                ref[:, u] = jnp.zeros((ref.shape[0],) + ref.shape[2:], jnp.float32)
            loop(ref.shape[1], one, 3)

    clear(x0, s0, f0)
    for k in range(5):
        loads[k].wait()
    for k, at in enumerate((0, 32, 96)):
        line0[k] = jnp.zeros(line0.shape[1:], jnp.float32)
        line0[k, :, :, at : at + nv] = mask0[...].astype(jnp.float32)
    for k, at in enumerate((0, 16, 32, 96, 112)):
        line1[k] = jnp.zeros(line1.shape[1:], jnp.float32)
        line1[k, :, :, at : at + mv] = mask1[...].astype(jnp.float32)
    ones = jnp.ones((128, 128), jnp.bfloat16)

    def spread(pattern, line):
        return (pattern * line).astype(jnp.bfloat16)

    def own(i):
        marks = [[spread(pick[...], line0[0, i * 4 + j, w : w + 1, :]) for j in range(4)] for w in range(planes)]
        full = mul(jnp.concatenate([m for row in marks for m in row], axis=0), ones)
        for w in range(planes):
            for j in range(4):
                u, k = i * 4 + j, w * 4 + j
                m = full[k * nv : (k + 1) * nv]
                lanes = slice(w * 128, w * 128 + 128)
                x0[w, U0 + u, V0 : V0 + nv] = m * guess[u, :, lanes]
                f0[w, U0 + u, V0 : V0 + nv] = OMEGA * m * rs[u, :, lanes]
                s0[w, U0 + u, V0 : V0 + nv] = KAPPA * m

    loop(nu // 4, own)

    def prepare():
        clear(x1, s1, f1)
        for ref in (coarse[0], coarse[1], coarse[2], coarse[3], coarse[6], coarse[7], coarse[8], c2, tv):
            ref[...] = jnp.zeros_like(ref)
        for load in loads[5:]:
            load.wait()

    pl.semaphore_wait(barrier, n_all - 1)

    def mask_items():
        first, second = [], []
        for b in (0, 1, -1):
            for a in (0, 1, -1):
                if a or b:
                    rows = slice(0, nu) if a == 0 else (slice(nu - U0, nu) if a > 0 else slice(0, U0))
                    to = slice(U0, U0 + nu) if a == 0 else (slice(0, U0) if a > 0 else slice(U0 + nu, U0 + nu + U0))
                    first.append((line0.at[{0: 0, 1: 2, -1: 1}[b], rows], lines0.at[(-b) % 3, to], a, b))
        for b in range(-2, 3):
            for a in range(-2, 3):
                if a or b:
                    rows, to = block_rows(a)
                    second.append((line1.at[(-b) % 5, rows], lines1.at[(-b) % 5, to], a, b))
        return first + second

    def block_rows(a):
        edge = U1 - mu
        if abs(a) < 2:
            return slice(0, mu), slice(U1 - a * mu, U1 - a * mu + mu)
        return (slice(mu - edge, mu), slice(0, edge)) if a > 0 else (slice(0, edge), slice(U1 + 2 * mu, U1 + 2 * mu + edge))

    masks = copies(mask_items(), number(8 + 24))

    def expand():
        received(masks)
        for a, at, n in ((0, U0, nu), (-1, 0, U0), (1, U0 + nu, U0)):
            def body():
                def one(i):
                    u = at + 3 * i
                    marks = []
                    for w in range(planes):
                        for j in range(3):
                            line = lines0[1, u + j, w : w + 1, :] + lines0[2, u + j, w : w + 1, :]
                            if a == 0:
                                line = line + line0[0, u + j - U0, w : w + 1, :]
                            else:
                                line = line + lines0[0, u + j, w : w + 1, :]
                            marks.append(spread(pick0[...], line))
                    full = KAPPA * mul(jnp.concatenate(marks, axis=0), ones)
                    n0 = s0.shape[2]
                    for w in range(planes):
                        for j in range(3):
                            s0[w, u + j] = full[(w * 3 + j) * n0 : (w * 3 + j + 1) * n0]
                loop(n // 3, one)
            given(present(a), body)
        for a in (0, -1, 1, -2, 2):
            rows, to = block_rows(-a)
            def body():
                def one(i):
                    marks = []
                    for j in range(3):
                        u = to.start + 3 * i + j
                        line = line1[0, u - U1] if a == 0 else lines1[0, u]
                        for b in range(1, 5):
                            line = line + lines1[b, u]
                        marks.append(spread(pick1[...], line))
                    full = KAPPA * mul(jnp.concatenate(marks, axis=0), ones)
                    n1 = s1.shape[2]
                    for j in range(3):
                        s1[0, to.start + 3 * i + j] = full[j * n1 : (j + 1) * n1]
                loop((to.stop - to.start) // 3, one)
            given(present(a), body)

    def operate(x, d, e, table, u0, count, window, use):
        lo, size = window
        n = x.shape[0]

        def one(i):
            u = u0 - 3 + i
            for w in range(n):
                t = [x[w, u, lo - 3 + k : lo - 3 + k + size, :] for k in range(7)]
                d[w, u, 0:size], e[w, u, 0:size] = first_pass(t)

        loop(count + 6, one, 6)
        rows = rows_at_once(count, size)

        def some(i):
            u = u0 + i * rows
            gs, qs = [], []
            for w in range(n):
                both = [second_pass([d[w, u + j + k, 0:size] for k in range(-3, 4)], [e[w, u + j + k, 0:size] for k in range(-3, 4)])
                        for j in range(rows)]
                gs.append(jnp.concatenate([g for g, _ in both], axis=0))
                qs.append(jnp.concatenate([q for _, q in both], axis=0))
            use(u, rows, last_pass(jnp.concatenate(gs, axis=1), jnp.concatenate(qs, axis=1), table))

        loop(count // rows, some)

    def sweep(x, s, f, d, e, table, u0, count, window, result=None):
        lo, size = window

        def use(u, rows, value):
            for j in range(rows):
                for w in range(x.shape[0]):
                    v = value[j * size : (j + 1) * size, w * 128 : (w + 1) * 128]
                    at = (w, u + j, slice(lo, lo + size))
                    new = x[at] + (f[at] - s[at] * v)
                    if result is None:
                        x[at] = new
                    else:
                        result[u + j - u0, :, w * 128 : (w + 1) * 128] = new

        operate(x, d, e, table, u0, count, window, use)

    def residual(x, s, f, d, e, table, down, scale, u0, count, window, narrow):
        lo, size = window

        def use(u, rows, value):
            lines = []
            for j in range(rows):
                line = []
                for w in range(x.shape[0]):
                    v = value[j * size : (j + 1) * size, w * 128 : (w + 1) * 128]
                    at = (w, u + j, slice(lo, lo + size))
                    line.append(scale * (f[at] - s[at] * v))
                lines.append(jnp.concatenate(line, axis=1))
            n = split_mul(jnp.concatenate(lines, axis=0), down[...])
            for j in range(rows):
                narrow[u + j - u0, 0:size] = n[j * size : (j + 1) * size]

        operate(x, d, e, table, u0, count, window, use)

    def restrict(narrow, i, size, first, n):
        total = None
        for k in range(5):
            term = SUBDIV[k] * narrow[2 * i + k, 0:size]
            total = term if total is None else total + term
        t1[i, 0:size] = total
        line = None
        for m in range(5):
            term = SUBDIV[m] * t1[i, pl.ds(first + m, n, stride=2), :]
            line = term if line is None else line + term
        return line

    def near_items(x, h, strips, sides, ups):
        items = []
        top = U0 + nu
        for a, b in AROUND:
            k = 0 if b > 0 else 1
            if b == 0:
                rows = slice(top - h, top) if a > 0 else slice(U0, U0 + h)
                items.append((x.at[:, rows, V0 : V0 + nv], ups.at[0 if a > 0 else 1], a, b))
                continue
            reach = (sides.shape[-3] - nu) // 2
            rows = slice(0, nu) if a == 0 else (slice(nu - h, nu) if a > 0 else slice(0, h))
            at = reach if a == 0 else (reach - h if a > 0 else reach + nu)
            to = slice(at, at + rows.stop - rows.start)
            items.append((strips.at[1 - k, :, rows], sides.at[k, :, to], a, b))
        return items

    def stage(x, h, strips, skip=0):
        def one(u):
            for w in range(planes):
                strips[0, w, u] = x[w, U0 + u, V0 + skip : V0 + skip + h]
                strips[1, w, u] = x[w, U0 + u, V0 + nv - skip - h : V0 + nv - skip]
        loop(nu, one, 4)

    def lay_sides(x, h, sides, reach, skip=0, extra=None):
        extra = reach if extra is None else extra
        for a, at, n in ((0, U0, nu), (-1, U0 - extra, extra), (1, U0 + nu, extra)):
            def body():
                def one(i):
                    u = at + i
                    for w in range(planes):
                        x[w, u, V0 - skip - h : V0 - skip] = sides[0, w, u - U0 + reach]
                        x[w, u, V0 + nv + skip : V0 + nv + skip + h] = sides[1, w, u - U0 + reach]
                loop(n, one, 4)
            given(present(a), body)

    def lay_ups(x, h, ups, skip=0):
        def low():
            x[:, U0 - skip - h : U0 - skip, V0 : V0 + nv] = ups[0]
        def high():
            x[:, U0 + nu + skip : U0 + nu + skip + h, V0 : V0 + nv] = ups[1]
        given(present(-1), low)
        given(present(1), high)

    def far_items(x, halo):
        h, near = halo.reach, halo.near
        body = slice(h, h + nu)
        first = [(halo.send_far.at[1], halo.far_v.at[0, :, body], 0, 1), (halo.send_far.at[0], halo.far_v.at[1, :, body], 0, -1)]
        top = U0 + nu
        first.append((x.at[:, top - h : top - near, V0 : V0 + nv], halo.far_u.at[0], 1, 0))
        first.append((x.at[:, U0 + near : U0 + h, V0 : V0 + nv], halo.far_u.at[1], -1, 0))
        second = []
        for k in range(2):
            second.append((halo.far_v.at[k, :, nu : nu + h], halo.far_v.at[k, :, 0:h], 1, 0))
            second.append((halo.far_v.at[k, :, h : 2 * h], halo.far_v.at[k, :, h + nu : nu + 2 * h], -1, 0))
            second.append((halo.near_v.at[k, :, nu : nu + FAR], halo.near_v.at[k, :, 0:FAR], 1, 0))
            second.append((halo.near_v.at[k, :, h + near : 2 * h], halo.near_v.at[k, :, h + nu + near : nu + 2 * h], -1, 0))
        return first, second

    xf, xs = far_items(x0, xh)
    ff, fs = far_items(f0, fh)
    x_far, f_far = copies(xf, number(4)), copies(ff, number(4))
    far_second = copies(xs + fs, number(16))
    def sweep_tiles(tiles, send):
        gs, qs = [], []
        for w in range(planes):
            both = [second_pass([du[w, u, 8 * t + 5 + k : 8 * t + 13 + k] for k in range(7)],
                                [eu[w, u, 8 * t + 5 + k : 8 * t + 13 + k] for k in range(7)])
                    for u in range(nu) for t in tiles]
            gs.append(jnp.concatenate([g for g, _ in both], axis=0))
            qs.append(jnp.concatenate([q for _, q in both], axis=0))
        value = last_pass(jnp.concatenate(gs, axis=1), jnp.concatenate(qs, axis=1), band0)
        for u in range(nu):
            for n, t in enumerate(tiles):
                for w in range(planes):
                    r = (u * len(tiles) + n) * 8
                    at = (w, U0 + u, slice(V0 + 8 * t, V0 + 8 * t + 8))
                    new = x0[at] + (f0[at] - s0[at] * value[r : r + 8, w * 128 : (w + 1) * 128])
                    x0[at] = new
                    if t == 0:
                        send[0, w, u] = new[0:3]
                    if t == nv // 8 - 1:
                        send[1, w, u] = new[5:8]

    base = number(8 * SWEEPS)
    f_near = copies(near_items(f0, fh.near, fh.send_near, fh.near_v, fh.near_u), number(8))
    block0 = (V0, nv)

    def smooth0(i):
        made = copies(near_items(x0, 3, side_send.at[i], side_recv.at[i], up_recv.at[i]), base + 8 * i)
        start(made)

        @pl.when(i == 0)
        def _():
            start(masks)
            stage(f0, fh.near, fh.send_near)
            start(f_near)
            prepare()

        pl.when(i == 1)(expand)
        received(made[2:4])
        lay_ups(x0, 3, up_recv.at[i])

        def own_columns(u):
            for w in range(planes):
                d, e = first_pass([x0[w, U0 + u - 3 + k, V0 : V0 + nv] for k in range(7)])
                du[w, u, 8 : 8 + nv], eu[w, u, 8 : 8 + nv] = d, e

        loop(nu, own_columns, 6)
        sent(made[2:4])
        sweep_tiles(range(1, nv // 8 - 1), side_send.at[i + 1])
        received(made[:2])
        received(made[4:])

        def side_columns(u):
            for w in range(planes):
                for s, at in ((0, 5), (1, 8 + nv)):
                    d, e = first_pass([side_recv[i, s, w, u + k] for k in range(7)])
                    du[w, u, at : at + 3], eu[w, u, at : at + 3] = d, e

        loop(nu, side_columns, 6)
        sent(made[:2])
        sent(made[4:])
        sweep_tiles((0, nv // 8 - 1), side_send.at[i + 1])

    stage(x0, 3, side_send.at[0])
    loop(SWEEPS, smooth0)

    stage(x0, xh.near, xh.send_near)
    x_near = copies(near_items(x0, xh.near, xh.send_near, xh.near_v, xh.near_u), number(8))
    start(x_near)
    stage(x0, FAR, xh.send_far, xh.near)
    stage(f0, FAR, fh.send_far, fh.near)
    received(f_near)
    lay_sides(f0, fh.near, fh.near_v, fh.reach, 0, fh.near)
    lay_ups(f0, fh.near, fh.near_u)
    received(x_near)
    start(f_far)
    lay_sides(x0, xh.near, xh.near_v, xh.reach, 0, xh.near)
    lay_ups(x0, xh.near, xh.near_u)
    residual(x0, s0, f0, d0, e0, band0, down0, 2.0, U0 - 2, nu + 4, wide, r1)

    mid = slice(U1, U1 + mu)

    def load1(i):
        line = (OMEGA / 2 / KAPPA) * s1[0, U1 + i, V1 : V1 + mv] * restrict(r1, i, wide[1], V0 - wide[0] - 2, mv)
        slab_f[0, U1 + i] = line

    loop(mu, load1, 4)

    def slab_items(slab, b_from, steps):
        items = []
        for a in steps:
            rows, to = block_rows(a)
            items.append((slab.at[b_from, slice(U1 + rows.start, U1 + rows.stop)], slab.at[b_from, to], a, 0))
        return items

    f_v = copies([(slab_f.at[0, mid], slab_f.at[(-b) % 3, mid], 0, b) for b in (1, -1)]
                 + slab_items(slab_f, 0, (1, -1)), number(4))
    f_u = copies(slab_items(slab_f, 1, (1, -1)) + slab_items(slab_f, 2, (1, -1)), number(4))
    start(f_v)
    received(f_v[:2])
    start(f_u)
    received(f_v[2:])
    received(f_u)
    start(x_far)

    def lay_slab(slab, targets, steps):
        for a in steps:
            rows, to = block_rows(-a)
            def body():
                def one(i):
                    u = to.start + i
                    for x in targets:
                        for b in (-1, 0, 1):
                            x[0, u, V1 + b * mv : V1 + (b + 1) * mv] = slab[b % 3, u]
                loop(to.stop - to.start, one, 3)
            given(present(a), body)

    lay_slab(slab_f, (f1, x1), (0, -1, 1))

    def window1(h):
        lo = (V1 - h) // 8 * 8
        return lo, up8(V1 + mv + h) - lo

    level1 = (x1, s1, f1, d1, e1, band1)
    sweep(*level1, U1 - 8, mu + 16, window1(8))
    sweep(*level1, U1 - 6, mu + 12, window1(5))

    def own_x1(u):
        slab_x[0, U1 + u] = x1[0, U1 + u, V1 : V1 + mv]
        strip_x[0, u] = x1[0, U1 + u, V1 : V1 + 3]
        strip_x[1, u] = x1[0, U1 + u, V1 + mv - 3 : V1 + mv]

    loop(mu, own_x1, 3)
    at1 = window1(2)
    residual(*level1, down1, 4.0, U1 - 2, mu + 4, at1, r2)

    def load_2(i):
        c2[i, 0:cv] = restrict(r2, i, at1[1], V1 - at1[0] - 2, cv)

    loop(cu, load_2, 3)

    half = cu // 2
    for j in range(half):
        packed[j] = (c2[j] + pltpu.roll(c2[j + half], 64, 1))[0:cv]
        slots[me_u, 1, j] = packed[j]

    def gather(i, incoming):
        flat = lax.rem(me + 1 + i, n_all) if not incoming else lax.rem(me + n_all - 1 - i, n_all)
        u, v = place(flat)
        source_u, source_v, target_v = (u, v, me_v) if incoming else (me_u, me_v, v)
        return pltpu.make_async_remote_copy(
            src_ref=packed,
            dst_ref=slots.at[source_u, lax.rem(source_v - target_v + 1 + n_patch, n_patch)],
            send_sem=all_send.at[i],
            recv_sem=all_recv.at[i],
            device_id={"dir": u, "patch": v},
            device_id_type=MESH,
        )

    loop(n_all - 1, lambda i: gather(i, False).start())
    loop(n_all - 1, lambda i: gather(i, False).wait_send())
    loop(n_all - 1, lambda i: gather(i, True).wait_recv())

    x_v = copies([(slab_x.at[0, mid], slab_x.at[(-b) % 3, mid], 0, b) for b in (1, -1)]
                 + [(strip_x.at[1], slab_far.at[0, mid], 0, 2), (strip_x.at[0], slab_far.at[1, mid], 0, -2)], number(4))
    x_u = []
    for b in range(3):
        x_u += slab_items(slab_x, b, (1, -1, 2, -2))
    for b in range(2):
        x_u += slab_items(slab_far, b, (1, -1, 2, -2))
    x_u = copies(x_u, number(len(x_u)))

    start(x_v)

    low = lax.broadcasted_iota(jnp.int32, (cv, 128), 1) < 64
    for d in range(n_dir):
        for k in range(n_patch // 2):
            for j in range(half):
                a, b = slots[d, k, j], slots[d, k + n_patch // 2, j]
                load2[d * cu + j, k * cv : (k + 1) * cv] = jnp.where(low, a, pltpu.roll(b, 64, 1))
                load2[d * cu + half + j, k * cv : (k + 1) * cv] = jnp.where(low, pltpu.roll(a, 64, 1), b)

    def second_leg():
        received(x_v)
        start(x_u)
        received(x_far[:2])
        received(f_far[:2])
        start(far_second)

    coarse_cycle((cu * n_dir, cv * n_patch // 2), load2, tables, coarse, second_leg)

    span = (tv.shape[1] - 12) // 2

    def prolong(line, first, table, x, s):
        def one(i):
            b, h, a = (line(i, first + k) for k in range(3))
            tv[i, pl.ds(6, span, stride=2), :] = 0.125 * (b + a) + 0.75 * h
            tv[i, pl.ds(7, span, stride=2), :] = 0.5 * (h + a)

        loop(24, one, 3)
        n = tv.shape[1]

        def widen(i):
            y = split_mul(tv[pl.ds(4 * i, 4)].reshape(4 * n, 128), table[...])
            for w in range(x.shape[0]):
                for j in range(4):
                    tw[w, 4 * i + j] = y[j * n : (j + 1) * n, w * 128 : (w + 1) * 128]

        loop(6, widen)

        def add(t):
            for w in range(x.shape[0]):
                p, q, r = tw[w, t], tw[w, t + 1], tw[w, t + 2]
                for j, y in enumerate((0.5 * (p + q), 0.125 * (p + r) + 0.75 * q)):
                    u = 2 * t + j
                    x[w, u] = x[w, u] + jnp.where(s[w, u] > 0.0, y, 0.0)

        loop(21, add)

    received(x_u)
    lay_slab(slab_x, (x1,), (0, -1, 1, -2, 2))
    for a in (0, -1, 1, -2, 2):
        rows, to = block_rows(-a)
        def body():
            def one(i):
                u = to.start + i
                x1[0, u, V1 - mv - 3 : V1 - mv] = slab_far[0, u]
                x1[0, u, V1 + 2 * mv : V1 + 2 * mv + 3] = slab_far[1, u]
            loop(to.stop - to.start, one, 3)
        given(present(a), body)
    x2 = coarse[0]
    edge = (x2.shape[0] - cu * n_dir) // 2
    prolong(lambda i, k: x2[edge + me_u * cu - (U1 + 1) // 2 + i, k : k + span], 5, up1, x1, s1)
    sweep(*level1, U1 - 12, mu + 24, window1(12))
    sweep(*level1, U1 - 9, mu + 18, window1(9))
    sweep(*level1, U1 - 6, mu + 12, window1(6))
    received(x_far[2:])
    received(f_far[2:])
    received(far_second)
    for x, halo in ((x0, xh), (f0, fh)):
        lay_sides(x, FAR, halo.far_v, halo.reach, halo.near)
        lay_sides(x, halo.near, halo.near_v, halo.reach)
        lay_ups(x, FAR, halo.far_u, halo.near)
    for made in (masks, f_near, x_near, f_v, f_u, x_v, x_u, x_far, f_far, far_second):
        sent(made)
    prolong(lambda i, k: x1[0, U1 - (U0 + 1) // 2 + i, k : k + span], 16, up0, x0, s0)
    level0 = (x0, s0, f0, d0, e0, band0)
    sweep(*level0, U0 - 6, nu + 12, wide)
    sweep(*level0, U0 - 3, nu + 6, wide)
    sweep(*level0, U0, nu, block0, out)
    assert taken[0] <= send_sem.shape[0]


def on_device(right_side, guess, mask_fine, mask_next):
    nu, nv, nw = right_side.shape
    n_dir, n_patch = lax.axis_size("dir"), lax.axis_size("patch")
    planes = nw // 128
    mu, mv = nu // 2, nv // 2
    cu, cv = mu // 2, mv // 2
    gu, gh = cu * n_dir, cv * n_patch // 2
    eu, eq = gu // 2, up8(gh // 4)
    rows0, cols0, rows1, cols1 = nu + 18, nv + 32, mu + 30, up8(mv + 37)
    operands = [right_side, guess, jnp.transpose(mask_fine, (0, 2, 1)), jnp.transpose(mask_next, (0, 2, 1))]
    operands += [jnp.asarray(np.eye(nv, 128, dtype=np.float32))]
    operands += [jnp.asarray(spots(nv, 16, cols0, 32, 9)), jnp.asarray(spots(mv, mv + 10, cols1, 16, mu + 3))]
    operands += [jnp.asarray(t) for t in fine_weights(nw) + coarse_weights(nw)]

    def vmem(*shape):
        return pltpu.VMEM(shape, jnp.float32)

    scratch = [pltpu.VMEM(t.shape, t.dtype) for t in operands]
    scratch += [vmem(planes, rows0, cols0, 128)] * 3 + [vmem(planes, rows0, nv + 16, 128)] * 2
    scratch += [vmem(1, rows1, cols1, 128)] * 3 + [vmem(1, rows1, cols1 - 16, 128)] * 2
    scratch += [vmem(nu + 4, nv + 16, 128), vmem(mu + 4, cols1 - 16, 128), vmem(mu, nv + 16, 128)]
    scratch += [vmem(24, cols1, 128), vmem(planes, 24, cols1, 128)] + [vmem(planes, nu, nv + 16, 128)] * 2
    scratch += [vmem(SWEEPS + 1, 2, planes, nu, 3, 128), vmem(SWEEPS, 2, planes, nu + 6, 3, 128)]
    scratch += [vmem(SWEEPS, 2, planes, 3, nv, 128)]
    scratch += Halo.scratch(planes, nu, nv, 5) + Halo.scratch(planes, nu, nv, 2)
    scratch += [vmem(3, rows0, planes, 128), vmem(5, rows1, 1, 128), vmem(3, nu, planes, 128), vmem(5, mu, 1, 128)]
    scratch += [vmem(3, rows1, mv, 128), vmem(3, rows1, mv, 128), vmem(2, mu, 3, 128), vmem(2, rows1, 3, 128)]
    scratch += [vmem(cu, up8(cv), 128), vmem(cu // 2, cv, 128), vmem(n_dir, n_patch, cu // 2, cv, 128)]
    scratch += [vmem(gu, gh, 128), vmem(gu + 20, gh + 16, 128), vmem(gu + 6, gh, 128), vmem(gu + 6, gh, 128)]
    scratch += [vmem(gu + 4, gh + 16, 128), vmem(gu, gh, 128), vmem(eu, eq + 16, 128), vmem(eu, eq, 128)]
    scratch += [vmem(eu + 6, eq, 128), vmem(eu + 6, eq, 128), vmem(eu, gh + 16, 128)]
    scratch += [pltpu.SemaphoreType.DMA((160,))] * 2 + [pltpu.SemaphoreType.DMA((n_dir * n_patch - 1,))] * 2
    scratch += [pltpu.SemaphoreType.DMA((len(operands),))]
    space = pl.BlockSpec(memory_space=pltpu.MemorySpace.HBM)
    return pl.pallas_call(
        functools.partial(kernel, (n_dir, n_patch, nu, nv, planes)),
        out_shape=jax.ShapeDtypeStruct(right_side.shape, jnp.float32),
        in_specs=[space] * len(operands),
        out_specs=pl.BlockSpec(memory_space=pltpu.VMEM),
        scratch_shapes=scratch,
        compiler_params=pltpu.CompilerParams(
            collective_id=0, has_side_effects=True, vmem_limit_bytes=60 * 2**20
        ),
        name="vcycle",
    )(*operands)


def solution(mesh):
    spec = P("dir", "patch", None)
    return jax.shard_map(
        on_device, mesh=mesh, in_specs=(spec,) * 4, out_specs=spec, check_vma=False
    )
```

```python
import functools

import jax
import jax.numpy as jnp
import numpy as np
from jax import lax
from jax.experimental import pallas as pl
from jax.experimental.pallas import tpu as pltpu
from jax.sharding import PartitionSpec as P

TILE = 128
SWEEPS = 3
LEVELS = 4
SUBDIV = (0.125, 0.5, 0.75, 0.5, 0.125)
OMEGA = 0.5
MESH = pl.DeviceIdType.MESH
AROUND = ((0, 1), (0, -1), (1, 0), (-1, 0), (1, 1), (1, -1), (-1, 1), (-1, -1))
FIVE = (0, 192, 2352, 4992, 2352, 192, 0)
STIFF = (-3, -72, -45, 240, -45, -72, -3)
KAPPA = OMEGA * 42 / 5040.0**3
FAR = 4


def up8(n):
    return -(-n // 8) * 8


def band(n, size, coeffs):
    i, j = np.indices((size, size))
    out = np.zeros((size, size), np.float32)
    for k, c in enumerate(coeffs):
        out[(j - i + 3 == k) & (i < n) & (j < n)] = c
    return out


def subdivision(n, rows, columns):
    i, j = np.indices((rows, columns))
    out = np.zeros((rows, columns), np.float32)
    for k, c in enumerate(SUBDIV):
        out[(i - 2 * j + 2 == k) & (i < 2 * n) & (j < n)] = c
    return out


def coarse_weights(width):
    wide, narrow = width >> 2, width >> 3
    tables = []
    for n in (wide, narrow):
        copies = np.eye(128 // n, dtype=np.float32)
        five = band(n, n, FIVE)
        stiff = band(n, n, STIFF)
        tables.append(np.stack([np.kron(copies, five), np.kron(copies, stiff)]))
    move = subdivision(narrow, wide, narrow)
    halves = np.eye(128 // wide, dtype=np.float32)
    down = np.kron(halves, np.concatenate([move, move], axis=1))
    zero = np.zeros_like(move.T)
    even = np.kron(halves, np.concatenate([move.T, zero], axis=0))
    odd = np.kron(halves, np.concatenate([zero, move.T], axis=0))
    tables.append(np.stack([down, even, odd]))
    return [t.astype(jnp.bfloat16) for t in tables]


def parts(x):
    high = x.astype(jnp.bfloat16)
    return high, (x - high.astype(jnp.float32)).astype(jnp.bfloat16)


def mul(a, b):
    return jnp.dot(a, b, preferred_element_type=jnp.float32)


def sums(x):
    return x[3], x[2] + x[4], x[1] + x[5], x[0] + x[6]


def first_pass(x):
    s = sums(x)
    d = s[3] + 72.0 * s[2] + 603.0 * s[1] + 1168.0 * s[0]
    e = s[3] + 88.0 * s[2] + 799.0 * s[1] + 1584.0 * s[0]
    return d, e


def second_pass(d, e):
    d, e = sums(d), sums(e)
    g = (3744.0 * e[0] + 1764.0 * e[1] + 144.0 * e[2]) - (4912.0 * d[0] + 2367.0 * d[1] + 216.0 * d[2] + d[3])
    q = (1664.0 * d[0] + 784.0 * d[1] + 64.0 * d[2]) - (80.0 * e[0] - 15.0 * e[1] - 24.0 * e[2] - e[3])
    return g, q


def split_mul(x, table):
    high, low = parts(x)
    n = x.shape[0]
    both = mul(jnp.concatenate([high, low], axis=0), table)
    return both[:n] + both[n:]


def last_pass(g, q, table):
    width = g.shape[1]
    if width < 256:
        return split_mul(jnp.concatenate([g, q], axis=1), table[...].reshape(2 * width, width))
    return split_mul(g, table[0]) + split_mul(q, table[1])


def rows_at_once(count, rows):
    best = 1
    for n in range(1, count + 1):
        if count % n == 0 and n * rows <= 600:
            best = n
    return best


def loop(count, body, unroll=1):
    while count % unroll:
        unroll -= 1
    lax.fori_loop(0, count, lambda i, _: (body(i), 0)[1], 0, unroll=unroll)


def apply_packed(x, d, e, table, at, base, rows, count, use):
    def one(u):
        d[u + 3], e[u + 3] = first_pass([x[at + u, base - 3 + k : base - 3 + k + rows, :] for k in range(7)])

    loop(count, one, 8)
    size = rows_at_once(count, rows)

    def some(i):
        u = i * size
        gs, qs = [], []
        for j in range(size):
            g, q = second_pass([d[u + j + k] for k in range(7)], [e[u + j + k] for k in range(7)])
            gs.append(g)
            qs.append(q)
        value = last_pass(jnp.concatenate(gs, axis=0), jnp.concatenate(qs, axis=0), table)
        for j in range(size):
            use(u + j, value[j * rows : (j + 1) * rows])

    loop(count // size, some)


def coarse_cycle(shape, load2, tables, refs, midway):
    nu, nh = shape
    cu, nq = nu // 2, nh // 4
    nqp = up8(nq)
    x2, d2, e2, b2, t2, x3, f3, d3, e3, z3 = refs
    edge = (x2.shape[0] - nu) // 2

    def put2(u, new):
        x2[edge + u, 8 : 8 + nh] = new
        x2[edge + u, 0:8] = pltpu.roll(new[nh - 8 : nh], 64, 1)
        x2[edge + u, 8 + nh : 16 + nh] = pltpu.roll(new[0:8], 64, 1)

    def put3(u, new):
        x3[u, 8 : 8 + nqp] = new
        left, right = pltpu.roll(new, 32, 1), pltpu.roll(new[0:8], 96, 1)
        x3[u, 5:8] = left[nq - 3 : nq]
        x3[u, 8 + nq : 11 + nq] = right[0:3]

    def smooth2():
        def use(u, value):
            put2(u, x2[edge + u, 8 : 8 + nh] + ((OMEGA / 4) * load2[u] - KAPPA * value))
        apply_packed(x2, d2, e2, tables[0], edge, 8, nh, nu, use)

    loop(nu, lambda u: put2(u, (OMEGA / 4) * load2[u]), 4)
    loop(SWEEPS - 1, lambda i: smooth2())

    size = rows_at_once(nu, nh)

    def keep(u, value):
        t2[u] = load2[u] - (8 * KAPPA) * value

    apply_packed(x2, d2, e2, tables[0], edge, 8, nh, nu, keep)

    def narrow(i):
        at = pl.ds(i * size, size)
        n = split_mul(t2[at].reshape(size * nh, 128), tables[2][0]).reshape(size, nh, 128)
        b2[pl.ds(i * size + 2, size), 8 : 8 + nh] = n
        for j in range(size):
            b2[i * size + 2 + j, 0:8] = pltpu.roll(n[j, nh - 8 : nh], 64, 1)
            b2[i * size + 2 + j, 8 + nh : 16 + nh] = pltpu.roll(n[j, 0:8], 64, 1)

    loop(nu // size, narrow)
    lane = lax.broadcasted_iota(jnp.int32, (nq, 128), 1)
    first = lax.rem(lane // 32, 2) == 0

    def restrict(i):
        total = None
        for k in range(5):
            term = SUBDIV[k] * b2[2 * i + k]
            total = term if total is None else total + term
        z3[i] = total
        lines = []
        for start in (6, 6 + 2 * nq):
            line = None
            for m in range(5):
                term = SUBDIV[m] * z3[i, pl.ds(start + m, nq, stride=2), :]
                line = term if line is None else line + term
            lines.append(line)
        f3[i, 0:nq] = jnp.where(first, lines[0], lines[1])

    loop(cu, restrict, 12)
    loop(cu, lambda u: put3(u, (OMEGA / 8) * f3[u]), 4)

    def smooth3(i):
        def use(u, value):
            put3(u, x3[u, 8 : 8 + nqp] + ((OMEGA / 8) * f3[u] - KAPPA * value))
        apply_packed(x3, d3, e3, tables[1], 0, 8, nqp, cu, use)

    loop(2 * SWEEPS - 1, smooth3)

    midway()
    nf = 2 * nq
    for u in range(cu):
        b, h, a = (x3[u, 7 + s : 7 + s + nq] for s in range(3))
        b2[2 + u, pl.ds(0, nq, stride=2), :] = 0.125 * (b + a) + 0.75 * h
        b2[2 + u, pl.ds(1, nq, stride=2), :] = 0.5 * (h + a)
    fine = up8(nf)
    for u in range(cu):
        here = b2[2 + u, 0:fine]
        after = b2[3 + u, 0:fine] if u + 1 < cu else jnp.zeros_like(here)
        before = b2[1 + u, 0:fine] if u > 0 else jnp.zeros_like(here)
        t2[2 * u, 0:fine] = 0.125 * (before + after) + 0.75 * here
        t2[2 * u + 1, 0:fine] = 0.5 * (here + after)

    def widen(i):
        at = pl.ds(i * size, size)
        z = t2[at, 0:fine].reshape(size * fine, 128)
        y = (split_mul(z, tables[2][1]).reshape(size, fine, 128), split_mul(z, tables[2][2]).reshape(size, fine, 128))
        for j in range(size):
            u = edge + i * size + j
            for s in range(2):
                x2[u, 8 + s * nf : 8 + (s + 1) * nf] += y[s][j, 0:nf]
            put2(i * size + j, x2[u, 8 : 8 + nh])

    loop(nu // size, widen)
    loop(SWEEPS, lambda i: smooth2())


def fine_weights(width):
    tables = []
    for n in (width, width // 2):
        five = band(n, n, FIVE)
        stiff = band(n, n, STIFF)
        move = subdivision(n // 2, n, max(n // 2, 128))
        tables += [np.stack([five, stiff]), move, np.ascontiguousarray(move.T)]
    return [t.astype(jnp.bfloat16) for t in tables]


def spots(n, at, rows, gap, reach):
    out = np.zeros((rows, 128), np.float32)
    for p in range(at - reach, at + n + reach):
        b, v = divmod(p - at, n)
        out[p, gap * (b % (128 // gap)) + v] = 1
    return out


class Halo:
    def __init__(self, refs, near):
        self.near, self.reach = near, near + FAR
        (self.send_near, self.send_far, self.near_v, self.far_v, self.near_u, self.far_u) = refs

    @staticmethod
    def scratch(planes, nu, nv, near):
        rows = nu + 2 * (near + FAR)
        shapes = [(2, planes, nu, near, 128), (2, planes, nu, FAR, 128), (2, planes, rows, near, 128)]
        shapes += [(2, planes, rows, FAR, 128), (2, planes, near, nv, 128), (2, planes, FAR, nv, 128)]
        return [pltpu.VMEM(shape, jnp.float32) for shape in shapes]


def kernel(dims, *refs):
    n_dir, n_patch, nu, nv, planes = dims
    mu, mv = nu // 2, nv // 2
    cu, cv = mu // 2, mv // 2
    sources, out, held, refs = refs[:16], refs[16], refs[17:33], refs[33:]
    rs, guess, mask0, mask1, pick, pick0, pick1, band0, down0, up0, band1, down1, up1 = held[:13]
    tables = held[13:]
    x0, s0, f0, d0, e0, x1, s1, f1, d1, e1, r1, r2, t1, tv, tw, du, eu = refs[:17]
    refs = refs[17:]
    side_send, side_recv, up_recv = refs[:3]
    xh, fh = Halo(refs[3:9], 5), Halo(refs[9:15], 2)
    lines0, lines1, line0, line1 = refs[15:19]
    slab_f, slab_x, strip_x, slab_far = refs[19:23]
    c2, packed, slots, load2 = refs[23:27]
    coarse = refs[27:37]
    send_sem, recv_sem, all_send, all_recv, load_sem = refs[37:]

    U0, V0, U1, V1 = 9, 16, mu + 3, mv + 10
    wide = (V0 - 8, nv + 16)
    me_u, me_v = lax.axis_index("dir"), lax.axis_index("patch")
    n_all = n_dir * n_patch
    me = me_u * n_patch + me_v

    def place(flat):
        return lax.div(flat, n_patch), lax.rem(flat, n_patch)

    def present(a):
        return None if a == 0 else (me_u < n_dir - a if a > 0 else me_u >= -a)

    def given(flag, body):
        body() if flag is None else pl.when(flag)(body)

    taken = [0]

    def number(count):
        taken[0] += count
        return taken[0] - count

    def copies(items, first):
        made = []
        for k, (src, dst, a, b) in enumerate(items):
            made.append((a, functools.partial(
                pltpu.make_async_remote_copy,
                src_ref=src, dst_ref=dst, send_sem=send_sem.at[first + k], recv_sem=recv_sem.at[first + k],
                device_id={"dir": me_u + a, "patch": lax.rem(me_v + b + 2 * n_patch, n_patch)},
                device_id_type=MESH)))
        return made

    def grouped(made, sign, act):
        for step in sorted({a for a, _ in made}, key=abs):
            def body():
                for a, make in made:
                    if a == step:
                        act(make())
            given(present(sign * step), body)

    def start(made):
        grouped(made, 1, lambda c: c.start())

    def sent(made):
        grouped(made, 1, lambda c: c.wait_send())

    def received(made):
        grouped(made, -1, lambda c: c.wait_recv())

    barrier = pltpu.get_barrier_semaphore()

    def greet(i):
        u, v = place(lax.rem(me + 1 + i, n_all))
        pl.semaphore_signal(barrier, inc=1, device_id={"dir": u, "patch": v}, device_id_type=MESH)

    for flag, rows in ((me_u == 0, slice(0, 3)), (me_u == n_dir - 1, slice(nu + 3, nu + 6))):
        @pl.when(flag)
        def _():
            side_recv[:, :, :, rows] = jnp.zeros((SWEEPS, 2, planes, 3, 3, 128), jnp.float32)

    loop(n_all - 1, greet)
    loads = [pltpu.make_async_copy(source, to, load_sem.at[k]) for k, (source, to) in enumerate(zip(sources, held))]
    for k in (1, 2, 4, 0, 3, *range(5, 16)):
        loads[k].start()


    def clear(*refs):
        for ref in refs:
            def one(u):
                ref[:, u] = jnp.zeros((ref.shape[0],) + ref.shape[2:], jnp.float32)
            loop(ref.shape[1], one, 3)

    clear(x0, s0, f0)
    for k in range(5):
        loads[k].wait()
    for k, at in enumerate((0, 32, 96)):
        line0[k] = jnp.zeros(line0.shape[1:], jnp.float32)
        line0[k, :, :, at : at + nv] = mask0[...].astype(jnp.float32)
    for k, at in enumerate((0, 16, 32, 96, 112)):
        line1[k] = jnp.zeros(line1.shape[1:], jnp.float32)
        line1[k, :, :, at : at + mv] = mask1[...].astype(jnp.float32)
    ones = jnp.ones((128, 128), jnp.bfloat16)

    def spread(pattern, line):
        return (pattern * line).astype(jnp.bfloat16)

    def own(i):
        marks = [[spread(pick[...], line0[0, i * 4 + j, w : w + 1, :]) for j in range(4)] for w in range(planes)]
        full = mul(jnp.concatenate([m for row in marks for m in row], axis=0), ones)
        for w in range(planes):
            for j in range(4):
                u, k = i * 4 + j, w * 4 + j
                m = full[k * nv : (k + 1) * nv]
                lanes = slice(w * 128, w * 128 + 128)
                x0[w, U0 + u, V0 : V0 + nv] = m * guess[u, :, lanes]
                f0[w, U0 + u, V0 : V0 + nv] = OMEGA * m * rs[u, :, lanes]
                s0[w, U0 + u, V0 : V0 + nv] = KAPPA * m

    loop(nu // 4, own)

    def prepare():
        clear(x1, s1, f1)
        for ref in (coarse[0], coarse[1], coarse[2], coarse[3], coarse[6], coarse[7], coarse[8], c2, tv):
            ref[...] = jnp.zeros_like(ref)
        for load in loads[5:]:
            load.wait()

    pl.semaphore_wait(barrier, n_all - 1)

    def mask_items():
        first, second = [], []
        for b in (0, 1, -1):
            for a in (0, 1, -1):
                if a or b:
                    rows = slice(0, nu) if a == 0 else (slice(nu - U0, nu) if a > 0 else slice(0, U0))
                    to = slice(U0, U0 + nu) if a == 0 else (slice(0, U0) if a > 0 else slice(U0 + nu, U0 + nu + U0))
                    first.append((line0.at[{0: 0, 1: 2, -1: 1}[b], rows], lines0.at[(-b) % 3, to], a, b))
        for b in range(-2, 3):
            for a in range(-2, 3):
                if a or b:
                    rows, to = block_rows(a)
                    second.append((line1.at[(-b) % 5, rows], lines1.at[(-b) % 5, to], a, b))
        return first + second

    def block_rows(a):
        edge = U1 - mu
        if abs(a) < 2:
            return slice(0, mu), slice(U1 - a * mu, U1 - a * mu + mu)
        return (slice(mu - edge, mu), slice(0, edge)) if a > 0 else (slice(0, edge), slice(U1 + 2 * mu, U1 + 2 * mu + edge))

    masks = copies(mask_items(), number(8 + 24))

    def expand():
        received(masks)
        for a, at, n in ((0, U0, nu), (-1, 0, U0), (1, U0 + nu, U0)):
            def body():
                def one(i):
                    u = at + 3 * i
                    marks = []
                    for w in range(planes):
                        for j in range(3):
                            line = lines0[1, u + j, w : w + 1, :] + lines0[2, u + j, w : w + 1, :]
                            if a == 0:
                                line = line + line0[0, u + j - U0, w : w + 1, :]
                            else:
                                line = line + lines0[0, u + j, w : w + 1, :]
                            marks.append(spread(pick0[...], line))
                    full = KAPPA * mul(jnp.concatenate(marks, axis=0), ones)
                    n0 = s0.shape[2]
                    for w in range(planes):
                        for j in range(3):
                            s0[w, u + j] = full[(w * 3 + j) * n0 : (w * 3 + j + 1) * n0]
                loop(n // 3, one)
            given(present(a), body)
        for a in (0, -1, 1, -2, 2):
            rows, to = block_rows(-a)
            def body():
                def one(i):
                    marks = []
                    for j in range(3):
                        u = to.start + 3 * i + j
                        line = line1[0, u - U1] if a == 0 else lines1[0, u]
                        for b in range(1, 5):
                            line = line + lines1[b, u]
                        marks.append(spread(pick1[...], line))
                    full = KAPPA * mul(jnp.concatenate(marks, axis=0), ones)
                    n1 = s1.shape[2]
                    for j in range(3):
                        s1[0, to.start + 3 * i + j] = full[j * n1 : (j + 1) * n1]
                loop((to.stop - to.start) // 3, one)
            given(present(a), body)

    def operate(x, d, e, table, u0, count, window, use):
        lo, size = window
        n = x.shape[0]

        def one(i):
            u = u0 - 3 + i
            for w in range(n):
                t = [x[w, u, lo - 3 + k : lo - 3 + k + size, :] for k in range(7)]
                d[w, u, 0:size], e[w, u, 0:size] = first_pass(t)

        loop(count + 6, one, 6)
        rows = rows_at_once(count, size)

        def some(i):
            u = u0 + i * rows
            gs, qs = [], []
            for w in range(n):
                both = [second_pass([d[w, u + j + k, 0:size] for k in range(-3, 4)], [e[w, u + j + k, 0:size] for k in range(-3, 4)])
                        for j in range(rows)]
                gs.append(jnp.concatenate([g for g, _ in both], axis=0))
                qs.append(jnp.concatenate([q for _, q in both], axis=0))
            use(u, rows, last_pass(jnp.concatenate(gs, axis=1), jnp.concatenate(qs, axis=1), table))

        loop(count // rows, some)

    def sweep(x, s, f, d, e, table, u0, count, window, result=None):
        lo, size = window

        def use(u, rows, value):
            for j in range(rows):
                for w in range(x.shape[0]):
                    v = value[j * size : (j + 1) * size, w * 128 : (w + 1) * 128]
                    at = (w, u + j, slice(lo, lo + size))
                    new = x[at] + (f[at] - s[at] * v)
                    if result is None:
                        x[at] = new
                    else:
                        result[u + j - u0, :, w * 128 : (w + 1) * 128] = new

        operate(x, d, e, table, u0, count, window, use)

    def residual(x, s, f, d, e, table, down, scale, u0, count, window, narrow):
        lo, size = window

        def use(u, rows, value):
            lines = []
            for j in range(rows):
                line = []
                for w in range(x.shape[0]):
                    v = value[j * size : (j + 1) * size, w * 128 : (w + 1) * 128]
                    at = (w, u + j, slice(lo, lo + size))
                    line.append(scale * (f[at] - s[at] * v))
                lines.append(jnp.concatenate(line, axis=1))
            n = split_mul(jnp.concatenate(lines, axis=0), down[...])
            for j in range(rows):
                narrow[u + j - u0, 0:size] = n[j * size : (j + 1) * size]

        operate(x, d, e, table, u0, count, window, use)

    def restrict(narrow, i, size, first, n):
        total = None
        for k in range(5):
            term = SUBDIV[k] * narrow[2 * i + k, 0:size]
            total = term if total is None else total + term
        t1[i, 0:size] = total
        line = None
        for m in range(5):
            term = SUBDIV[m] * t1[i, pl.ds(first + m, n, stride=2), :]
            line = term if line is None else line + term
        return line

    def near_items(x, h, strips, sides, ups):
        items = []
        top = U0 + nu
        for a, b in AROUND:
            k = 0 if b > 0 else 1
            if b == 0:
                rows = slice(top - h, top) if a > 0 else slice(U0, U0 + h)
                items.append((x.at[:, rows, V0 : V0 + nv], ups.at[0 if a > 0 else 1], a, b))
                continue
            reach = (sides.shape[-3] - nu) // 2
            rows = slice(0, nu) if a == 0 else (slice(nu - h, nu) if a > 0 else slice(0, h))
            at = reach if a == 0 else (reach - h if a > 0 else reach + nu)
            to = slice(at, at + rows.stop - rows.start)
            items.append((strips.at[1 - k, :, rows], sides.at[k, :, to], a, b))
        return items

    def stage(x, h, strips, skip=0):
        def one(u):
            for w in range(planes):
                strips[0, w, u] = x[w, U0 + u, V0 + skip : V0 + skip + h]
                strips[1, w, u] = x[w, U0 + u, V0 + nv - skip - h : V0 + nv - skip]
        loop(nu, one, 12)

    def lay_sides(x, h, sides, reach, skip=0, extra=None):
        extra = reach if extra is None else extra
        for a, at, n in ((0, U0, nu), (-1, U0 - extra, extra), (1, U0 + nu, extra)):
            def body():
                def one(i):
                    u = at + i
                    for w in range(planes):
                        x[w, u, V0 - skip - h : V0 - skip] = sides[0, w, u - U0 + reach]
                        x[w, u, V0 + nv + skip : V0 + nv + skip + h] = sides[1, w, u - U0 + reach]
                loop(n, one, 9)
            given(present(a), body)

    def lay_ups(x, h, ups, skip=0):
        def low():
            x[:, U0 - skip - h : U0 - skip, V0 : V0 + nv] = ups[0]
        def high():
            x[:, U0 + nu + skip : U0 + nu + skip + h, V0 : V0 + nv] = ups[1]
        given(present(-1), low)
        given(present(1), high)

    def far_items(x, halo):
        h, near = halo.reach, halo.near
        body = slice(h, h + nu)
        first = [(halo.send_far.at[1], halo.far_v.at[0, :, body], 0, 1), (halo.send_far.at[0], halo.far_v.at[1, :, body], 0, -1)]
        top = U0 + nu
        first.append((x.at[:, top - h : top - near, V0 : V0 + nv], halo.far_u.at[0], 1, 0))
        first.append((x.at[:, U0 + near : U0 + h, V0 : V0 + nv], halo.far_u.at[1], -1, 0))
        second = []
        for k in range(2):
            second.append((halo.far_v.at[k, :, nu : nu + h], halo.far_v.at[k, :, 0:h], 1, 0))
            second.append((halo.far_v.at[k, :, h : 2 * h], halo.far_v.at[k, :, h + nu : nu + 2 * h], -1, 0))
            second.append((halo.near_v.at[k, :, nu : nu + FAR], halo.near_v.at[k, :, 0:FAR], 1, 0))
            second.append((halo.near_v.at[k, :, h + near : 2 * h], halo.near_v.at[k, :, h + nu + near : nu + 2 * h], -1, 0))
        return first, second

    xf, xs = far_items(x0, xh)
    ff, fs = far_items(f0, fh)
    x_far, f_far = copies(xf, number(4)), copies(ff, number(4))
    far_second = copies(xs + fs, number(16))
    def sweep_tiles(tiles, send):
        gs, qs = [], []
        for w in range(planes):
            both = [second_pass([du[w, u, 8 * t + 5 + k : 8 * t + 13 + k] for k in range(7)],
                                [eu[w, u, 8 * t + 5 + k : 8 * t + 13 + k] for k in range(7)])
                    for u in range(nu) for t in tiles]
            gs.append(jnp.concatenate([g for g, _ in both], axis=0))
            qs.append(jnp.concatenate([q for _, q in both], axis=0))
        value = last_pass(jnp.concatenate(gs, axis=1), jnp.concatenate(qs, axis=1), band0)
        for u in range(nu):
            for n, t in enumerate(tiles):
                for w in range(planes):
                    r = (u * len(tiles) + n) * 8
                    at = (w, U0 + u, slice(V0 + 8 * t, V0 + 8 * t + 8))
                    new = x0[at] + (f0[at] - s0[at] * value[r : r + 8, w * 128 : (w + 1) * 128])
                    x0[at] = new
                    if t == 0:
                        send[0, w, u] = new[0:3]
                    if t == nv // 8 - 1:
                        send[1, w, u] = new[5:8]

    base = number(8 * SWEEPS)
    f_near = copies(near_items(f0, fh.near, fh.send_near, fh.near_v, fh.near_u), number(8))
    block0 = (V0, nv)

    def smooth0(i):
        made = copies(near_items(x0, 3, side_send.at[i], side_recv.at[i], up_recv.at[i]), base + 8 * i)
        start(made)

        @pl.when(i == 0)
        def _():
            start(masks)
            stage(f0, fh.near, fh.send_near)
            start(f_near)
            prepare()

        pl.when(i == 1)(expand)
        received(made[2:4])
        lay_ups(x0, 3, up_recv.at[i])

        def own_columns(u):
            for w in range(planes):
                d, e = first_pass([x0[w, U0 + u - 3 + k, V0 : V0 + nv] for k in range(7)])
                du[w, u, 8 : 8 + nv], eu[w, u, 8 : 8 + nv] = d, e

        loop(nu, own_columns, 12)
        sent(made[2:4])
        sweep_tiles(range(1, nv // 8 - 1), side_send.at[i + 1])
        received(made[:2])
        received(made[4:])

        def side_columns(u):
            for w in range(planes):
                for s, at in ((0, 5), (1, 8 + nv)):
                    d, e = first_pass([side_recv[i, s, w, u + k] for k in range(7)])
                    du[w, u, at : at + 3], eu[w, u, at : at + 3] = d, e

        loop(nu, side_columns, 12)
        sent(made[:2])
        sent(made[4:])
        sweep_tiles((0, nv // 8 - 1), side_send.at[i + 1])

    stage(x0, 3, side_send.at[0])
    loop(SWEEPS, smooth0)

    stage(x0, xh.near, xh.send_near)
    x_near = copies(near_items(x0, xh.near, xh.send_near, xh.near_v, xh.near_u), number(8))
    start(x_near)
    stage(x0, FAR, xh.send_far, xh.near)
    stage(f0, FAR, fh.send_far, fh.near)
    received(f_near)
    lay_sides(f0, fh.near, fh.near_v, fh.reach, 0, fh.near)
    lay_ups(f0, fh.near, fh.near_u)
    received(x_near)
    start(f_far)
    lay_sides(x0, xh.near, xh.near_v, xh.reach, 0, xh.near)
    lay_ups(x0, xh.near, xh.near_u)
    residual(x0, s0, f0, d0, e0, band0, down0, 2.0, U0 - 2, nu + 4, wide, r1)

    mid = slice(U1, U1 + mu)

    def load1(i):
        line = (OMEGA / 2 / KAPPA) * s1[0, U1 + i, V1 : V1 + mv] * restrict(r1, i, wide[1], V0 - wide[0] - 2, mv)
        slab_f[0, U1 + i] = line

    loop(mu, load1, 12)

    def slab_items(slab, b_from, steps):
        items = []
        for a in steps:
            rows, to = block_rows(a)
            items.append((slab.at[b_from, slice(U1 + rows.start, U1 + rows.stop)], slab.at[b_from, to], a, 0))
        return items

    f_v = copies([(slab_f.at[0, mid], slab_f.at[(-b) % 3, mid], 0, b) for b in (1, -1)]
                 + slab_items(slab_f, 0, (1, -1)), number(4))
    f_u = copies(slab_items(slab_f, 1, (1, -1)) + slab_items(slab_f, 2, (1, -1)), number(4))
    start(f_v)
    received(f_v[:2])
    start(f_u)
    received(f_v[2:])
    received(f_u)
    start(x_far)

    def lay_slab(slab, targets, steps):
        for a in steps:
            rows, to = block_rows(-a)
            def body():
                def one(i):
                    u = to.start + i
                    for x in targets:
                        for b in (-1, 0, 1):
                            x[0, u, V1 + b * mv : V1 + (b + 1) * mv] = slab[b % 3, u]
                loop(to.stop - to.start, one, 6)
            given(present(a), body)

    lay_slab(slab_f, (f1, x1), (0, -1, 1))

    def window1(h):
        lo = (V1 - h) // 8 * 8
        return lo, up8(V1 + mv + h) - lo

    level1 = (x1, s1, f1, d1, e1, band1)
    sweep(*level1, U1 - 8, mu + 16, window1(8))
    sweep(*level1, U1 - 6, mu + 12, window1(5))

    def own_x1(u):
        slab_x[0, U1 + u] = x1[0, U1 + u, V1 : V1 + mv]
        strip_x[0, u] = x1[0, U1 + u, V1 : V1 + 3]
        strip_x[1, u] = x1[0, U1 + u, V1 + mv - 3 : V1 + mv]

    loop(mu, own_x1, 12)
    at1 = window1(2)
    residual(*level1, down1, 4.0, U1 - 2, mu + 4, at1, r2)

    def load_2(i):
        c2[i, 0:cv] = restrict(r2, i, at1[1], V1 - at1[0] - 2, cv)

    loop(cu, load_2, 6)

    half = cu // 2
    for j in range(half):
        packed[j] = (c2[j] + pltpu.roll(c2[j + half], 64, 1))[0:cv]
        slots[me_u, 1, j] = packed[j]

    def gather(i, incoming):
        flat = lax.rem(me + 1 + i, n_all) if not incoming else lax.rem(me + n_all - 1 - i, n_all)
        u, v = place(flat)
        source_u, source_v, target_v = (u, v, me_v) if incoming else (me_u, me_v, v)
        return pltpu.make_async_remote_copy(
            src_ref=packed,
            dst_ref=slots.at[source_u, lax.rem(source_v - target_v + 1 + n_patch, n_patch)],
            send_sem=all_send.at[i],
            recv_sem=all_recv.at[i],
            device_id={"dir": u, "patch": v},
            device_id_type=MESH,
        )

    loop(n_all - 1, lambda i: gather(i, False).start())
    loop(n_all - 1, lambda i: gather(i, False).wait_send())
    loop(n_all - 1, lambda i: gather(i, True).wait_recv())

    x_v = copies([(slab_x.at[0, mid], slab_x.at[(-b) % 3, mid], 0, b) for b in (1, -1)]
                 + [(strip_x.at[1], slab_far.at[0, mid], 0, 2), (strip_x.at[0], slab_far.at[1, mid], 0, -2)], number(4))
    x_u = []
    for b in range(3):
        x_u += slab_items(slab_x, b, (1, -1, 2, -2))
    for b in range(2):
        x_u += slab_items(slab_far, b, (1, -1, 2, -2))
    x_u = copies(x_u, number(len(x_u)))

    start(x_v)

    low = lax.broadcasted_iota(jnp.int32, (cv, 128), 1) < 64
    for d in range(n_dir):
        for k in range(n_patch // 2):
            for j in range(half):
                a, b = slots[d, k, j], slots[d, k + n_patch // 2, j]
                load2[d * cu + j, k * cv : (k + 1) * cv] = jnp.where(low, a, pltpu.roll(b, 64, 1))
                load2[d * cu + half + j, k * cv : (k + 1) * cv] = jnp.where(low, pltpu.roll(a, 64, 1), b)

    def second_leg():
        received(x_v)
        start(x_u)
        received(x_far[:2])
        received(f_far[:2])
        start(far_second)

    coarse_cycle((cu * n_dir, cv * n_patch // 2), load2, tables, coarse, second_leg)

    span = (tv.shape[1] - 12) // 2

    def prolong(line, first, table, x, s):
        def one(i):
            b, h, a = (line(i, first + k) for k in range(3))
            tv[i, pl.ds(6, span, stride=2), :] = 0.125 * (b + a) + 0.75 * h
            tv[i, pl.ds(7, span, stride=2), :] = 0.5 * (h + a)

        loop(24, one, 8)
        n = tv.shape[1]

        def widen(i):
            y = split_mul(tv[pl.ds(8 * i, 8)].reshape(8 * n, 128), table[...])
            for w in range(x.shape[0]):
                for j in range(8):
                    tw[w, 8 * i + j] = y[j * n : (j + 1) * n, w * 128 : (w + 1) * 128]

        loop(3, widen)

        def add(t):
            for w in range(x.shape[0]):
                p, q, r = tw[w, t], tw[w, t + 1], tw[w, t + 2]
                for j, y in enumerate((0.5 * (p + q), 0.125 * (p + r) + 0.75 * q)):
                    u = 2 * t + j
                    x[w, u] = x[w, u] + jnp.where(s[w, u] > 0.0, y, 0.0)

        loop(21, add, 3)

    received(x_u)
    lay_slab(slab_x, (x1,), (0, -1, 1, -2, 2))
    for a in (0, -1, 1, -2, 2):
        rows, to = block_rows(-a)
        def body():
            def one(i):
                u = to.start + i
                x1[0, u, V1 - mv - 3 : V1 - mv] = slab_far[0, u]
                x1[0, u, V1 + 2 * mv : V1 + 2 * mv + 3] = slab_far[1, u]
            loop(to.stop - to.start, one, 3)
        given(present(a), body)
    x2 = coarse[0]
    edge = (x2.shape[0] - cu * n_dir) // 2
    prolong(lambda i, k: x2[edge + me_u * cu - (U1 + 1) // 2 + i, k : k + span], 5, up1, x1, s1)
    sweep(*level1, U1 - 12, mu + 24, window1(12))
    sweep(*level1, U1 - 9, mu + 18, window1(9))
    sweep(*level1, U1 - 6, mu + 12, window1(6))
    received(x_far[2:])
    received(f_far[2:])
    received(far_second)
    for x, halo in ((x0, xh), (f0, fh)):
        lay_sides(x, FAR, halo.far_v, halo.reach, halo.near)
        lay_sides(x, halo.near, halo.near_v, halo.reach)
        lay_ups(x, FAR, halo.far_u, halo.near)
    for made in (masks, f_near, x_near, f_v, f_u, x_v, x_u, x_far, f_far, far_second):
        sent(made)
    prolong(lambda i, k: x1[0, U1 - (U0 + 1) // 2 + i, k : k + span], 16, up0, x0, s0)
    level0 = (x0, s0, f0, d0, e0, band0)
    sweep(*level0, U0 - 6, nu + 12, wide)
    sweep(*level0, U0 - 3, nu + 6, wide)
    sweep(*level0, U0, nu, block0, out)
    assert taken[0] <= send_sem.shape[0]


def on_device(right_side, guess, mask_fine, mask_next):
    nu, nv, nw = right_side.shape
    n_dir, n_patch = lax.axis_size("dir"), lax.axis_size("patch")
    planes = nw // 128
    mu, mv = nu // 2, nv // 2
    cu, cv = mu // 2, mv // 2
    gu, gh = cu * n_dir, cv * n_patch // 2
    eu, eq = gu // 2, up8(gh // 4)
    rows0, cols0, rows1, cols1 = nu + 18, nv + 32, mu + 30, up8(mv + 37)
    operands = [right_side, guess, jnp.transpose(mask_fine, (0, 2, 1)), jnp.transpose(mask_next, (0, 2, 1))]
    operands += [jnp.asarray(np.eye(nv, 128, dtype=np.float32))]
    operands += [jnp.asarray(spots(nv, 16, cols0, 32, 9)), jnp.asarray(spots(mv, mv + 10, cols1, 16, mu + 3))]
    operands += [jnp.asarray(t) for t in fine_weights(nw) + coarse_weights(nw)]

    def vmem(*shape):
        return pltpu.VMEM(shape, jnp.float32)

    scratch = [pltpu.VMEM(t.shape, t.dtype) for t in operands]
    scratch += [vmem(planes, rows0, cols0, 128)] * 3 + [vmem(planes, rows0, nv + 16, 128)] * 2
    scratch += [vmem(1, rows1, cols1, 128)] * 3 + [vmem(1, rows1, cols1 - 16, 128)] * 2
    scratch += [vmem(nu + 4, nv + 16, 128), vmem(mu + 4, cols1 - 16, 128), vmem(mu, nv + 16, 128)]
    scratch += [vmem(24, cols1, 128), vmem(planes, 24, cols1, 128)] + [vmem(planes, nu, nv + 16, 128)] * 2
    scratch += [vmem(SWEEPS + 1, 2, planes, nu, 3, 128), vmem(SWEEPS, 2, planes, nu + 6, 3, 128)]
    scratch += [vmem(SWEEPS, 2, planes, 3, nv, 128)]
    scratch += Halo.scratch(planes, nu, nv, 5) + Halo.scratch(planes, nu, nv, 2)
    scratch += [vmem(3, rows0, planes, 128), vmem(5, rows1, 1, 128), vmem(3, nu, planes, 128), vmem(5, mu, 1, 128)]
    scratch += [vmem(3, rows1, mv, 128), vmem(3, rows1, mv, 128), vmem(2, mu, 3, 128), vmem(2, rows1, 3, 128)]
    scratch += [vmem(cu, up8(cv), 128), vmem(cu // 2, cv, 128), vmem(n_dir, n_patch, cu // 2, cv, 128)]
    scratch += [vmem(gu, gh, 128), vmem(gu + 20, gh + 16, 128), vmem(gu + 6, gh, 128), vmem(gu + 6, gh, 128)]
    scratch += [vmem(gu + 4, gh + 16, 128), vmem(gu, gh, 128), vmem(eu, eq + 16, 128), vmem(eu, eq, 128)]
    scratch += [vmem(eu + 6, eq, 128), vmem(eu + 6, eq, 128), vmem(eu, gh + 16, 128)]
    scratch += [pltpu.SemaphoreType.DMA((160,))] * 2 + [pltpu.SemaphoreType.DMA((n_dir * n_patch - 1,))] * 2
    scratch += [pltpu.SemaphoreType.DMA((len(operands),))]
    space = pl.BlockSpec(memory_space=pltpu.MemorySpace.HBM)
    return pl.pallas_call(
        functools.partial(kernel, (n_dir, n_patch, nu, nv, planes)),
        out_shape=jax.ShapeDtypeStruct(right_side.shape, jnp.float32),
        in_specs=[space] * len(operands),
        out_specs=pl.BlockSpec(memory_space=pltpu.VMEM),
        scratch_shapes=scratch,
        compiler_params=pltpu.CompilerParams(
            collective_id=0, has_side_effects=True, vmem_limit_bytes=60 * 2**20
        ),
        name="vcycle",
    )(*operands)


def solution(mesh):
    spec = P("dir", "patch", None)
    return jax.shard_map(
        on_device, mesh=mesh, in_specs=(spec,) * 4, out_specs=spec, check_vma=False
    )
```

```python
import functools

import jax
import jax.numpy as jnp
import numpy as np
from jax import lax
from jax.experimental import pallas as pl
from jax.experimental.pallas import tpu as pltpu
from jax.sharding import PartitionSpec as P

TILE = 128
SWEEPS = 3
LEVELS = 4
SUBDIV = (0.125, 0.5, 0.75, 0.5, 0.125)
OMEGA = 0.5
MESH = pl.DeviceIdType.MESH
AROUND = ((0, 1), (0, -1), (1, 0), (-1, 0), (1, 1), (1, -1), (-1, 1), (-1, -1))
FIVE = (0, 192, 2352, 4992, 2352, 192, 0)
STIFF = (-3, -72, -45, 240, -45, -72, -3)
KAPPA = OMEGA * 42 / 5040.0**3
FAR = 4


def up8(n):
    return -(-n // 8) * 8


def band(n, size, coeffs):
    i, j = np.indices((size, size))
    out = np.zeros((size, size), np.float32)
    for k, c in enumerate(coeffs):
        out[(j - i + 3 == k) & (i < n) & (j < n)] = c
    return out


def subdivision(n, rows, columns):
    i, j = np.indices((rows, columns))
    out = np.zeros((rows, columns), np.float32)
    for k, c in enumerate(SUBDIV):
        out[(i - 2 * j + 2 == k) & (i < 2 * n) & (j < n)] = c
    return out


def coarse_weights(width):
    wide, narrow = width >> 2, width >> 3
    tables = []
    for n in (wide, narrow):
        copies = np.eye(128 // n, dtype=np.float32)
        five = band(n, n, FIVE)
        stiff = band(n, n, STIFF)
        tables.append(np.stack([np.kron(copies, five), np.kron(copies, stiff)]))
    move = subdivision(narrow, wide, narrow)
    halves = np.eye(128 // wide, dtype=np.float32)
    down = np.kron(halves, np.concatenate([move, move], axis=1))
    zero = np.zeros_like(move.T)
    even = np.kron(halves, np.concatenate([move.T, zero], axis=0))
    odd = np.kron(halves, np.concatenate([zero, move.T], axis=0))
    tables.append(np.stack([down, even, odd]))
    return [t.astype(jnp.bfloat16) for t in tables]


def parts(x):
    high = x.astype(jnp.bfloat16)
    return high, (x - high.astype(jnp.float32)).astype(jnp.bfloat16)


def mul(a, b):
    return jnp.dot(a, b, preferred_element_type=jnp.float32)


def sums(x):
    return x[3], x[2] + x[4], x[1] + x[5], x[0] + x[6]


def first_pass(x):
    s = sums(x)
    d = s[3] + 72.0 * s[2] + 603.0 * s[1] + 1168.0 * s[0]
    e = s[3] + 88.0 * s[2] + 799.0 * s[1] + 1584.0 * s[0]
    return d, e


def second_pass(d, e):
    d, e = sums(d), sums(e)
    g = (3744.0 * e[0] + 1764.0 * e[1] + 144.0 * e[2]) - (4912.0 * d[0] + 2367.0 * d[1] + 216.0 * d[2] + d[3])
    q = (1664.0 * d[0] + 784.0 * d[1] + 64.0 * d[2]) - (80.0 * e[0] - 15.0 * e[1] - 24.0 * e[2] - e[3])
    return g, q


def split_mul(x, table):
    high, low = parts(x)
    n = x.shape[0]
    both = mul(jnp.concatenate([high, low], axis=0), table)
    return both[:n] + both[n:]


def last_pass(g, q, table):
    width = g.shape[1]
    if width < 256:
        return split_mul(jnp.concatenate([g, q], axis=1), table[...].reshape(2 * width, width))
    return split_mul(g, table[0]) + split_mul(q, table[1])


def rows_at_once(count, rows):
    best = 1
    for n in range(1, count + 1):
        if count % n == 0 and n * rows <= 600:
            best = n
    return best


def loop(count, body, unroll=1):
    while count % unroll:
        unroll -= 1
    lax.fori_loop(0, count, lambda i, _: (body(i), 0)[1], 0, unroll=unroll)


def apply_packed(x, d, e, table, at, base, rows, count, use):
    def one(u):
        d[u + 3], e[u + 3] = first_pass([x[at + u, base - 3 + k : base - 3 + k + rows, :] for k in range(7)])

    loop(count, one, 12)
    size = rows_at_once(count, rows)

    def some(i):
        u = i * size
        gs, qs = [], []
        for j in range(size):
            g, q = second_pass([d[u + j + k] for k in range(7)], [e[u + j + k] for k in range(7)])
            gs.append(g)
            qs.append(q)
        value = last_pass(jnp.concatenate(gs, axis=0), jnp.concatenate(qs, axis=0), table)
        for j in range(size):
            use(u + j, value[j * rows : (j + 1) * rows])

    loop(count // size, some)


def coarse_cycle(shape, load2, tables, refs, midway):
    nu, nh = shape
    cu, nq = nu // 2, nh // 4
    nqp = up8(nq)
    x2, d2, e2, b2, t2, x3, f3, d3, e3, z3 = refs
    edge = (x2.shape[0] - nu) // 2

    def put2(u, new):
        x2[edge + u, 8 : 8 + nh] = new
        x2[edge + u, 0:8] = pltpu.roll(new[nh - 8 : nh], 64, 1)
        x2[edge + u, 8 + nh : 16 + nh] = pltpu.roll(new[0:8], 64, 1)

    def put3(u, new):
        x3[u, 8 : 8 + nqp] = new
        left, right = pltpu.roll(new, 32, 1), pltpu.roll(new[0:8], 96, 1)
        x3[u, 5:8] = left[nq - 3 : nq]
        x3[u, 8 + nq : 11 + nq] = right[0:3]

    def smooth2():
        def use(u, value):
            put2(u, x2[edge + u, 8 : 8 + nh] + ((OMEGA / 4) * load2[u] - KAPPA * value))
        apply_packed(x2, d2, e2, tables[0], edge, 8, nh, nu, use)

    loop(nu, lambda u: put2(u, (OMEGA / 4) * load2[u]), 4)
    loop(SWEEPS - 1, lambda i: smooth2())

    size = rows_at_once(nu, nh)

    def keep(u, value):
        t2[u] = load2[u] - (8 * KAPPA) * value

    apply_packed(x2, d2, e2, tables[0], edge, 8, nh, nu, keep)

    def narrow(i):
        at = pl.ds(i * size, size)
        n = split_mul(t2[at].reshape(size * nh, 128), tables[2][0]).reshape(size, nh, 128)
        b2[pl.ds(i * size + 2, size), 8 : 8 + nh] = n
        for j in range(size):
            b2[i * size + 2 + j, 0:8] = pltpu.roll(n[j, nh - 8 : nh], 64, 1)
            b2[i * size + 2 + j, 8 + nh : 16 + nh] = pltpu.roll(n[j, 0:8], 64, 1)

    loop(nu // size, narrow)
    lane = lax.broadcasted_iota(jnp.int32, (nq, 128), 1)
    first = lax.rem(lane // 32, 2) == 0

    def restrict(i):
        total = None
        for k in range(5):
            term = SUBDIV[k] * b2[2 * i + k]
            total = term if total is None else total + term
        z3[i] = total
        lines = []
        for start in (6, 6 + 2 * nq):
            line = None
            for m in range(5):
                term = SUBDIV[m] * z3[i, pl.ds(start + m, nq, stride=2), :]
                line = term if line is None else line + term
            lines.append(line)
        f3[i, 0:nq] = jnp.where(first, lines[0], lines[1])

    loop(cu, restrict, 12)
    loop(cu, lambda u: put3(u, (OMEGA / 8) * f3[u]), 4)

    def smooth3(i):
        def use(u, value):
            put3(u, x3[u, 8 : 8 + nqp] + ((OMEGA / 8) * f3[u] - KAPPA * value))
        apply_packed(x3, d3, e3, tables[1], 0, 8, nqp, cu, use)

    loop(2 * SWEEPS - 1, smooth3)

    midway()
    nf = 2 * nq
    for u in range(cu):
        b, h, a = (x3[u, 7 + s : 7 + s + nq] for s in range(3))
        b2[2 + u, pl.ds(0, nq, stride=2), :] = 0.125 * (b + a) + 0.75 * h
        b2[2 + u, pl.ds(1, nq, stride=2), :] = 0.5 * (h + a)
    fine = up8(nf)
    for u in range(cu):
        here = b2[2 + u, 0:fine]
        after = b2[3 + u, 0:fine] if u + 1 < cu else jnp.zeros_like(here)
        before = b2[1 + u, 0:fine] if u > 0 else jnp.zeros_like(here)
        t2[2 * u, 0:fine] = 0.125 * (before + after) + 0.75 * here
        t2[2 * u + 1, 0:fine] = 0.5 * (here + after)

    def widen(i):
        at = pl.ds(i * size, size)
        z = t2[at, 0:fine].reshape(size * fine, 128)
        y = (split_mul(z, tables[2][1]).reshape(size, fine, 128), split_mul(z, tables[2][2]).reshape(size, fine, 128))
        for j in range(size):
            u = edge + i * size + j
            for s in range(2):
                x2[u, 8 + s * nf : 8 + (s + 1) * nf] += y[s][j, 0:nf]
            put2(i * size + j, x2[u, 8 : 8 + nh])

    loop(nu // size, widen)
    loop(SWEEPS, lambda i: smooth2())


def fine_weights(width):
    tables = []
    for n in (width, width // 2):
        five = band(n, n, FIVE)
        stiff = band(n, n, STIFF)
        move = subdivision(n // 2, n, max(n // 2, 128))
        tables += [np.stack([five, stiff]), move, np.ascontiguousarray(move.T)]
    return [t.astype(jnp.bfloat16) for t in tables]


def spots(n, at, rows, gap, reach):
    out = np.zeros((rows, 128), np.float32)
    for p in range(at - reach, at + n + reach):
        b, v = divmod(p - at, n)
        out[p, gap * (b % (128 // gap)) + v] = 1
    return out


class Halo:
    def __init__(self, refs, near):
        self.near, self.reach = near, near + FAR
        (self.send_near, self.send_far, self.near_v, self.far_v, self.near_u, self.far_u) = refs

    @staticmethod
    def scratch(planes, nu, nv, near):
        rows = nu + 2 * (near + FAR)
        shapes = [(2, planes, nu, near, 128), (2, planes, nu, FAR, 128), (2, planes, rows, near, 128)]
        shapes += [(2, planes, rows, FAR, 128), (2, planes, near, nv, 128), (2, planes, FAR, nv, 128)]
        return [pltpu.VMEM(shape, jnp.float32) for shape in shapes]


def kernel(dims, *refs):
    n_dir, n_patch, nu, nv, planes = dims
    mu, mv = nu // 2, nv // 2
    cu, cv = mu // 2, mv // 2
    sources, out, held, refs = refs[:16], refs[16], refs[17:33], refs[33:]
    rs, guess, mask0, mask1, pick, pick0, pick1, band0, down0, up0, band1, down1, up1 = held[:13]
    tables = held[13:]
    x0, s0, f0, d0, e0, x1, s1, f1, d1, e1, r1, r2, t1, tv, tw, du, eu = refs[:17]
    refs = refs[17:]
    side_send, side_recv, up_recv = refs[:3]
    xh, fh = Halo(refs[3:9], 5), Halo(refs[9:15], 2)
    lines0, lines1, line0, line1 = refs[15:19]
    slab_f, slab_x, strip_x, slab_far = refs[19:23]
    c2, packed, slots, load2 = refs[23:27]
    coarse = refs[27:37]
    send_sem, recv_sem, all_send, all_recv, load_sem = refs[37:]

    U0, V0, U1, V1 = 9, 16, mu + 3, mv + 10
    wide = (V0 - 8, nv + 16)
    me_u, me_v = lax.axis_index("dir"), lax.axis_index("patch")
    n_all = n_dir * n_patch
    me = me_u * n_patch + me_v

    def place(flat):
        return lax.div(flat, n_patch), lax.rem(flat, n_patch)

    def present(a):
        return None if a == 0 else (me_u < n_dir - a if a > 0 else me_u >= -a)

    def given(flag, body):
        body() if flag is None else pl.when(flag)(body)

    taken = [0]

    def number(count):
        taken[0] += count
        return taken[0] - count

    def copies(items, first):
        made = []
        for k, (src, dst, a, b) in enumerate(items):
            made.append((a, functools.partial(
                pltpu.make_async_remote_copy,
                src_ref=src, dst_ref=dst, send_sem=send_sem.at[first + k], recv_sem=recv_sem.at[first + k],
                device_id={"dir": me_u + a, "patch": lax.rem(me_v + b + 2 * n_patch, n_patch)},
                device_id_type=MESH)))
        return made

    def grouped(made, sign, act):
        for step in sorted({a for a, _ in made}, key=abs):
            def body():
                for a, make in made:
                    if a == step:
                        act(make())
            given(present(sign * step), body)

    def start(made):
        grouped(made, 1, lambda c: c.start())

    def sent(made):
        grouped(made, 1, lambda c: c.wait_send())

    def received(made):
        grouped(made, -1, lambda c: c.wait_recv())

    barrier = pltpu.get_barrier_semaphore()

    def greet(i):
        u, v = place(lax.rem(me + 1 + i, n_all))
        pl.semaphore_signal(barrier, inc=1, device_id={"dir": u, "patch": v}, device_id_type=MESH)

    for flag, rows in ((me_u == 0, slice(0, 3)), (me_u == n_dir - 1, slice(nu + 3, nu + 6))):
        @pl.when(flag)
        def _():
            side_recv[:, :, :, rows] = jnp.zeros((SWEEPS, 2, planes, 3, 3, 128), jnp.float32)

    loop(n_all - 1, greet)
    loads = [pltpu.make_async_copy(source, to, load_sem.at[k]) for k, (source, to) in enumerate(zip(sources, held))]
    for k in (1, 2, 4, 0, 3, *range(5, 16)):
        loads[k].start()


    def clear(*refs):
        for ref in refs:
            def one(u):
                ref[:, u] = jnp.zeros((ref.shape[0],) + ref.shape[2:], jnp.float32)
            loop(ref.shape[1], one, 3)

    clear(x0, s0, f0)
    for k in range(5):
        loads[k].wait()
    for k, at in enumerate((0, 32, 96)):
        line0[k] = jnp.zeros(line0.shape[1:], jnp.float32)
        line0[k, :, :, at : at + nv] = mask0[...].astype(jnp.float32)
    for k, at in enumerate((0, 16, 32, 96, 112)):
        line1[k] = jnp.zeros(line1.shape[1:], jnp.float32)
        line1[k, :, :, at : at + mv] = mask1[...].astype(jnp.float32)
    ones = jnp.ones((128, 128), jnp.bfloat16)

    def spread(pattern, line):
        return (pattern * line).astype(jnp.bfloat16)

    def own(i):
        marks = [[spread(pick[...], line0[0, i * 4 + j, w : w + 1, :]) for j in range(4)] for w in range(planes)]
        full = mul(jnp.concatenate([m for row in marks for m in row], axis=0), ones)
        for w in range(planes):
            for j in range(4):
                u, k = i * 4 + j, w * 4 + j
                m = full[k * nv : (k + 1) * nv]
                lanes = slice(w * 128, w * 128 + 128)
                x0[w, U0 + u, V0 : V0 + nv] = m * guess[u, :, lanes]
                f0[w, U0 + u, V0 : V0 + nv] = OMEGA * m * rs[u, :, lanes]
                s0[w, U0 + u, V0 : V0 + nv] = KAPPA * m

    loop(nu // 4, own)

    def prepare():
        clear(x1, s1, f1)
        for ref in (coarse[0], coarse[1], coarse[2], coarse[3], coarse[6], coarse[7], coarse[8], c2, tv):
            ref[...] = jnp.zeros_like(ref)
        for load in loads[5:]:
            load.wait()

    pl.semaphore_wait(barrier, n_all - 1)

    def mask_items():
        first, second = [], []
        for b in (0, 1, -1):
            for a in (0, 1, -1):
                if a or b:
                    rows = slice(0, nu) if a == 0 else (slice(nu - U0, nu) if a > 0 else slice(0, U0))
                    to = slice(U0, U0 + nu) if a == 0 else (slice(0, U0) if a > 0 else slice(U0 + nu, U0 + nu + U0))
                    first.append((line0.at[{0: 0, 1: 2, -1: 1}[b], rows], lines0.at[(-b) % 3, to], a, b))
        for b in range(-2, 3):
            for a in range(-2, 3):
                if a or b:
                    rows, to = block_rows(a)
                    second.append((line1.at[(-b) % 5, rows], lines1.at[(-b) % 5, to], a, b))
        return first + second

    def block_rows(a):
        edge = U1 - mu
        if abs(a) < 2:
            return slice(0, mu), slice(U1 - a * mu, U1 - a * mu + mu)
        return (slice(mu - edge, mu), slice(0, edge)) if a > 0 else (slice(0, edge), slice(U1 + 2 * mu, U1 + 2 * mu + edge))

    masks = copies(mask_items(), number(8 + 24))

    def expand():
        received(masks)
        for a, at, n in ((0, U0, nu), (-1, 0, U0), (1, U0 + nu, U0)):
            def body():
                def one(i):
                    u = at + 3 * i
                    marks = []
                    for w in range(planes):
                        for j in range(3):
                            line = lines0[1, u + j, w : w + 1, :] + lines0[2, u + j, w : w + 1, :]
                            if a == 0:
                                line = line + line0[0, u + j - U0, w : w + 1, :]
                            else:
                                line = line + lines0[0, u + j, w : w + 1, :]
                            marks.append(spread(pick0[...], line))
                    full = KAPPA * mul(jnp.concatenate(marks, axis=0), ones)
                    n0 = s0.shape[2]
                    for w in range(planes):
                        for j in range(3):
                            s0[w, u + j] = full[(w * 3 + j) * n0 : (w * 3 + j + 1) * n0]
                loop(n // 3, one)
            given(present(a), body)
        for a in (0, -1, 1, -2, 2):
            rows, to = block_rows(-a)
            def body():
                def one(i):
                    marks = []
                    for j in range(3):
                        u = to.start + 3 * i + j
                        line = line1[0, u - U1] if a == 0 else lines1[0, u]
                        for b in range(1, 5):
                            line = line + lines1[b, u]
                        marks.append(spread(pick1[...], line))
                    full = KAPPA * mul(jnp.concatenate(marks, axis=0), ones)
                    n1 = s1.shape[2]
                    for j in range(3):
                        s1[0, to.start + 3 * i + j] = full[j * n1 : (j + 1) * n1]
                loop((to.stop - to.start) // 3, one)
            given(present(a), body)

    def operate(x, d, e, table, u0, count, window, use):
        lo, size = window
        n = x.shape[0]

        def one(i):
            u = u0 - 3 + i
            for w in range(n):
                t = [x[w, u, lo - 3 + k : lo - 3 + k + size, :] for k in range(7)]
                d[w, u, 0:size], e[w, u, 0:size] = first_pass(t)

        loop(count + 6, one, 12)
        rows = rows_at_once(count, size)

        def some(i):
            u = u0 + i * rows
            gs, qs = [], []
            for w in range(n):
                both = [second_pass([d[w, u + j + k, 0:size] for k in range(-3, 4)], [e[w, u + j + k, 0:size] for k in range(-3, 4)])
                        for j in range(rows)]
                gs.append(jnp.concatenate([g for g, _ in both], axis=0))
                qs.append(jnp.concatenate([q for _, q in both], axis=0))
            use(u, rows, last_pass(jnp.concatenate(gs, axis=1), jnp.concatenate(qs, axis=1), table))

        loop(count // rows, some)

    def sweep(x, s, f, d, e, table, u0, count, window, result=None):
        lo, size = window

        def use(u, rows, value):
            for j in range(rows):
                for w in range(x.shape[0]):
                    v = value[j * size : (j + 1) * size, w * 128 : (w + 1) * 128]
                    at = (w, u + j, slice(lo, lo + size))
                    new = x[at] + (f[at] - s[at] * v)
                    if result is None:
                        x[at] = new
                    else:
                        result[u + j - u0, :, w * 128 : (w + 1) * 128] = new

        operate(x, d, e, table, u0, count, window, use)

    def residual(x, s, f, d, e, table, down, scale, u0, count, window, narrow):
        lo, size = window

        def use(u, rows, value):
            lines = []
            for j in range(rows):
                line = []
                for w in range(x.shape[0]):
                    v = value[j * size : (j + 1) * size, w * 128 : (w + 1) * 128]
                    at = (w, u + j, slice(lo, lo + size))
                    line.append(scale * (f[at] - s[at] * v))
                lines.append(jnp.concatenate(line, axis=1))
            n = split_mul(jnp.concatenate(lines, axis=0), down[...])
            for j in range(rows):
                narrow[u + j - u0, 0:size] = n[j * size : (j + 1) * size]

        operate(x, d, e, table, u0, count, window, use)

    def restrict(narrow, i, size, first, n):
        total = None
        for k in range(5):
            term = SUBDIV[k] * narrow[2 * i + k, 0:size]
            total = term if total is None else total + term
        t1[i, 0:size] = total
        line = None
        for m in range(5):
            term = SUBDIV[m] * t1[i, pl.ds(first + m, n, stride=2), :]
            line = term if line is None else line + term
        return line

    def near_items(x, h, strips, sides, ups):
        items = []
        top = U0 + nu
        for a, b in AROUND:
            k = 0 if b > 0 else 1
            if b == 0:
                rows = slice(top - h, top) if a > 0 else slice(U0, U0 + h)
                items.append((x.at[:, rows, V0 : V0 + nv], ups.at[0 if a > 0 else 1], a, b))
                continue
            reach = (sides.shape[-3] - nu) // 2
            rows = slice(0, nu) if a == 0 else (slice(nu - h, nu) if a > 0 else slice(0, h))
            at = reach if a == 0 else (reach - h if a > 0 else reach + nu)
            to = slice(at, at + rows.stop - rows.start)
            items.append((strips.at[1 - k, :, rows], sides.at[k, :, to], a, b))
        return items

    def stage(x, h, strips, skip=0):
        def one(u):
            for w in range(planes):
                strips[0, w, u] = x[w, U0 + u, V0 + skip : V0 + skip + h]
                strips[1, w, u] = x[w, U0 + u, V0 + nv - skip - h : V0 + nv - skip]
        loop(nu, one, 12)

    def lay_sides(x, h, sides, reach, skip=0, extra=None):
        extra = reach if extra is None else extra
        for a, at, n in ((0, U0, nu), (-1, U0 - extra, extra), (1, U0 + nu, extra)):
            def body():
                def one(i):
                    u = at + i
                    for w in range(planes):
                        x[w, u, V0 - skip - h : V0 - skip] = sides[0, w, u - U0 + reach]
                        x[w, u, V0 + nv + skip : V0 + nv + skip + h] = sides[1, w, u - U0 + reach]
                loop(n, one, 9)
            given(present(a), body)

    def lay_ups(x, h, ups, skip=0):
        def low():
            x[:, U0 - skip - h : U0 - skip, V0 : V0 + nv] = ups[0]
        def high():
            x[:, U0 + nu + skip : U0 + nu + skip + h, V0 : V0 + nv] = ups[1]
        given(present(-1), low)
        given(present(1), high)

    def far_items(x, halo):
        h, near = halo.reach, halo.near
        body = slice(h, h + nu)
        first = [(halo.send_far.at[1], halo.far_v.at[0, :, body], 0, 1), (halo.send_far.at[0], halo.far_v.at[1, :, body], 0, -1)]
        top = U0 + nu
        first.append((x.at[:, top - h : top - near, V0 : V0 + nv], halo.far_u.at[0], 1, 0))
        first.append((x.at[:, U0 + near : U0 + h, V0 : V0 + nv], halo.far_u.at[1], -1, 0))
        second = []
        for k in range(2):
            second.append((halo.far_v.at[k, :, nu : nu + h], halo.far_v.at[k, :, 0:h], 1, 0))
            second.append((halo.far_v.at[k, :, h : 2 * h], halo.far_v.at[k, :, h + nu : nu + 2 * h], -1, 0))
            second.append((halo.near_v.at[k, :, nu : nu + FAR], halo.near_v.at[k, :, 0:FAR], 1, 0))
            second.append((halo.near_v.at[k, :, h + near : 2 * h], halo.near_v.at[k, :, h + nu + near : nu + 2 * h], -1, 0))
        return first, second

    xf, xs = far_items(x0, xh)
    ff, fs = far_items(f0, fh)
    x_far, f_far = copies(xf, number(4)), copies(ff, number(4))
    far_second = copies(xs + fs, number(16))
    def sweep_tiles(tiles, send):
        gs, qs = [], []
        for w in range(planes):
            both = [second_pass([du[w, u, 8 * t + 5 + k : 8 * t + 13 + k] for k in range(7)],
                                [eu[w, u, 8 * t + 5 + k : 8 * t + 13 + k] for k in range(7)])
                    for u in range(nu) for t in tiles]
            gs.append(jnp.concatenate([g for g, _ in both], axis=0))
            qs.append(jnp.concatenate([q for _, q in both], axis=0))
        value = last_pass(jnp.concatenate(gs, axis=1), jnp.concatenate(qs, axis=1), band0)
        for u in range(nu):
            for n, t in enumerate(tiles):
                for w in range(planes):
                    r = (u * len(tiles) + n) * 8
                    at = (w, U0 + u, slice(V0 + 8 * t, V0 + 8 * t + 8))
                    new = x0[at] + (f0[at] - s0[at] * value[r : r + 8, w * 128 : (w + 1) * 128])
                    x0[at] = new
                    if t == 0:
                        send[0, w, u] = new[0:3]
                    if t == nv // 8 - 1:
                        send[1, w, u] = new[5:8]

    base = number(8 * SWEEPS)
    f_near = copies(near_items(f0, fh.near, fh.send_near, fh.near_v, fh.near_u), number(8))
    block0 = (V0, nv)

    def smooth0(i):
        made = copies(near_items(x0, 3, side_send.at[i], side_recv.at[i], up_recv.at[i]), base + 8 * i)
        start(made)

        @pl.when(i == 0)
        def _():
            start(masks)
            stage(f0, fh.near, fh.send_near)
            start(f_near)
            prepare()

        pl.when(i == 1)(expand)
        received(made[2:4])
        lay_ups(x0, 3, up_recv.at[i])

        def own_columns(u):
            for w in range(planes):
                d, e = first_pass([x0[w, U0 + u - 3 + k, V0 : V0 + nv] for k in range(7)])
                du[w, u, 8 : 8 + nv], eu[w, u, 8 : 8 + nv] = d, e

        loop(nu, own_columns, 12)
        sent(made[2:4])
        sweep_tiles(range(1, nv // 8 - 1), side_send.at[i + 1])
        received(made[:2])
        received(made[4:])

        def side_columns(u):
            for w in range(planes):
                for s, at in ((0, 5), (1, 8 + nv)):
                    d, e = first_pass([side_recv[i, s, w, u + k] for k in range(7)])
                    du[w, u, at : at + 3], eu[w, u, at : at + 3] = d, e

        loop(nu, side_columns, 12)
        sent(made[:2])
        sent(made[4:])
        sweep_tiles((0, nv // 8 - 1), side_send.at[i + 1])

    stage(x0, 3, side_send.at[0])
    loop(SWEEPS, smooth0)

    stage(x0, xh.near, xh.send_near)
    x_near = copies(near_items(x0, xh.near, xh.send_near, xh.near_v, xh.near_u), number(8))
    start(x_near)
    stage(x0, FAR, xh.send_far, xh.near)
    stage(f0, FAR, fh.send_far, fh.near)
    received(f_near)
    lay_sides(f0, fh.near, fh.near_v, fh.reach, 0, fh.near)
    lay_ups(f0, fh.near, fh.near_u)
    received(x_near)
    start(f_far)
    lay_sides(x0, xh.near, xh.near_v, xh.reach, 0, xh.near)
    lay_ups(x0, xh.near, xh.near_u)
    residual(x0, s0, f0, d0, e0, band0, down0, 2.0, U0 - 2, nu + 4, wide, r1)

    mid = slice(U1, U1 + mu)

    def load1(i):
        line = (OMEGA / 2 / KAPPA) * s1[0, U1 + i, V1 : V1 + mv] * restrict(r1, i, wide[1], V0 - wide[0] - 2, mv)
        slab_f[0, U1 + i] = line

    loop(mu, load1, 12)

    def slab_items(slab, b_from, steps):
        items = []
        for a in steps:
            rows, to = block_rows(a)
            items.append((slab.at[b_from, slice(U1 + rows.start, U1 + rows.stop)], slab.at[b_from, to], a, 0))
        return items

    f_v = copies([(slab_f.at[0, mid], slab_f.at[(-b) % 3, mid], 0, b) for b in (1, -1)]
                 + slab_items(slab_f, 0, (1, -1)), number(4))
    f_u = copies(slab_items(slab_f, 1, (1, -1)) + slab_items(slab_f, 2, (1, -1)), number(4))
    start(f_v)
    received(f_v[:2])
    start(f_u)
    received(f_v[2:])
    received(f_u)
    start(x_far)

    def lay_slab(slab, targets, steps):
        for a in steps:
            rows, to = block_rows(-a)
            def body():
                def one(i):
                    u = to.start + i
                    for x in targets:
                        for b in (-1, 0, 1):
                            x[0, u, V1 + b * mv : V1 + (b + 1) * mv] = slab[b % 3, u]
                loop(to.stop - to.start, one, 6)
            given(present(a), body)

    lay_slab(slab_f, (f1, x1), (0, -1, 1))

    def window1(h):
        lo = (V1 - h) // 8 * 8
        return lo, up8(V1 + mv + h) - lo

    level1 = (x1, s1, f1, d1, e1, band1)
    sweep(*level1, U1 - 8, mu + 16, window1(8))
    sweep(*level1, U1 - 6, mu + 12, window1(5))

    def own_x1(u):
        slab_x[0, U1 + u] = x1[0, U1 + u, V1 : V1 + mv]
        strip_x[0, u] = x1[0, U1 + u, V1 : V1 + 3]
        strip_x[1, u] = x1[0, U1 + u, V1 + mv - 3 : V1 + mv]

    loop(mu, own_x1, 12)
    at1 = window1(2)
    residual(*level1, down1, 4.0, U1 - 2, mu + 4, at1, r2)

    def load_2(i):
        c2[i, 0:cv] = restrict(r2, i, at1[1], V1 - at1[0] - 2, cv)

    loop(cu, load_2, 6)

    half = cu // 2
    for j in range(half):
        packed[j] = (c2[j] + pltpu.roll(c2[j + half], 64, 1))[0:cv]
        slots[me_u, 1, j] = packed[j]

    def gather(i, incoming):
        flat = lax.rem(me + 1 + i, n_all) if not incoming else lax.rem(me + n_all - 1 - i, n_all)
        u, v = place(flat)
        source_u, source_v, target_v = (u, v, me_v) if incoming else (me_u, me_v, v)
        return pltpu.make_async_remote_copy(
            src_ref=packed,
            dst_ref=slots.at[source_u, lax.rem(source_v - target_v + 1 + n_patch, n_patch)],
            send_sem=all_send.at[i],
            recv_sem=all_recv.at[i],
            device_id={"dir": u, "patch": v},
            device_id_type=MESH,
        )

    loop(n_all - 1, lambda i: gather(i, False).start())
    loop(n_all - 1, lambda i: gather(i, False).wait_send())
    loop(n_all - 1, lambda i: gather(i, True).wait_recv())

    x_v = copies([(slab_x.at[0, mid], slab_x.at[(-b) % 3, mid], 0, b) for b in (1, -1)]
                 + [(strip_x.at[1], slab_far.at[0, mid], 0, 2), (strip_x.at[0], slab_far.at[1, mid], 0, -2)], number(4))
    x_u = []
    for b in range(3):
        x_u += slab_items(slab_x, b, (1, -1, 2, -2))
    for b in range(2):
        x_u += slab_items(slab_far, b, (1, -1, 2, -2))
    x_u = copies(x_u, number(len(x_u)))

    start(x_v)

    low = lax.broadcasted_iota(jnp.int32, (cv, 128), 1) < 64
    for d in range(n_dir):
        for k in range(n_patch // 2):
            for j in range(half):
                a, b = slots[d, k, j], slots[d, k + n_patch // 2, j]
                load2[d * cu + j, k * cv : (k + 1) * cv] = jnp.where(low, a, pltpu.roll(b, 64, 1))
                load2[d * cu + half + j, k * cv : (k + 1) * cv] = jnp.where(low, pltpu.roll(a, 64, 1), b)

    def second_leg():
        received(x_v)
        start(x_u)
        received(x_far[:2])
        received(f_far[:2])
        start(far_second)

    coarse_cycle((cu * n_dir, cv * n_patch // 2), load2, tables, coarse, second_leg)

    span = (tv.shape[1] - 12) // 2

    def prolong(line, first, table, x, s):
        def one(i):
            b, h, a = (line(i, first + k) for k in range(3))
            tv[i, pl.ds(6, span, stride=2), :] = 0.125 * (b + a) + 0.75 * h
            tv[i, pl.ds(7, span, stride=2), :] = 0.5 * (h + a)

        loop(24, one, 8)
        n = tv.shape[1]

        def widen(i):
            y = split_mul(tv[pl.ds(8 * i, 8)].reshape(8 * n, 128), table[...])
            for w in range(x.shape[0]):
                for j in range(8):
                    tw[w, 8 * i + j] = y[j * n : (j + 1) * n, w * 128 : (w + 1) * 128]

        loop(3, widen)

        def add(t):
            for w in range(x.shape[0]):
                p, q, r = tw[w, t], tw[w, t + 1], tw[w, t + 2]
                for j, y in enumerate((0.5 * (p + q), 0.125 * (p + r) + 0.75 * q)):
                    u = 2 * t + j
                    x[w, u] = x[w, u] + jnp.where(s[w, u] > 0.0, y, 0.0)

        loop(21, add, 3)

    received(x_u)
    lay_slab(slab_x, (x1,), (0, -1, 1, -2, 2))
    for a in (0, -1, 1, -2, 2):
        rows, to = block_rows(-a)
        def body():
            def one(i):
                u = to.start + i
                x1[0, u, V1 - mv - 3 : V1 - mv] = slab_far[0, u]
                x1[0, u, V1 + 2 * mv : V1 + 2 * mv + 3] = slab_far[1, u]
            loop(to.stop - to.start, one, 3)
        given(present(a), body)
    x2 = coarse[0]
    edge = (x2.shape[0] - cu * n_dir) // 2
    prolong(lambda i, k: x2[edge + me_u * cu - (U1 + 1) // 2 + i, k : k + span], 5, up1, x1, s1)
    sweep(*level1, U1 - 12, mu + 24, window1(12))
    sweep(*level1, U1 - 9, mu + 18, window1(9))
    sweep(*level1, U1 - 6, mu + 12, window1(6))
    received(x_far[2:])
    received(f_far[2:])
    received(far_second)
    for x, halo in ((x0, xh), (f0, fh)):
        lay_sides(x, FAR, halo.far_v, halo.reach, halo.near)
        lay_sides(x, halo.near, halo.near_v, halo.reach)
        lay_ups(x, FAR, halo.far_u, halo.near)
    for made in (masks, f_near, x_near, f_v, f_u, x_v, x_u, x_far, f_far, far_second):
        sent(made)
    prolong(lambda i, k: x1[0, U1 - (U0 + 1) // 2 + i, k : k + span], 16, up0, x0, s0)
    level0 = (x0, s0, f0, d0, e0, band0)
    sweep(*level0, U0 - 6, nu + 12, wide)
    sweep(*level0, U0 - 3, nu + 6, wide)
    sweep(*level0, U0, nu, block0, out)
    assert taken[0] <= send_sem.shape[0]


def on_device(right_side, guess, mask_fine, mask_next):
    nu, nv, nw = right_side.shape
    n_dir, n_patch = lax.axis_size("dir"), lax.axis_size("patch")
    planes = nw // 128
    mu, mv = nu // 2, nv // 2
    cu, cv = mu // 2, mv // 2
    gu, gh = cu * n_dir, cv * n_patch // 2
    eu, eq = gu // 2, up8(gh // 4)
    rows0, cols0, rows1, cols1 = nu + 18, nv + 32, mu + 30, up8(mv + 37)
    operands = [right_side, guess, jnp.transpose(mask_fine, (0, 2, 1)), jnp.transpose(mask_next, (0, 2, 1))]
    operands += [jnp.asarray(np.eye(nv, 128, dtype=np.float32))]
    operands += [jnp.asarray(spots(nv, 16, cols0, 32, 9)), jnp.asarray(spots(mv, mv + 10, cols1, 16, mu + 3))]
    operands += [jnp.asarray(t) for t in fine_weights(nw) + coarse_weights(nw)]

    def vmem(*shape):
        return pltpu.VMEM(shape, jnp.float32)

    scratch = [pltpu.VMEM(t.shape, t.dtype) for t in operands]
    scratch += [vmem(planes, rows0, cols0, 128)] * 3 + [vmem(planes, rows0, nv + 16, 128)] * 2
    scratch += [vmem(1, rows1, cols1, 128)] * 3 + [vmem(1, rows1, cols1 - 16, 128)] * 2
    scratch += [vmem(nu + 4, nv + 16, 128), vmem(mu + 4, cols1 - 16, 128), vmem(mu, nv + 16, 128)]
    scratch += [vmem(24, cols1, 128), vmem(planes, 24, cols1, 128)] + [vmem(planes, nu, nv + 16, 128)] * 2
    scratch += [vmem(SWEEPS + 1, 2, planes, nu, 3, 128), vmem(SWEEPS, 2, planes, nu + 6, 3, 128)]
    scratch += [vmem(SWEEPS, 2, planes, 3, nv, 128)]
    scratch += Halo.scratch(planes, nu, nv, 5) + Halo.scratch(planes, nu, nv, 2)
    scratch += [vmem(3, rows0, planes, 128), vmem(5, rows1, 1, 128), vmem(3, nu, planes, 128), vmem(5, mu, 1, 128)]
    scratch += [vmem(3, rows1, mv, 128), vmem(3, rows1, mv, 128), vmem(2, mu, 3, 128), vmem(2, rows1, 3, 128)]
    scratch += [vmem(cu, up8(cv), 128), vmem(cu // 2, cv, 128), vmem(n_dir, n_patch, cu // 2, cv, 128)]
    scratch += [vmem(gu, gh, 128), vmem(gu + 20, gh + 16, 128), vmem(gu + 6, gh, 128), vmem(gu + 6, gh, 128)]
    scratch += [vmem(gu + 4, gh + 16, 128), vmem(gu, gh, 128), vmem(eu, eq + 16, 128), vmem(eu, eq, 128)]
    scratch += [vmem(eu + 6, eq, 128), vmem(eu + 6, eq, 128), vmem(eu, gh + 16, 128)]
    scratch += [pltpu.SemaphoreType.DMA((160,))] * 2 + [pltpu.SemaphoreType.DMA((n_dir * n_patch - 1,))] * 2
    scratch += [pltpu.SemaphoreType.DMA((len(operands),))]
    space = pl.BlockSpec(memory_space=pltpu.MemorySpace.HBM)
    return pl.pallas_call(
        functools.partial(kernel, (n_dir, n_patch, nu, nv, planes)),
        out_shape=jax.ShapeDtypeStruct(right_side.shape, jnp.float32),
        in_specs=[space] * len(operands),
        out_specs=pl.BlockSpec(memory_space=pltpu.VMEM),
        scratch_shapes=scratch,
        compiler_params=pltpu.CompilerParams(
            collective_id=0, has_side_effects=True, vmem_limit_bytes=60 * 2**20
        ),
        name="vcycle",
    )(*operands)


def solution(mesh):
    spec = P("dir", "patch", None)
    return jax.shard_map(
        on_device, mesh=mesh, in_specs=(spec,) * 4, out_specs=spec, check_vma=False
    )
```
